32 devices in a mesh: pod: 1 (over z), data: 4 (over y), model: 8 (over x, core).
Axes of the slice: x: 4, y: 4, z: 1, core: 2. Of those that a mesh axis runs over, the one named last changes fastest.
The devices are a block of a 4x4x8 slice.
Arguments:
- x_in: bfloat16 [4, 512, 6144], P(('pod', 'data'), 'model')
- dy_in: bfloat16 [4, 512, 6144], P(('pod', 'data'), 'model')
- w_q: bfloat16 [6144, 48, 128], P(None, 'model')
- w_k: bfloat16 [4, 6144, 128], replicated
- w_v: bfloat16 [4, 6144, 128], replicated
- w_o: bfloat16 [48, 128, 6144], P('model')
Outputs:
- output 1: bfloat16 [4, 512, 6144], P(('pod', 'data'), 'model')
- output 2: float32 [6144, 48, 128], P(('pod', 'data'), 'model')
- output 3: float32 [24576, 128], P(('pod', 'model', 'data'))
- output 4: float32 [24576, 128], P(('pod', 'model', 'data'))
- output 5: float32 [48, 128, 6144], P(('pod', 'model'), None, 'data')
All inputs are finite; a program needn't handle non-finite values.
Results may differ from the reference program's by a relative error of at most 0.0094734.
Values are sent between devices in bfloat16 or wider.
A program may use at most 768 MiB of HBM per device.

```python
import jax
import jax.numpy as jnp
from jax import lax

NUM_SEQS = 4
SEQ_LEN = 512
MODEL_DIM = 6144
Q_HEADS = 48
KV_HEADS = 4
HEAD_DIM = 128

GROUP_HEADS = Q_HEADS // KV_HEADS


def setup_inputs(seed: int = 0, part: int = 0) -> dict:
    shared_key = jax.random.key(seed)
    part_key = jax.random.fold_in(jax.random.key(seed + 1), part)
    key_x, key_dy = jax.random.split(part_key, 2)
    key_wq, key_wk, key_wv, key_wo = jax.random.split(shared_key, 4)
    act_shape = (NUM_SEQS, SEQ_LEN, MODEL_DIM)
    in_scale = MODEL_DIM ** -0.5
    out_scale = (Q_HEADS * HEAD_DIM) ** -0.5
    x_in = jax.random.normal(key_x, act_shape, jnp.float32)
    dy_in = jax.random.normal(key_dy, act_shape, jnp.float32)
    w_q = jax.random.normal(key_wq, (MODEL_DIM, Q_HEADS, HEAD_DIM), jnp.float32) * in_scale
    w_k = jax.random.normal(key_wk, (KV_HEADS, MODEL_DIM, HEAD_DIM), jnp.float32) * in_scale
    w_v = jax.random.normal(key_wv, (KV_HEADS, MODEL_DIM, HEAD_DIM), jnp.float32) * in_scale
    w_o = jax.random.normal(key_wo, (Q_HEADS, HEAD_DIM, MODEL_DIM), jnp.float32) * out_scale
    return {'x_in': x_in.astype(jnp.bfloat16), 'dy_in': dy_in.astype(jnp.bfloat16),
            'w_q': w_q.astype(jnp.bfloat16), 'w_k': w_k.astype(jnp.bfloat16),
            'w_v': w_v.astype(jnp.bfloat16), 'w_o': w_o.astype(jnp.bfloat16)}


def group_attention(operands):
    q_grp, k_one, v_one, dout_grp = operands
    score_scale = HEAD_DIM ** -0.5
    q_f32 = q_grp.astype(jnp.float32)
    k_f32 = k_one.astype(jnp.float32)
    v_f32 = v_one.astype(jnp.float32)
    dout_f32 = dout_grp.astype(jnp.float32)
    positions = jnp.arange(SEQ_LEN)
    causal = positions[:, None] >= positions[None, :]
    scores = jnp.einsum('qhe,ke->hqk', q_f32, k_f32) * score_scale
    attn_prob = jax.nn.softmax(jnp.where(causal, scores, -jnp.inf), axis=-1)
    prob_bf = attn_prob.astype(jnp.bfloat16).astype(jnp.float32)
    attn_out = jnp.einsum('hqk,ke->qhe', prob_bf, v_f32).astype(jnp.bfloat16)
    grad_prob = jnp.einsum('qhe,ke->hqk', dout_f32, v_f32)
    row_delta = jnp.einsum('qhe,qhe->hq', dout_f32, attn_out.astype(jnp.float32))
    grad_score = (attn_prob * (grad_prob - row_delta[:, :, None])).astype(jnp.bfloat16).astype(jnp.float32)
    grad_q = (jnp.einsum('hqk,ke->qhe', grad_score, k_f32) * score_scale).astype(jnp.bfloat16)
    grad_k = (jnp.einsum('hqk,qhe->ke', grad_score, q_f32) * score_scale).astype(jnp.bfloat16)
    grad_v = jnp.einsum('hqk,qhe->ke', prob_bf, dout_f32).astype(jnp.bfloat16)
    return attn_out, grad_q, grad_k, grad_v


def heads_to_items(per_head):
    return per_head.reshape(NUM_SEQS, SEQ_LEN, KV_HEADS, GROUP_HEADS, HEAD_DIM).transpose(0, 2, 1, 3, 4).reshape(NUM_SEQS * KV_HEADS, SEQ_LEN, GROUP_HEADS, HEAD_DIM)


def items_to_heads(per_item):
    return per_item.reshape(NUM_SEQS, KV_HEADS, SEQ_LEN, GROUP_HEADS, HEAD_DIM).transpose(0, 2, 1, 3, 4).reshape(NUM_SEQS, SEQ_LEN, Q_HEADS, HEAD_DIM)


def reference(x_in, dy_in, w_q, w_k, w_v, w_o):
    x_f32 = x_in.astype(jnp.float32)
    dy_f32 = dy_in.astype(jnp.float32)
    wq_f32 = w_q.astype(jnp.float32)
    wk_f32 = w_k.astype(jnp.float32)
    wv_f32 = w_v.astype(jnp.float32)
    wo_f32 = w_o.astype(jnp.float32)
    q_proj = jnp.einsum('std,dhe->sthe', x_f32, wq_f32).astype(jnp.bfloat16)
    k_proj = jnp.einsum('std,jde->sjte', x_f32, wk_f32).astype(jnp.bfloat16)
    v_proj = jnp.einsum('std,jde->sjte', x_f32, wv_f32).astype(jnp.bfloat16)
    dout_proj = jnp.einsum('std,hed->sthe', dy_f32, wo_f32).astype(jnp.bfloat16)
    item_count = NUM_SEQS * KV_HEADS
    attn_out, grad_q, grad_k, grad_v = lax.map(group_attention, (
        heads_to_items(q_proj), k_proj.reshape(item_count, SEQ_LEN, HEAD_DIM),
        v_proj.reshape(item_count, SEQ_LEN, HEAD_DIM), heads_to_items(dout_proj)))
    out_f32 = items_to_heads(attn_out).astype(jnp.float32)
    gq_f32 = items_to_heads(grad_q).astype(jnp.float32)
    gk_f32 = grad_k.reshape(NUM_SEQS, KV_HEADS, SEQ_LEN, HEAD_DIM).astype(jnp.float32)
    gv_f32 = grad_v.reshape(NUM_SEQS, KV_HEADS, SEQ_LEN, HEAD_DIM).astype(jnp.float32)
    dw_q = jnp.einsum('std,sthe->dhe', x_f32, gq_f32)
    dw_k = jnp.einsum('std,sjte->jde', x_f32, gk_f32).reshape(KV_HEADS * MODEL_DIM, HEAD_DIM)
    dw_v = jnp.einsum('std,sjte->jde', x_f32, gv_f32).reshape(KV_HEADS * MODEL_DIM, HEAD_DIM)
    dw_o = jnp.einsum('sthe,std->hed', out_f32, dy_f32)
    dx_f32 = (jnp.einsum('sthe,dhe->std', gq_f32, wq_f32)
              + jnp.einsum('sjte,jde->std', gk_f32, wk_f32)
              + jnp.einsum('sjte,jde->std', gv_f32, wv_f32))
    return dx_f32.astype(jnp.bfloat16), dw_q, dw_k, dw_v, dw_o
```

```python
import functools

import jax
import jax.numpy as jnp
from jax import lax
from jax.experimental import pallas as pl
from jax.experimental.pallas import tpu as pltpu
from jax.sharding import PartitionSpec as P

MESH = pl.DeviceIdType.MESH
F32 = jnp.float32
BF16 = jnp.bfloat16
VMEM_BYTES = 67043328


def dot(a, b, ca, cb):
    return lax.dot_general(a, b, (((ca,), (cb,)), ((), ())), preferred_element_type=F32)


def tile_of(n, t):
    return t if n % t == 0 else n


def kernel(cfg, x_ref, dy_ref, wq_ref, wk_ref, wv_ref, wo_ref,
           dx_ref, dwq_ref, dwk_ref, dwv_ref, dwo_ref,
           XS, DYS, XC, DYC, OA, DQA, QB, DOB, KV, QACC, KVACC, DKVR, DKVB,
           WQ, WKV, WO, MY, SX, RX, DXO, KS, KR, KOUT, OWQ, OWO,
           agr, ags, a2ar, a2as, yr, ys, dkr, dks, pxr, pxs, rsr, rss, exs, exr,
           lx, ldy, lwq, lwkv, lwo, lout):
    T, CW, E, NX, NY, NH = cfg
    NP = NH // 2
    R = 2 * NX * T
    HR = NX * T
    TH = T // 2
    scale = E ** -0.5
    pod = lax.axis_index('pod')
    y = lax.axis_index('data')
    m = lax.axis_index('model')
    c = lax.div(m, 2)
    h = lax.rem(m, 2)

    def at(dy_, dx_):
        return (pod, lax.rem(y + dy_ + NY, NY), 2 * lax.rem(c + dx_ + NX, NX) + h)

    XR, XL = at(0, 1), at(0, -1)
    YU, YD = at(1, 0), at(-1, 0)
    PT = (pod, y, 2 * c + 1 - h)

    def rc(src, dst, ssem, rsem, dev):
        return pltpu.make_async_remote_copy(src_ref=src, dst_ref=dst, send_sem=ssem, recv_sem=rsem,
                                            device_id=dev, device_id_type=MESH)

    def wait_recv(dst, sem):
        rc(dst, dst, sem, sem, PT).wait_recv()

    def wait_send(src, sem):
        rc(src, src, sem, sem, PT).wait_send()

    def chip(k):
        return lax.rem(c + k + NX, NX)

    def seq(k):
        return lax.rem(y + k + NY, NY)

    def rb(k):
        return pl.multiple_of((h * NX + chip(k)) * T, T)

    my_rows = rb(0)
    lxc = [pltpu.make_async_copy(x_ref.at[:, pl.ds(k * CW, CW)], XS.at[k, pl.ds(my_rows, T)], lx.at[k]) for k in range(NY)]
    ldc = [pltpu.make_async_copy(dy_ref.at[:, pl.ds(k * CW, CW)], DYS.at[k, pl.ds(my_rows, T)], ldy.at[k]) for k in range(NY)]
    for cp in lxc + ldc:
        cp.start()

    def wq_cp(k):
        return pltpu.make_async_copy(wq_ref.at[:, pl.ds(k * CW, CW), :], WQ, lwq.at[0])

    def wkv_cp(k):
        return [pltpu.make_async_copy(wk_ref.at[c, pl.ds(k * CW, CW)], WKV.at[0], lwkv.at[0]),
                pltpu.make_async_copy(wv_ref.at[c, pl.ds(k * CW, CW)], WKV.at[1], lwkv.at[1])]

    def wo_cp(k):
        return pltpu.make_async_copy(wo_ref.at[:, :, pl.ds(k * CW, CW)], WO, lwo.at[0])

    wq_cp(0).start()
    for cp in wkv_cp(0):
        cp.start()
    wo_cp(0).start()

    bar = pltpu.get_barrier_semaphore()
    peers = [XR, XL, PT] + [at(j, 0) for j in range(1, NY)]
    for dev in peers:
        pl.semaphore_signal(bar, inc=1, device_id=dev, device_id_type=MESH)
    pl.semaphore_wait(bar, len(peers))
    for cp in lxc + ldc:
        cp.wait()

    items = ([(XS, k) for k in range(NY)] + [(DYS, k) for k in range(NY)]
             + [(XC, seq(j)) for j in range(1, NY)] + [(DYC, seq(j)) for j in range(1, NY)])
    N_IT = len(items)

    def own(i):
        buf, ix = items[i]
        if i >= 2 * NY:
            t, j = divmod(i - 2 * NY, NY - 1)
            wait_recv(buf.at[ix, pl.ds(my_rows, T)], a2ar.at[t, j])
        blk = buf.at[ix, pl.ds(my_rows, T)]
        rc(blk, blk, ags.at[i], agr.at[i, 0], XR).start()
        rc(blk, blk, ags.at[i], agr.at[i, 1], XL).start()
        rc(blk, blk, ags.at[i], agr.at[i, 4], PT).start()

    def fwd(i):
        buf, ix = items[i]
        lb, rb_ = rb(-1), rb(1)
        blk = buf.at[ix, pl.ds(lb, T)]
        wait_recv(blk, agr.at[i, 0])
        half = buf.at[ix, pl.ds(lb, TH)]
        rc(half, half, ags.at[i], agr.at[i, 2], XR).start()
        rc(blk, blk, ags.at[i], agr.at[i, 4], PT).start()
        blk = buf.at[ix, pl.ds(rb_, T)]
        wait_recv(blk, agr.at[i, 1])
        half = buf.at[ix, pl.ds(pl.multiple_of(rb_ + TH, TH), TH)]
        rc(half, half, ags.at[i], agr.at[i, 3], XL).start()
        rc(blk, blk, ags.at[i], agr.at[i, 4], PT).start()

    def opp(i):
        buf, ix = items[i]
        ob = rb(2)
        wait_recv(buf.at[ix, pl.ds(ob, TH)], agr.at[i, 2])
        wait_recv(buf.at[ix, pl.ds(pl.multiple_of(ob + TH, TH), TH)], agr.at[i, 3])
        blk = buf.at[ix, pl.ds(ob, T)]
        rc(blk, blk, ags.at[i], agr.at[i, 4], PT).start()

    def fin(i):
        buf, ix = items[i]
        wait_recv(buf.at[ix, pl.ds(pl.multiple_of((1 - h) * HR, HR), HR)], agr.at[i, 4])

    def ag_sent(i):
        buf, ix = items[i]
        wait_send(buf.at[ix, pl.ds(0, 7 * T)], ags.at[i])

    def ybuf(q):
        return (OA if q < NP else DQA).at[q % NP]

    def yown(q):
        b = ybuf(q).at[y]
        rc(b, b, ys.at[q], yr.at[q, 0], YU).start()
        rc(b, b, ys.at[q], yr.at[q, 1], YD).start()

    def yfwd(q):
        b = ybuf(q)
        wait_recv(b.at[seq(-1)], yr.at[q, 0])
        half = b.at[seq(-1), pl.ds(0, HR)]
        rc(half, half, ys.at[q], yr.at[q, 2], YU).start()
        wait_recv(b.at[seq(1)], yr.at[q, 1])
        half = b.at[seq(1), pl.ds(HR, HR)]
        rc(half, half, ys.at[q], yr.at[q, 3], YD).start()

    def yopp(q):
        b = ybuf(q)
        wait_recv(b.at[seq(2), pl.ds(0, HR)], yr.at[q, 2])
        wait_recv(b.at[seq(2), pl.ds(HR, HR)], yr.at[q, 3])

    def ysent(q):
        wait_send(ybuf(q).at[pl.ds(0, 3)], ys.at[q])

    def proj_x(k):
        wq_cp(k).wait()
        for cp in wkv_cp(k):
            cp.wait()

        def body(p, _):
            w = jnp.concatenate([WQ[2 * p], WQ[2 * p + 1]], axis=1)
            d = dot(XS[k], w, 1, 0)
            QACC[p] = d if k == 0 else QACC[p] + d
            return 0
        lax.fori_loop(0, NP, body, 0)
        d = dot(XS[k], jnp.concatenate([WKV[0], WKV[1]], axis=1), 1, 0)
        KVACC[...] = d if k == 0 else KVACC[...] + d
        nk = (k + 1) % NY
        wq_cp(nk).start()
        for cp in wkv_cp(nk):
            cp.start()

    def proj_dy(k):
        wo_cp(k).wait()

        def body(p, _):
            w = WO[pl.ds(2 * p, 2)].reshape(2 * E, CW)
            d = dot(DYS[k], w, 1, 1)
            QACC[p] = d if k == 0 else QACC[p] + d
            return 0
        lax.fori_loop(0, NP, body, 0)
        if k + 1 < NY:
            wo_cp(k + 1).start()

    def copy_acc(dst):
        def body(p, _):
            dst[p] = QACC[p].astype(BF16)
            return 0
        lax.fori_loop(0, NP, body, 0)

    QR = HR

    def pos(i):
        g = lax.div(i, T)
        return (2 * lax.rem(g, NX) + lax.div(g, NX)) * T + lax.rem(i, T)

    def probs(p, a, rows0):
        q = QB[p, pl.ds(rows0, QR), a * E:(a + 1) * E]
        s = dot(q, KV[0], 1, 1) * scale
        qp = pos(lax.broadcasted_iota(jnp.int32, (QR, 1), 0) + rows0)
        kp = pos(lax.broadcasted_iota(jnp.int32, (1, R), 1))
        s = jnp.where(qp >= kp, s, -jnp.inf)
        e = jnp.exp(s - jnp.max(s, axis=1, keepdims=True))
        return q, e / jnp.sum(e, axis=1, keepdims=True)

    def attn_fwd(p):
        def body(b, _):
            rows0 = pl.multiple_of(b * QR, QR)
            for a in range(2):
                _, pr = probs(p, a, rows0)
                OA[p, y, pl.ds(rows0, QR), a * E:(a + 1) * E] = dot(pr.astype(BF16), KV[1], 1, 0).astype(BF16)
            return 0
        lax.fori_loop(0, R // QR, body, 0)

    def attn_bwd(p):
        def body(b, _):
            rows0 = pl.multiple_of(b * QR, QR)
            for a in range(2):
                ln = slice(a * E, (a + 1) * E)
                q, pr = probs(p, a, rows0)
                do = DOB[p, pl.ds(rows0, QR), ln]
                o = OA[p, y, pl.ds(rows0, QR), ln]
                delta = jnp.sum(do.astype(F32) * o.astype(F32), axis=1, keepdims=True)
                dp = dot(do, KV[1], 1, 1)
                ds = (pr * (dp - delta)).astype(BF16)
                DQA[p, y, pl.ds(rows0, QR), ln] = (dot(ds, KV[0], 1, 0) * scale).astype(BF16)
                KVACC[:, :E] = KVACC[:, :E] + dot(ds, q, 0, 0)
                KVACC[:, E:] = KVACC[:, E:] + dot(pr.astype(BF16), do, 0, 0)
            return 0
        lax.fori_loop(0, R // QR, body, 0)

    def dkv_send():
        KVACC[:, :E] = KVACC[:, :E] * scale
        rc(KVACC, DKVR, exs.at[0], exr.at[0], PT).start()

    def dkv_sum():
        wait_recv(DKVR, exr.at[0])
        tot = (KVACC[...] + DKVR[...]).astype(BF16)
        DKVB[0] = tot[:, :E]
        DKVB[1] = tot[:, E:]

    KB = CW // 2
    KT = tile_of(KB, 256)

    def dwkv_tile(r, t):
        ck = 2 * h + lax.div(r, 2)
        off = pl.multiple_of(KB * lax.rem(r, 2) + t * KT, KT)
        kv = jnp.concatenate([DKVB[0], DKVB[1]], axis=1)
        return dot(XS[ck, :, pl.ds(off, KT)], kv, 0, 0)

    def dwkv_send(j):
        r = seq(j)

        def body(t, _):
            KS[j - 1, pl.ds(pl.multiple_of(t * KT, KT), KT), :] = dwkv_tile(r, t).astype(BF16)
            return 0
        lax.fori_loop(0, KB // KT, body, 0)
        rc(KS.at[j - 1], KR.at[NY - j - 1], dks.at[0], dkr.at[NY - j - 1], at(j, 0)).start()

    def dwkv_final():
        for j in range(NY - 1):
            wait_recv(KR.at[j], dkr.at[j])

        def body(t, _):
            rows = pl.ds(pl.multiple_of(t * KT, KT), KT)
            v = dwkv_tile(y, t)
            for j in range(NY - 1):
                v = v + KR[j, rows, :].astype(F32)
            KOUT[0, rows, :] = v[:, :E]
            KOUT[1, rows, :] = v[:, E:]
            return 0
        lax.fori_loop(0, KB // KT, body, 0)
        for i, ref in enumerate((dwk_ref, dwv_ref)):
            pltpu.make_async_copy(KOUT.at[i], ref, lout.at[i]).start()

    def dwkv_out_wait():
        for i, ref in enumerate((dwk_ref, dwv_ref)):
            pltpu.make_async_copy(KOUT.at[i], ref, lout.at[i]).wait()

    NT = tile_of(CW, 256)

    def dxc(k):
        wq_cp(k).wait()
        for cp in wkv_cp(k):
            cp.wait()

        def body(t, _):
            off = pl.multiple_of(t * NT, NT)
            rows = pl.ds(off, NT)
            v = dot(DKVB[h], WKV[h, rows, :], 1, 1)
            for p in range(NP):
                w = jnp.concatenate([WQ[2 * p, rows, :], WQ[2 * p + 1, rows, :]], axis=1)
                v = v + dot(DQA[p, y], w, 1, 1)
            lo, hi = v[:HR], v[HR:]
            MY[k, :, pl.ds(off, NT)] = jnp.where(h == 0, lo, hi)
            DYS[k, pl.ds(HR, HR), pl.ds(off, NT)] = jnp.where(h == 0, hi, lo).astype(BF16)
            return 0
        lax.fori_loop(0, CW // NT, body, 0)
        if k + 1 < NY:
            wq_cp(k + 1).start()
            for cp in wkv_cp(k + 1):
                cp.start()
        rc(DYS.at[k, pl.ds(HR, HR)], DYS.at[k, pl.ds(0, HR)], pxs.at[k], pxr.at[k], PT).start()

    def blk(k, cc, o, n):
        rows = pl.ds(pl.multiple_of(cc * T + o, TH), n)
        return MY[k, rows, :] + DYS[k, rows, :].astype(F32)

    def rs1(k):
        wait_recv(DYS.at[k, pl.ds(0, HR)], pxr.at[k])
        SX[k, 0:T, :] = blk(k, chip(2), 0, T).astype(BF16)
        s, d = SX.at[k, pl.ds(0, TH)], RX.at[k, pl.ds(0, TH)]
        rc(s, d, rss.at[k], rsr.at[k, 0], XR).start()
        s, d = SX.at[k, pl.ds(TH, TH)], RX.at[k, pl.ds(TH, TH)]
        rc(s, d, rss.at[k], rsr.at[k, 1], XL).start()

    def rs2(k):
        wait_recv(RX.at[k, pl.ds(0, TH)], rsr.at[k, 0])
        SX[k, T:T + TH, :] = (blk(k, chip(1), 0, TH) + RX[k, 0:TH, :].astype(F32)).astype(BF16)
        SX[k, T + TH:2 * T, :] = blk(k, chip(1), TH, TH).astype(BF16)
        s, d = SX.at[k, pl.ds(T, T)], RX.at[k, pl.ds(T, T)]
        rc(s, d, rss.at[k], rsr.at[k, 2], XR).start()
        wait_recv(RX.at[k, pl.ds(TH, TH)], rsr.at[k, 1])
        SX[k, 2 * T:2 * T + TH, :] = blk(k, chip(-1), 0, TH).astype(BF16)
        SX[k, 2 * T + TH:3 * T, :] = (blk(k, chip(-1), TH, TH) + RX[k, TH:T, :].astype(F32)).astype(BF16)
        s, d = SX.at[k, pl.ds(2 * T, T)], RX.at[k, pl.ds(2 * T, T)]
        rc(s, d, rss.at[k], rsr.at[k, 3], XL).start()

    def dx_out(k):
        return pltpu.make_async_copy(DXO.at[k], dx_ref.at[:, pl.ds(k * CW, CW)], lout.at[2 + k])

    def rs3(k):
        wait_recv(RX.at[k, pl.ds(T, T)], rsr.at[k, 2])
        wait_recv(RX.at[k, pl.ds(2 * T, T)], rsr.at[k, 3])
        v = blk(k, c, 0, T) + RX[k, T:2 * T, :].astype(F32) + RX[k, 2 * T:3 * T, :].astype(F32)
        DXO[k] = v.astype(BF16)
        dx_out(k).start()

    def dwo_out(p):
        return pltpu.make_async_copy(OWO, dwo_ref.at[pl.ds(2 * p, 2)], lout.at[2 + NY])

    def dwq_out(p):
        return pltpu.make_async_copy(OWQ, dwq_ref.at[pl.ds(2 * p, 2)], lout.at[3 + NY])

    OT = tile_of(CW, 512)

    def dwo(p):
        yopp(p)
        if p:
            dwo_out(p - 1).wait()

        def body(t, _):
            cols = pl.ds(pl.multiple_of(t * OT, OT), OT)
            v = dot(OA[p, 0], DYC[0, :, cols], 0, 0)
            for s in range(1, NY):
                v = v + dot(OA[p, s], DYC[s, :, cols], 0, 0)
            OWO[0, :, cols] = v[:E]
            OWO[1, :, cols] = v[E:]
            return 0
        lax.fori_loop(0, CW // OT, body, 0)
        dwo_out(p).start()

    def dwq(p):
        yopp(NP + p)
        if p:
            dwq_out(p - 1).wait()

        def body(t, _):
            cols = pl.ds(pl.multiple_of(t * NT, NT), NT)
            v = dot(XC[0, :, cols], DQA[p, 0], 0, 0)
            for s in range(1, NY):
                v = v + dot(XC[s, :, cols], DQA[p, s], 0, 0)
            OWQ[0, cols, :] = v[:, :E]
            OWQ[1, cols, :] = v[:, E:]
            return 0
        lax.fori_loop(0, CW // NT, body, 0)
        dwq_out(p).start()

    def own_cols(dst, src):
        def body(t, _):
            rows = pl.ds(pl.multiple_of(t * T, T), T)
            dst[y, rows, :] = src[y, rows, :]
            return 0
        lax.fori_loop(0, R // T, body, 0)

    own(0)
    own(1)
    for t, (src, dst) in enumerate(((XS, XC), (DYS, DYC))):
        for j in range(1, NY):
            rc(src.at[seq(j), pl.ds(my_rows, T)], dst.at[y, pl.ds(my_rows, T)],
               a2as.at[t], a2ar.at[t, NY - j - 1], at(j, 0)).start()

    def compute(i):
        if i < NY:
            proj_x(i)
            if i == NY - 1:
                copy_acc(QB)
                KV[0] = KVACC[:, :E].astype(BF16)
                KV[1] = KVACC[:, E:].astype(BF16)
                for p in range(NP):
                    attn_fwd(p)
                    yown(p)
                own_cols(XC, XS)
        elif i < 2 * NY:
            proj_dy(i - NY)
            if i >= NY + 1:
                yfwd(i - NY - 1)
            if i == 2 * NY - 1:
                copy_acc(DOB)
                own_cols(DYC, DYS)
                KVACC[...] = jnp.zeros_like(KVACC)
                attn_bwd(0)
                yown(NP)
        elif i < 2 * NY + NP - 1:
            p = i - 2 * NY + 1
            attn_bwd(p)
            yown(NP + p)
            if p == NP - 1:
                for k in range(NY):
                    ag_sent(NY + k)
                wait_send(DYS.at[0, pl.ds(0, 3 * T)], a2as.at[1])
                dkv_send()
        elif i == 2 * NY + NP - 1:
            dkv_sum()
            for j in range(1, NY):
                dwkv_send(j)
            yfwd(NP)
        elif i == 2 * NY + NP:
            dxc(0)
            yfwd(NP + 1)
        elif i == 2 * NY + NP + 1:
            dxc(1)
            rs1(0)
            yfwd(NP + 2)

    for i in range(N_IT + 1):
        if i < N_IT:
            fwd(i)
        if i + 2 < N_IT:
            own(i + 2)
        if i >= 1:
            opp(i - 1)
            fin(i - 1)
            compute(i - 1)

    rs1(1)
    rs2(0)
    dxc(2)
    rs1(2)
    rs2(1)
    dxc(3)
    rs1(3)
    rs2(2)
    rs3(0)
    dwo(0)
    rs2(3)
    rs3(1)
    dwq(0)
    rs3(2)
    dwo(1)
    dwq(1)
    rs3(3)
    dwo(2)
    dwq(2)
    dwkv_final()

    for i in list(range(NY)) + list(range(2 * NY, N_IT)):
        ag_sent(i)
    wait_send(XS.at[0, pl.ds(0, 3 * T)], a2as.at[0])
    for q in range(2 * NP):
        ysent(q)
    wait_send(KVACC, exs.at[0])
    wait_send(KS, dks.at[0])
    for k in range(NY):
        wait_send(DYS.at[k, pl.ds(HR, HR)], pxs.at[k])
        wait_send(SX.at[k], rss.at[k])
        dx_out(k).wait()
    dwkv_out_wait()
    dwo_out(NP - 1).wait()
    dwq_out(NP - 1).wait()


def solution(mesh):
    model_size = mesh.shape['model']
    tok_spec = P(('pod', 'data'), 'model', None)

    def device_step(x_loc, dy_loc, w_q, w_k, w_v, w_o):
        T, D = x_loc.shape[1:]
        NH, E = w_q.shape[1:]
        KVH = w_k.shape[0]
        NX = model_size // 2
        NY = mesh.shape['data']
        assert NX == 4 and NY == 4 and KVH == NX and NH == 6
        NP = NH // 2
        CW = D // NY
        R = model_size * T
        KB = CW // 2
        cfg = (T, CW, E, NX, NY, NH)
        V = pltpu.VMEM
        S = pltpu.SemaphoreType.DMA
        n_it = 4 * NY - 2
        scratch = [
            V((NY, R, CW), BF16), V((NY, R, CW), BF16), V((NY, R, CW), BF16), V((NY, R, CW), BF16),
            V((NP, NY, R, 2 * E), BF16), V((NP, NY, R, 2 * E), BF16),
            V((NP, R, 2 * E), BF16), V((NP, R, 2 * E), BF16), V((2, R, E), BF16),
            V((NP, R, 2 * E), F32), V((R, 2 * E), F32), V((R, 2 * E), F32), V((2, R, E), BF16),
            V((NH, CW, E), BF16), V((2, CW, E), BF16), V((NH, E, CW), BF16),
            V((NY, R // 2, CW), F32), V((NY, 3 * T, CW), BF16), V((NY, 3 * T, CW), BF16), V((NY, T, CW), BF16),
            V((NY - 1, KB, 2 * E), BF16), V((NY - 1, KB, 2 * E), BF16), V((2, KB, E), F32),
            V((2, CW, E), F32), V((2, E, CW), F32),
            S((n_it, 5)), S((n_it,)), S((2, NY - 1)), S((2,)), S((2 * NP, 4)), S((2 * NP,)),
            S((NY - 1,)), S((1,)), S((NY,)), S((NY,)), S((NY, 4)), S((NY,)), S((1,)), S((1,)),
            S((NY,)), S((NY,)), S((1,)), S((2,)), S((1,)), S((4 + NY,)),
        ]
        any_spec = pl.BlockSpec(memory_space=pl.ANY)
        dx, dwq, dwk, dwv, dwo = pl.pallas_call(
            functools.partial(kernel, cfg),
            out_shape=[jax.ShapeDtypeStruct((T, D), BF16), jax.ShapeDtypeStruct((NH, CW, E), F32),
                       jax.ShapeDtypeStruct((KB, E), F32), jax.ShapeDtypeStruct((KB, E), F32),
                       jax.ShapeDtypeStruct((NH, E, CW), F32)],
            in_specs=[any_spec] * 6,
            out_specs=[any_spec] * 5,
            scratch_shapes=scratch,
            compiler_params=pltpu.CompilerParams(collective_id=0, has_side_effects=True, vmem_limit_bytes=VMEM_BYTES),
            name='attn_bwd_fused',
        )(x_loc[0], dy_loc[0], w_q.transpose(1, 0, 2), w_k, w_v, w_o)
        return dx[None], dwq.transpose(1, 0, 2), dwk, dwv, dwo

    kv_rows = P(('pod', 'model', 'data'), None)
    return jax.shard_map(device_step, mesh=mesh,
                         in_specs=(tok_spec, tok_spec, P(None, 'model', None), P(), P(), P('model', None, None)),
                         out_specs=(tok_spec, P(('pod', 'data'), 'model', None), kv_rows, kv_rows, P(('pod', 'model'), None, 'data')),
                         check_vma=False)
```

```python
import functools

import jax
import jax.numpy as jnp
from jax import lax
from jax.experimental import pallas as pl
from jax.experimental.pallas import tpu as pltpu
from jax.sharding import PartitionSpec as P

MESH = pl.DeviceIdType.MESH
F32 = jnp.float32
BF16 = jnp.bfloat16
VMEM_BYTES = 67043328


def dot(a, b, ca, cb):
    return lax.dot_general(a, b, (((ca,), (cb,)), ((), ())), preferred_element_type=F32)


def tile_of(n, t):
    return t if n % t == 0 else n


def kernel(cfg, x_ref, dy_ref, wq_ref, wk_ref, wv_ref, wo_ref,
           dx_ref, dwq_ref, dwk_ref, dwv_ref, dwo_ref,
           XS, DYS, XC, DYC, OA, DQA, QB, DOB, KV, QACC, KVACC, DKVR, DKVB,
           WQ, WKV, WO, MY, SX, RX, DXO, KS, KR, KOUT, OWQ, OWO,
           agr, ags, a2ar, a2as, xcr, xcs, yr, ys, dkr, dks, pxr, pxs, rsr, rss, exs, exr,
           lx, ldy, lwq, lwkv, lwo, lout):
    T, CW, E, NX, NY, NH = cfg
    NP = NH // 2
    R = 2 * NX * T
    HR = NX * T
    TH = T // 2
    scale = E ** -0.5
    pod = lax.axis_index('pod')
    y = lax.axis_index('data')
    m = lax.axis_index('model')
    c = lax.div(m, 2)
    h = lax.rem(m, 2)

    def at(dy_, dx_):
        return (pod, lax.rem(y + dy_ + NY, NY), 2 * lax.rem(c + dx_ + NX, NX) + h)

    XR, XL = at(0, 1), at(0, -1)
    YU, YD = at(1, 0), at(-1, 0)
    PT = (pod, y, 2 * c + 1 - h)

    def rc(src, dst, ssem, rsem, dev):
        return pltpu.make_async_remote_copy(src_ref=src, dst_ref=dst, send_sem=ssem, recv_sem=rsem,
                                            device_id=dev, device_id_type=MESH)

    def wait_recv(dst, sem):
        rc(dst, dst, sem, sem, PT).wait_recv()

    def wait_send(src, sem):
        rc(src, src, sem, sem, PT).wait_send()

    def chip(k):
        return lax.rem(c + k + NX, NX)

    def seq(k):
        return lax.rem(y + k + NY, NY)

    def rb(k):
        return pl.multiple_of((h * NX + chip(k)) * T, T)

    my_rows = rb(0)
    def mul(k, n):
        return pl.multiple_of(k * n, n)

    def wq_cp(k):
        return pltpu.make_async_copy(wq_ref.at[:, pl.ds(mul(k, CW), CW), :], WQ, lwq.at[0])

    def wkv_cp(k):
        return [pltpu.make_async_copy(wk_ref.at[c, pl.ds(mul(k, CW), CW)], WKV.at[0], lwkv.at[0]),
                pltpu.make_async_copy(wv_ref.at[c, pl.ds(mul(k, CW), CW)], WKV.at[1], lwkv.at[1])]

    def wo_cp(k):
        return pltpu.make_async_copy(wo_ref.at[:, :, pl.ds(k * CW, CW)], WO, lwo.at[0])

    bar = pltpu.get_barrier_semaphore()
    peers = [XR, XL, PT] + [at(j, 0) for j in range(1, NY)]
    for dev in peers:
        pl.semaphore_signal(bar, inc=1, device_id=dev, device_id_type=MESH)
    x_order = [seq(1), seq(-1), seq(2), y]
    lxc = [pltpu.make_async_copy(x_ref.at[:, pl.ds(k * CW, CW)], XS.at[k, pl.ds(my_rows, T)], lx.at[k]) for k in range(NY)]
    ldc = [pltpu.make_async_copy(dy_ref.at[:, pl.ds(k * CW, CW)], DYS.at[k, pl.ds(my_rows, T)], ldy.at[k]) for k in range(NY)]
    for cp in lxc:
        cp.start()
    for cp in lxc:
        cp.wait()
    for cp in ldc:
        cp.start()
    wq_cp(x_order[0]).start()
    for cp in wkv_cp(x_order[0]):
        cp.start()
    wo_cp(0).start()
    pl.semaphore_wait(bar, len(peers))

    items = ([(XS, k) for k in x_order] + [(DYS, k) for k in range(NY)]
             + [(DYC, seq(j)) for j in range(1, NY)] + [(XC, seq(2))])
    N_IT = len(items)

    def own(i):
        buf, ix = items[i]
        if i >= 2 * NY:
            wait_recv(buf.at[ix, pl.ds(my_rows, T)], a2ar.at[i - 2 * NY])
        blk = buf.at[ix, pl.ds(my_rows, T)]
        rc(blk, blk, ags.at[i], agr.at[i, 0], XR).start()
        rc(blk, blk, ags.at[i], agr.at[i, 1], XL).start()
        rc(blk, blk, ags.at[i], agr.at[i, 4], PT).start()

    def fwd(i):
        buf, ix = items[i]
        lb, rb_ = rb(-1), rb(1)
        blk = buf.at[ix, pl.ds(lb, T)]
        wait_recv(blk, agr.at[i, 0])
        half = buf.at[ix, pl.ds(lb, TH)]
        rc(half, half, ags.at[i], agr.at[i, 2], XR).start()
        rc(blk, blk, ags.at[i], agr.at[i, 4], PT).start()
        blk = buf.at[ix, pl.ds(rb_, T)]
        wait_recv(blk, agr.at[i, 1])
        half = buf.at[ix, pl.ds(pl.multiple_of(rb_ + TH, TH), TH)]
        rc(half, half, ags.at[i], agr.at[i, 3], XL).start()
        rc(blk, blk, ags.at[i], agr.at[i, 4], PT).start()

    def opp(i):
        buf, ix = items[i]
        ob = rb(2)
        wait_recv(buf.at[ix, pl.ds(ob, TH)], agr.at[i, 2])
        wait_recv(buf.at[ix, pl.ds(pl.multiple_of(ob + TH, TH), TH)], agr.at[i, 3])
        blk = buf.at[ix, pl.ds(ob, T)]
        rc(blk, blk, ags.at[i], agr.at[i, 4], PT).start()

    def fin(i):
        buf, ix = items[i]
        wait_recv(buf.at[ix, pl.ds(pl.multiple_of((1 - h) * HR, HR), HR)], agr.at[i, 4])

    def ag_sent(i):
        buf, ix = items[i]
        wait_send(buf.at[ix, pl.ds(0, 7 * T)], ags.at[i])

    par = pl.ds(mul(h, HR), HR)

    def xc_send(n):
        rc(XS.at[x_order[n], par], XC.at[y, par], xcs.at[n], xcr.at[n], (YU, YD)[n]).start()

    def xc_fwd(n):
        b = XC.at[seq((-1, 1)[n]), par]
        wait_recv(b, xcr.at[n])
        rc(b, b, xcs.at[2 + n], xcr.at[2 + n], PT).start()

    def xc_fin(n):
        wait_recv(XC.at[seq((-1, 1)[n]), pl.ds(mul(1 - h, HR), HR)], xcr.at[2 + n])

    def ybuf(q):
        return (OA if q < NP else DQA).at[q % NP]

    def yown(q):
        b = ybuf(q).at[y]
        rc(b, b, ys.at[q], yr.at[q, 0], YU).start()
        rc(b, b, ys.at[q], yr.at[q, 1], YD).start()

    def yfwd(q):
        b = ybuf(q)
        wait_recv(b.at[seq(-1)], yr.at[q, 0])
        half = b.at[seq(-1), pl.ds(0, HR)]
        rc(half, half, ys.at[q], yr.at[q, 2], YU).start()
        wait_recv(b.at[seq(1)], yr.at[q, 1])
        half = b.at[seq(1), pl.ds(HR, HR)]
        rc(half, half, ys.at[q], yr.at[q, 3], YD).start()

    def yopp(q):
        b = ybuf(q)
        wait_recv(b.at[seq(2), pl.ds(0, HR)], yr.at[q, 2])
        wait_recv(b.at[seq(2), pl.ds(HR, HR)], yr.at[q, 3])

    def ysent(q):
        wait_send(ybuf(q).at[pl.ds(0, 3)], ys.at[q])

    def proj_x(i):
        k = x_order[i]
        wq_cp(k).wait()
        for cp in wkv_cp(k):
            cp.wait()

        def body(p, _):
            w = jnp.concatenate([WQ[2 * p], WQ[2 * p + 1]], axis=1)
            d = dot(XS[k], w, 1, 0)
            QACC[p] = d if i == 0 else QACC[p] + d
            return 0
        lax.fori_loop(0, NP, body, 0)
        d = dot(XS[k], jnp.concatenate([WKV[0], WKV[1]], axis=1), 1, 0)
        KVACC[...] = d if i == 0 else KVACC[...] + d
        nk = x_order[i + 1] if i + 1 < NY else 0
        wq_cp(nk).start()
        for cp in wkv_cp(nk):
            cp.start()

    def proj_dy(k):
        wo_cp(k).wait()

        def body(p, _):
            w = WO[pl.ds(2 * p, 2)].reshape(2 * E, CW)
            d = dot(DYS[k], w, 1, 1)
            QACC[p] = d if k == 0 else QACC[p] + d
            return 0
        lax.fori_loop(0, NP, body, 0)
        if k + 1 < NY:
            wo_cp(k + 1).start()

    def copy_acc(dst):
        def body(p, _):
            dst[p] = QACC[p].astype(BF16)
            return 0
        lax.fori_loop(0, NP, body, 0)

    QR = HR

    def pos(i):
        g = lax.div(i, T)
        return (2 * lax.rem(g, NX) + lax.div(g, NX)) * T + lax.rem(i, T)

    def probs(p, a, rows0):
        q = QB[p, pl.ds(rows0, QR), a * E:(a + 1) * E]
        s = dot(q, KV[0], 1, 1) * scale
        qp = pos(lax.broadcasted_iota(jnp.int32, (QR, 1), 0) + rows0)
        kp = pos(lax.broadcasted_iota(jnp.int32, (1, R), 1))
        s = jnp.where(qp >= kp, s, -jnp.inf)
        e = jnp.exp(s - jnp.max(s, axis=1, keepdims=True))
        return q, e / jnp.sum(e, axis=1, keepdims=True)

    def attn_fwd(p):
        def body(b, _):
            rows0 = pl.multiple_of(b * QR, QR)
            for a in range(2):
                _, pr = probs(p, a, rows0)
                OA[p, y, pl.ds(rows0, QR), a * E:(a + 1) * E] = dot(pr.astype(BF16), KV[1], 1, 0).astype(BF16)
            return 0
        lax.fori_loop(0, R // QR, body, 0)

    def attn_bwd(p):
        def body(b, _):
            rows0 = pl.multiple_of(b * QR, QR)
            for a in range(2):
                ln = slice(a * E, (a + 1) * E)
                q, pr = probs(p, a, rows0)
                do = DOB[p, pl.ds(rows0, QR), ln]
                o = OA[p, y, pl.ds(rows0, QR), ln]
                delta = jnp.sum(do.astype(F32) * o.astype(F32), axis=1, keepdims=True)
                dp = dot(do, KV[1], 1, 1)
                ds = (pr * (dp - delta)).astype(BF16)
                DQA[p, y, pl.ds(rows0, QR), ln] = (dot(ds, KV[0], 1, 0) * scale).astype(BF16)
                KVACC[:, :E] = KVACC[:, :E] + dot(ds, q, 0, 0)
                KVACC[:, E:] = KVACC[:, E:] + dot(pr.astype(BF16), do, 0, 0)
            return 0
        lax.fori_loop(0, R // QR, body, 0)

    def dkv_send():
        KVACC[:, :E] = KVACC[:, :E] * scale
        rc(KVACC, DKVR, exs.at[0], exr.at[0], PT).start()

    def dkv_sum():
        wait_recv(DKVR, exr.at[0])
        tot = (KVACC[...] + DKVR[...]).astype(BF16)
        DKVB[0] = tot[:, :E]
        DKVB[1] = tot[:, E:]

    KB = CW // 2
    KT = tile_of(KB, 256)

    def dwkv_tile(r, t):
        ck = 2 * h + lax.div(r, 2)
        off = pl.multiple_of(KB * lax.rem(r, 2) + t * KT, KT)
        kv = jnp.concatenate([DKVB[0], DKVB[1]], axis=1)
        return dot(XS[ck, :, pl.ds(off, KT)], kv, 0, 0)

    KH = KB // 2

    def dwkv_early():
        def body(t, _):
            KS[0, pl.ds(mul(t, KT), KT), :] = dwkv_tile(seq(2), t).astype(BF16)
            return 0
        lax.fori_loop(0, KB // KT, body, 0)
        rc(KS.at[0, pl.ds(0, KH)], KR.at[0, pl.ds(0, KH)], dks.at[0], dkr.at[0], YU).start()
        rc(KS.at[0, pl.ds(KH, KH)], KR.at[0, pl.ds(KH, KH)], dks.at[0], dkr.at[1], YD).start()

    def dwkv_mid():
        for n, (j, dev) in enumerate(((1, YU), (-1, YD))):
            def body(t, _):
                KS[n + 1, pl.ds(mul(t, KT), KT), :] = dwkv_tile(seq(j), t).astype(BF16)
                return 0
            lax.fori_loop(0, KB // KT, body, 0)
        for n, (j, dev) in enumerate(((1, YU), (-1, YD))):
            half = pl.ds(n * KH, KH)
            wait_recv(KR.at[0, half], dkr.at[n])
            KS[n + 1, half, :] = (KS[n + 1, half, :].astype(F32) + KR[0, half, :].astype(F32)).astype(BF16)
            rc(KS.at[n + 1], KR.at[n + 1], dks.at[n + 1], dkr.at[n + 2], dev).start()

    def dwkv_final():
        for n in range(2):
            wait_recv(KR.at[n + 1], dkr.at[n + 2])

        def body(t, _):
            rows = pl.ds(mul(t, KT), KT)
            v = dwkv_tile(y, t) + KR[1, rows, :].astype(F32) + KR[2, rows, :].astype(F32)
            KOUT[0, rows, :] = v[:, :E]
            KOUT[1, rows, :] = v[:, E:]
            return 0
        lax.fori_loop(0, KB // KT, body, 0)
        for i, ref in enumerate((dwk_ref, dwv_ref)):
            pltpu.make_async_copy(KOUT.at[i], ref, lout.at[i]).start()

    def dwkv_out_wait():
        for i, ref in enumerate((dwk_ref, dwv_ref)):
            pltpu.make_async_copy(KOUT.at[i], ref, lout.at[i]).wait()

    NT = tile_of(CW, 256)

    def dxc(k):
        wq_cp(k).wait()
        for cp in wkv_cp(k):
            cp.wait()

        def body(t, _):
            off = pl.multiple_of(t * NT, NT)
            rows = pl.ds(off, NT)
            v = dot(DKVB[h], WKV[h, rows, :], 1, 1)
            for p in range(NP):
                w = jnp.concatenate([WQ[2 * p, rows, :], WQ[2 * p + 1, rows, :]], axis=1)
                v = v + dot(DQA[p, y], w, 1, 1)
            lo, hi = v[:HR], v[HR:]
            MY[k, :, pl.ds(off, NT)] = jnp.where(h == 0, lo, hi)
            DYS[k, pl.ds(HR, HR), pl.ds(off, NT)] = jnp.where(h == 0, hi, lo).astype(BF16)
            return 0
        lax.fori_loop(0, CW // NT, body, 0)
        if k + 1 < NY:
            wq_cp(k + 1).start()
            for cp in wkv_cp(k + 1):
                cp.start()
        rc(DYS.at[k, pl.ds(HR, HR)], DYS.at[k, pl.ds(0, HR)], pxs.at[k], pxr.at[k], PT).start()

    def blk(k, cc, o, n):
        rows = pl.ds(pl.multiple_of(cc * T + o, TH), n)
        return MY[k, rows, :] + DYS[k, rows, :].astype(F32)

    def rs1(k):
        wait_recv(DYS.at[k, pl.ds(0, HR)], pxr.at[k])
        SX[k, 0:T, :] = blk(k, chip(2), 0, T).astype(BF16)
        s, d = SX.at[k, pl.ds(0, TH)], RX.at[k, pl.ds(0, TH)]
        rc(s, d, rss.at[k], rsr.at[k, 0], XR).start()
        s, d = SX.at[k, pl.ds(TH, TH)], RX.at[k, pl.ds(TH, TH)]
        rc(s, d, rss.at[k], rsr.at[k, 1], XL).start()

    def rs2(k):
        wait_recv(RX.at[k, pl.ds(0, TH)], rsr.at[k, 0])
        SX[k, T:T + TH, :] = (blk(k, chip(1), 0, TH) + RX[k, 0:TH, :].astype(F32)).astype(BF16)
        SX[k, T + TH:2 * T, :] = blk(k, chip(1), TH, TH).astype(BF16)
        s, d = SX.at[k, pl.ds(T, T)], RX.at[k, pl.ds(T, T)]
        rc(s, d, rss.at[k], rsr.at[k, 2], XR).start()
        wait_recv(RX.at[k, pl.ds(TH, TH)], rsr.at[k, 1])
        SX[k, 2 * T:2 * T + TH, :] = blk(k, chip(-1), 0, TH).astype(BF16)
        SX[k, 2 * T + TH:3 * T, :] = (blk(k, chip(-1), TH, TH) + RX[k, TH:T, :].astype(F32)).astype(BF16)
        s, d = SX.at[k, pl.ds(2 * T, T)], RX.at[k, pl.ds(2 * T, T)]
        rc(s, d, rss.at[k], rsr.at[k, 3], XL).start()

    def dx_out(k):
        return pltpu.make_async_copy(DXO.at[k], dx_ref.at[:, pl.ds(k * CW, CW)], lout.at[2 + k])

    def rs3(k):
        wait_recv(RX.at[k, pl.ds(T, T)], rsr.at[k, 2])
        wait_recv(RX.at[k, pl.ds(2 * T, T)], rsr.at[k, 3])
        v = blk(k, c, 0, T) + RX[k, T:2 * T, :].astype(F32) + RX[k, 2 * T:3 * T, :].astype(F32)
        DXO[k] = v.astype(BF16)
        dx_out(k).start()

    def dwo_out(p):
        return pltpu.make_async_copy(OWO, dwo_ref.at[pl.ds(2 * p, 2)], lout.at[2 + NY])

    def dwq_out(p):
        return pltpu.make_async_copy(OWQ, dwq_ref.at[pl.ds(2 * p, 2)], lout.at[3 + NY])

    OT = tile_of(CW, 512)

    def dwo(p):
        yopp(p)
        if p:
            dwo_out(p - 1).wait()

        def body(t, _):
            cols = pl.ds(pl.multiple_of(t * OT, OT), OT)
            v = dot(OA[p, 0], DYC[0, :, cols], 0, 0)
            for s in range(1, NY):
                v = v + dot(OA[p, s], DYC[s, :, cols], 0, 0)
            OWO[0, :, cols] = v[:E]
            OWO[1, :, cols] = v[E:]
            return 0
        lax.fori_loop(0, CW // OT, body, 0)
        dwo_out(p).start()

    def dwq(p):
        yopp(NP + p)
        if p:
            dwq_out(p - 1).wait()

        def body(t, _):
            cols = pl.ds(pl.multiple_of(t * NT, NT), NT)
            v = dot(XC[0, :, cols], DQA[p, 0], 0, 0)
            for s in range(1, NY):
                v = v + dot(XC[s, :, cols], DQA[p, s], 0, 0)
            OWQ[0, cols, :] = v[:, :E]
            OWQ[1, cols, :] = v[:, E:]
            return 0
        lax.fori_loop(0, CW // NT, body, 0)
        dwq_out(p).start()

    def own_cols(dst, src):
        def body(t, _):
            rows = pl.ds(pl.multiple_of(t * T, T), T)
            dst[y, rows, :] = src[y, rows, :]
            return 0
        lax.fori_loop(0, R // T, body, 0)

    own(0)
    own(1)
    rc(XS.at[seq(2), pl.ds(my_rows, T)], XC.at[y, pl.ds(my_rows, T)], a2as.at[0], a2ar.at[3], at(2, 0)).start()
    for cp in ldc:
        cp.wait()
    for j in range(1, NY):
        rc(DYS.at[seq(j), pl.ds(my_rows, T)], DYC.at[y, pl.ds(my_rows, T)],
           a2as.at[1], a2ar.at[NY - j - 1], at(j, 0)).start()

    def compute(i):
        if i < NY:
            if i < 2:
                xc_send(i)
            proj_x(i)
            if i == 3:
                copy_acc(QB)
                KV[0] = KVACC[:, :E].astype(BF16)
                KV[1] = KVACC[:, E:].astype(BF16)
                for p in range(NP):
                    attn_fwd(p)
                    yown(p)
                own_cols(XC, XS)
        elif i < 8:
            proj_dy(i - NY)
            if i == 5:
                xc_fwd(0)
            if i == 6:
                xc_fwd(1)
                yfwd(0)
            if i == 7:
                copy_acc(DOB)
                own_cols(DYC, DYS)
                KVACC[...] = jnp.zeros_like(KVACC)
                attn_bwd(0)
                yown(NP)
                yfwd(1)
        elif i == 8:
            attn_bwd(1)
            yown(NP + 1)
            attn_bwd(2)
            yown(NP + 2)
            for k in range(NY):
                ag_sent(NY + k)
            wait_send(DYS.at[0, pl.ds(0, 3 * T)], a2as.at[1])
            dkv_send()
            yfwd(2)
        elif i == 9:
            dkv_sum()
            dxc(0)
            dwkv_early()
            dxc(1)
        elif i == 10:
            dxc(2)
            rs1(0)
            dxc(3)
            rs1(1)
            yfwd(NP)

    for i in range(N_IT + 1):
        if i < N_IT:
            fwd(i)
        if i + 2 < N_IT:
            own(i + 2)
        if i >= 1:
            opp(i - 1)
            if i - 1 < 2 * NY:
                fin(i - 1)
            compute(i - 1)

    rs1(2)
    rs1(3)
    yfwd(NP + 1)
    dwkv_mid()
    yfwd(NP + 2)
    for i in range(2 * NY, 2 * NY + 3):
        fin(i)
    rs2(0)
    dwo(0)
    rs2(1)
    dwo(1)
    rs2(2)
    dwo(2)
    rs2(3)
    xc_fin(0)
    xc_fin(1)
    fin(N_IT - 1)
    dwq(0)
    rs3(0)
    dwq(1)
    rs3(1)
    dwq(2)
    rs3(2)
    dwkv_final()
    rs3(3)

    for i in list(range(NY)) + list(range(2 * NY, N_IT)):
        ag_sent(i)
    wait_send(XS.at[0, pl.ds(0, T)], a2as.at[0])
    for n in range(4):
        wait_send(XC.at[0, par], xcs.at[n])
    for q in range(2 * NP):
        ysent(q)
    wait_send(KVACC, exs.at[0])
    for n in range(3):
        wait_send(KS.at[n], dks.at[n])
    for k in range(NY):
        wait_send(DYS.at[k, pl.ds(HR, HR)], pxs.at[k])
        wait_send(SX.at[k], rss.at[k])
        dx_out(k).wait()
    dwkv_out_wait()
    dwo_out(NP - 1).wait()
    dwq_out(NP - 1).wait()


def solution(mesh):
    model_size = mesh.shape['model']
    tok_spec = P(('pod', 'data'), 'model', None)

    def device_step(x_loc, dy_loc, w_q, w_k, w_v, w_o):
        T, D = x_loc.shape[1:]
        NH, E = w_q.shape[1:]
        KVH = w_k.shape[0]
        NX = model_size // 2
        NY = mesh.shape['data']
        assert NX == 4 and NY == 4 and KVH == NX and NH == 6
        NP = NH // 2
        CW = D // NY
        R = model_size * T
        KB = CW // 2
        cfg = (T, CW, E, NX, NY, NH)
        V = pltpu.VMEM
        S = pltpu.SemaphoreType.DMA
        n_it = 3 * NY
        scratch = [
            V((NY, R, CW), BF16), V((NY, R, CW), BF16), V((NY, R, CW), BF16), V((NY, R, CW), BF16),
            V((NP, NY, R, 2 * E), BF16), V((NP, NY, R, 2 * E), BF16),
            V((NP, R, 2 * E), BF16), V((NP, R, 2 * E), BF16), V((2, R, E), BF16),
            V((NP, R, 2 * E), F32), V((R, 2 * E), F32), V((R, 2 * E), F32), V((2, R, E), BF16),
            V((NH, CW, E), BF16), V((2, CW, E), BF16), V((NH, E, CW), BF16),
            V((NY, R // 2, CW), F32), V((NY, 3 * T, CW), BF16), V((NY, 3 * T, CW), BF16), V((NY, T, CW), BF16),
            V((NY - 1, KB, 2 * E), BF16), V((NY - 1, KB, 2 * E), BF16), V((2, KB, E), F32),
            V((2, CW, E), F32), V((2, E, CW), F32),
            S((n_it, 5)), S((n_it,)), S((NY,)), S((2,)), S((4,)), S((4,)), S((2 * NP, 4)), S((2 * NP,)),
            S((4,)), S((3,)), S((NY,)), S((NY,)), S((NY, 4)), S((NY,)), S((1,)), S((1,)),
            S((NY,)), S((NY,)), S((1,)), S((2,)), S((1,)), S((4 + NY,)),
        ]
        any_spec = pl.BlockSpec(memory_space=pl.ANY)
        dx, dwq, dwk, dwv, dwo = pl.pallas_call(
            functools.partial(kernel, cfg),
            out_shape=[jax.ShapeDtypeStruct((T, D), BF16), jax.ShapeDtypeStruct((NH, CW, E), F32),
                       jax.ShapeDtypeStruct((KB, E), F32), jax.ShapeDtypeStruct((KB, E), F32),
                       jax.ShapeDtypeStruct((NH, E, CW), F32)],
            in_specs=[any_spec] * 6,
            out_specs=[any_spec] * 5,
            scratch_shapes=scratch,
            compiler_params=pltpu.CompilerParams(collective_id=0, has_side_effects=True, vmem_limit_bytes=VMEM_BYTES),
            name='attn_bwd_fused',
        )(x_loc[0], dy_loc[0], w_q.transpose(1, 0, 2), w_k, w_v, w_o)
        return dx[None], dwq.transpose(1, 0, 2), dwk, dwv, dwo

    kv_rows = P(('pod', 'model', 'data'), None)
    return jax.shard_map(device_step, mesh=mesh,
                         in_specs=(tok_spec, tok_spec, P(None, 'model', None), P(), P(), P('model', None, None)),
                         out_specs=(tok_spec, P(('pod', 'data'), 'model', None), kv_rows, kv_rows, P(('pod', 'model'), None, 'data')),
                         check_vma=False)
```

```python
import functools

import jax
import jax.numpy as jnp
from jax import lax
from jax.experimental import pallas as pl
from jax.experimental.pallas import tpu as pltpu
from jax.sharding import PartitionSpec as P

MESH = pl.DeviceIdType.MESH
F32 = jnp.float32
BF16 = jnp.bfloat16
VMEM_BYTES = 54 * 1000 * 1000
LOG2E = 1.4426950408889634


def dot(a, b, ca, cb):
    return lax.dot_general(a, b, (((ca,), (cb,)), ((), ())), preferred_element_type=F32)


def tile_of(n, t):
    return t if n % t == 0 else n


def kernel(cfg, x_ref, dy_ref, wq_ref, wk_ref, wv_ref, wo_ref,
           dx_ref, dwq_ref, dwk_ref, dwv_ref, dwo_ref,
           XS, DYS, XC, DYC, OA, DQA, QB, DOB, KV, KVACC, DKVR, DKVB,
           WQ, WKV, WO, MY, KS, KR,
           agr, ags, a2ar, a2as, xcr, xcs, yr, ys, dkr, dks, pxr, pxs, rsr, rss, exs, exr,
           lx, ldy, lwq, lwkv, lwo, cred):
    T, CW, E, NX, NY, NH = cfg
    NP = NH // 2
    R = 2 * NX * T
    HR = NX * T
    TH = T // 2
    scale = E ** -0.5
    scale2 = scale * LOG2E
    pod = lax.axis_index('pod')
    y = lax.axis_index('data')
    m = lax.axis_index('model')
    c = lax.div(m, 2)
    h = lax.rem(m, 2)

    def at(dy_, dx_):
        return (pod, lax.rem(y + dy_ + NY, NY), 2 * lax.rem(c + dx_ + NX, NX) + h)

    XR, XL = at(0, 1), at(0, -1)
    YU, YD = at(1, 0), at(-1, 0)
    PT = (pod, y, 2 * c + 1 - h)

    def rc(src, dst, ssem, rsem, dev):
        return pltpu.make_async_remote_copy(src_ref=src, dst_ref=dst, send_sem=ssem, recv_sem=rsem,
                                            device_id=dev, device_id_type=MESH)

    def wait_recv(dst, sem):
        rc(dst, dst, sem, sem, PT).wait_recv()

    def wait_send(src, sem):
        rc(src, src, sem, sem, PT).wait_send()

    def chip(k):
        return lax.rem(c + k + NX, NX)

    def seq(k):
        return lax.rem(y + k + NY, NY)

    def rb(k):
        return pl.multiple_of((h * NX + chip(k)) * T, T)

    my_rows = rb(0)
    def mul(k, n):
        return pl.multiple_of(k * n, n)

    def wq_cp(k):
        return pltpu.make_async_copy(wq_ref.at[:, pl.ds(mul(k, CW), CW), :], WQ, lwq.at[0])

    def wkv_cp(k):
        return [pltpu.make_async_copy(wk_ref.at[c, pl.ds(mul(k, CW), CW)], WKV.at[0], lwkv.at[0]),
                pltpu.make_async_copy(wv_ref.at[c, pl.ds(mul(k, CW), CW)], WKV.at[1], lwkv.at[1])]

    def wo_cp(k):
        return pltpu.make_async_copy(wo_ref.at[:, :, pl.ds(k * CW, CW)], WO, lwo.at[0])

    bar = pltpu.get_barrier_semaphore()
    peers = [XR, XL, PT] + [at(j, 0) for j in range(1, NY)]
    for dev in peers:
        pl.semaphore_signal(bar, inc=1, device_id=dev, device_id_type=MESH)
    x_order = [seq(1), seq(-1), seq(2), y]
    lxc = [pltpu.make_async_copy(x_ref.at[:, pl.ds(k * CW, CW)], XS.at[k, pl.ds(my_rows, T)], lx.at[k]) for k in range(NY)]
    ldc = [pltpu.make_async_copy(dy_ref.at[:, pl.ds(k * CW, CW)], DYS.at[k, pl.ds(my_rows, T)], ldy.at[k]) for k in range(NY)]
    for cp in lxc:
        cp.start()
    for cp in lxc:
        cp.wait()
    for cp in ldc:
        cp.start()
    wq_cp(x_order[0]).start()
    for cp in wkv_cp(x_order[0]):
        cp.start()
    wo_cp(0).start()
    pl.semaphore_wait(bar, len(peers))

    items = ([(XS, k) for k in x_order] + [(DYS, k) for k in range(NY)]
             + [(DYC, seq(j)) for j in range(1, NY)] + [(XC, seq(2))])
    N_IT = len(items)

    def own(i):
        buf, ix = items[i]
        if i >= 2 * NY:
            wait_recv(buf.at[ix, pl.ds(my_rows, T)], a2ar.at[i - 2 * NY])
        blk = buf.at[ix, pl.ds(my_rows, T)]
        rc(blk, blk, ags.at[i], agr.at[i, 0], XR).start()
        rc(blk, blk, ags.at[i], agr.at[i, 1], XL).start()
        rc(blk, blk, ags.at[i], agr.at[i, 4], PT).start()

    def fwd(i):
        buf, ix = items[i]
        lb, rb_ = rb(-1), rb(1)
        blk = buf.at[ix, pl.ds(lb, T)]
        wait_recv(blk, agr.at[i, 0])
        half = buf.at[ix, pl.ds(lb, TH)]
        rc(half, half, ags.at[i], agr.at[i, 2], XR).start()
        rc(blk, blk, ags.at[i], agr.at[i, 4], PT).start()
        blk = buf.at[ix, pl.ds(rb_, T)]
        wait_recv(blk, agr.at[i, 1])
        half = buf.at[ix, pl.ds(pl.multiple_of(rb_ + TH, TH), TH)]
        rc(half, half, ags.at[i], agr.at[i, 3], XL).start()
        rc(blk, blk, ags.at[i], agr.at[i, 4], PT).start()

    def opp(i):
        buf, ix = items[i]
        ob = rb(2)
        wait_recv(buf.at[ix, pl.ds(ob, TH)], agr.at[i, 2])
        wait_recv(buf.at[ix, pl.ds(pl.multiple_of(ob + TH, TH), TH)], agr.at[i, 3])
        blk = buf.at[ix, pl.ds(ob, T)]
        rc(blk, blk, ags.at[i], agr.at[i, 4], PT).start()

    def fin(i):
        buf, ix = items[i]
        wait_recv(buf.at[ix, pl.ds(pl.multiple_of((1 - h) * HR, HR), HR)], agr.at[i, 4])

    def ag_sent(i):
        buf, ix = items[i]
        wait_send(buf.at[ix, pl.ds(0, 7 * T)], ags.at[i])

    par = pl.ds(mul(h, HR), HR)

    def xc_send(n):
        rc(XS.at[x_order[n], par], XC.at[y, par], xcs.at[n], xcr.at[n], (YU, YD)[n]).start()

    def xc_fwd(n):
        b = XC.at[seq((-1, 1)[n]), par]
        wait_recv(b, xcr.at[n])
        rc(b, b, xcs.at[2 + n], xcr.at[2 + n], PT).start()

    def xc_fin(n):
        wait_recv(XC.at[seq((-1, 1)[n]), pl.ds(mul(1 - h, HR), HR)], xcr.at[2 + n])

    def ybuf(q):
        return (OA if q < NP else DQA).at[q % NP]

    def yown(q):
        b = ybuf(q).at[y]
        rc(b, b, ys.at[q], yr.at[q, 0], YU).start()
        rc(b, b, ys.at[q], yr.at[q, 1], YD).start()

    def yfwd(q):
        b = ybuf(q)
        wait_recv(b.at[seq(-1)], yr.at[q, 0])
        half = b.at[seq(-1), pl.ds(0, HR)]
        rc(half, half, ys.at[q], yr.at[q, 2], YU).start()
        wait_recv(b.at[seq(1)], yr.at[q, 1])
        half = b.at[seq(1), pl.ds(HR, HR)]
        rc(half, half, ys.at[q], yr.at[q, 3], YD).start()

    def yopp(q):
        b = ybuf(q)
        wait_recv(b.at[seq(2), pl.ds(0, HR)], yr.at[q, 2])
        wait_recv(b.at[seq(2), pl.ds(HR, HR)], yr.at[q, 3])

    def ysent(q):
        wait_send(ybuf(q).at[pl.ds(0, 3)], ys.at[q])

    def acc(p, d, first):
        cols = pl.ds(mul(p, 2 * E), 2 * E)
        MY[0, :, cols] = d[:HR] if first else MY[0, :, cols] + d[:HR]
        MY[1, :, cols] = d[HR:] if first else MY[1, :, cols] + d[HR:]

    def proj_x(i):
        k = x_order[i]
        wq_cp(k).wait()
        for cp in wkv_cp(k):
            cp.wait()

        def body(p, _):
            w = jnp.concatenate([WQ[2 * p], WQ[2 * p + 1]], axis=1)
            acc(p, dot(XS[k], w, 1, 0), i == 0)
            return 0
        lax.fori_loop(0, NP, body, 0)
        d = dot(XS[k], jnp.concatenate([WKV[0], WKV[1]], axis=1), 1, 0)
        KVACC[...] = d if i == 0 else KVACC[...] + d
        nk = x_order[i + 1] if i + 1 < NY else 0
        wq_cp(nk).start()
        for cp in wkv_cp(nk):
            cp.start()

    def proj_dy(k):
        wo_cp(k).wait()

        def body(p, _):
            w = WO[pl.ds(2 * p, 2)].reshape(2 * E, CW)
            acc(p, dot(DYS[k], w, 1, 1), k == 0)
            return 0
        lax.fori_loop(0, NP, body, 0)
        if k + 1 < NY:
            wo_cp(k + 1).start()

    def copy_acc(dst):
        def body(p, _):
            cols = pl.ds(mul(p, 2 * E), 2 * E)
            dst[p, 0:HR, :] = MY[0, :, cols].astype(BF16)
            dst[p, HR:R, :] = MY[1, :, cols].astype(BF16)
            return 0
        lax.fori_loop(0, NP, body, 0)

    T2 = 2 * T

    def pos(i):
        g = lax.div(i, T)
        return (2 * lax.rem(g, NX) + lax.div(g, NX)) * T + lax.rem(i, T)

    def brow(i, g):
        return lax.div(i, T2) * HR + g * T2 + lax.rem(i, T2)

    def pick(load, g):
        return jnp.concatenate([load(slice(g * T2, g * T2 + T2)), load(slice(HR + g * T2, HR + g * T2 + T2))], axis=0)

    def put(store, g, v):
        store(slice(g * T2, g * T2 + T2), v[:T2])
        store(slice(HR + g * T2, HR + g * T2 + T2), v[T2:])

    def keys(t, g):
        return pick(lambda r: KV[t, r, :], 0) if g == 0 else KV[t]

    def probs(q, g):
        s = dot(q, keys(0, g), 1, 1) * scale2
        n = s.shape[1]
        qp = pos(brow(lax.broadcasted_iota(jnp.int32, (HR, 1), 0), g))
        kp = lax.broadcasted_iota(jnp.int32, (1, n), 1)
        kp = pos(brow(kp, 0) if g == 0 else kp)
        s = jnp.where(qp >= kp, s, -jnp.inf)
        e = jnp.exp2(s - jnp.max(s, axis=1, keepdims=True))
        return e * (1.0 / jnp.sum(e, axis=1, keepdims=True))

    def attn_fwd(p):
        for g in range(2):
            for a in range(2):
                ln = slice(a * E, (a + 1) * E)
                pr = probs(pick(lambda r: QB[p, r, ln], g), g)
                o = dot(pr.astype(BF16), keys(1, g), 1, 0).astype(BF16)

                def store(r, v):
                    OA[p, y, r, ln] = v
                put(store, g, o)

    def attn_bwd(p):
        for g in range(2):
            for a in range(2):
                ln = slice(a * E, (a + 1) * E)
                q = pick(lambda r: QB[p, r, ln], g)
                do = pick(lambda r: DOB[p, r, ln], g)
                o = pick(lambda r: OA[p, y, r, ln], g)
                pr = probs(q, g)
                delta = jnp.sum(do.astype(F32) * o.astype(F32), axis=1, keepdims=True)
                dp = dot(do, keys(1, g), 1, 1)
                ds = (pr * (dp - delta)).astype(BF16)
                dq = (dot(ds, keys(0, g), 1, 0) * scale).astype(BF16)
                dkv = jnp.concatenate([dot(ds, q, 0, 0), dot(pr.astype(BF16), do, 0, 0)], axis=1)

                def store(r, v):
                    DQA[p, y, r, ln] = v
                put(store, g, dq)
                if g == 0:
                    def add(r, v):
                        KVACC[r, :] = KVACC[r, :] + v
                    put(add, 0, dkv)
                else:
                    KVACC[...] = KVACC[...] + dkv

    def dkv_send():
        KVACC[:, :E] = KVACC[:, :E] * scale
        rc(KVACC, DKVR, exs.at[0], exr.at[0], PT).start()

    def dkv_sum():
        wait_recv(DKVR, exr.at[0])
        tot = (KVACC[...] + DKVR[...]).astype(BF16)
        DKVB[0] = tot[:, :E]
        DKVB[1] = tot[:, E:]

    KB = CW // 2
    KT = tile_of(KB, 256)

    def dwkv_tile(r, t):
        ck = 2 * h + lax.div(r, 2)
        off = pl.multiple_of(KB * lax.rem(r, 2) + t * KT, KT)
        kv = jnp.concatenate([DKVB[0], DKVB[1]], axis=1)
        return dot(XS[ck, :, pl.ds(off, KT)], kv, 0, 0)

    KH = KB // 2

    def dwkv_early():
        def body(t, _):
            KS[0, pl.ds(mul(t, KT), KT), :] = dwkv_tile(seq(2), t).astype(BF16)
            return 0
        lax.fori_loop(0, KB // KT, body, 0)
        rc(KS.at[0, pl.ds(0, KH)], KR.at[0, pl.ds(0, KH)], dks.at[0], dkr.at[0], YU).start()
        rc(KS.at[0, pl.ds(KH, KH)], KR.at[0, pl.ds(KH, KH)], dks.at[0], dkr.at[1], YD).start()

    def dwkv_part(n):
        def body(t, _):
            KS[n + 1, pl.ds(mul(t, KT), KT), :] = dwkv_tile(seq((1, -1)[n]), t).astype(BF16)
            return 0
        lax.fori_loop(0, KB // KT, body, 0)

    def dwkv_own():
        def body(t, _):
            rows = pl.ds(mul(t, KT), KT)
            v = dwkv_tile(y, t)
            dwk_ref[rows, :] = v[:, :E]
            dwv_ref[rows, :] = v[:, E:]
            return 0
        lax.fori_loop(0, KB // KT, body, 0)

    def dwkv_mid():
        for n, dev in enumerate((YU, YD)):
            half = pl.ds(n * KH, KH)
            wait_recv(KR.at[0, half], dkr.at[n])
            KS[n + 1, half, :] = (KS[n + 1, half, :].astype(F32) + KR[0, half, :].astype(F32)).astype(BF16)
            rc(KS.at[n + 1], KR.at[n + 1], dks.at[n + 1], dkr.at[n + 2], dev).start()

    def dwkv_final():
        for n in range(2):
            wait_recv(KR.at[n + 1], dkr.at[n + 2])

        def body(t, _):
            rows = pl.ds(mul(t, KT), KT)
            v = KR[1, rows, :].astype(F32) + KR[2, rows, :].astype(F32)
            dwk_ref[rows, :] = dwk_ref[rows, :] + v[:, :E]
            dwv_ref[rows, :] = dwv_ref[rows, :] + v[:, E:]
            return 0
        lax.fori_loop(0, KB // KT, body, 0)

    def x_free():
        for i in range(NY):
            ag_sent(i)
        wait_send(XS.at[0, pl.ds(0, T)], a2as.at[0])
        for n in range(2):
            wait_send(XS.at[0, par], xcs.at[n])
        for dev in (XL, XR):
            pl.semaphore_signal(cred, inc=1, device_id=dev, device_id_type=MESH)

    NT = tile_of(CW, 256)

    def dxc(k):
        wq_cp(k).wait()
        for cp in wkv_cp(k):
            cp.wait()

        def body(t, _):
            off = pl.multiple_of(t * NT, NT)
            rows = pl.ds(off, NT)
            w = jnp.concatenate([WQ[i, rows, :] for i in range(NH)] + [WKV[h, rows, :]], axis=1)
            v = dot(jnp.concatenate([DQA[p, y] for p in range(NP)] + [DKVB[h]], axis=1), w, 1, 1)
            lo, hi = v[:HR], v[HR:]
            MY[k, :, pl.ds(off, NT)] = jnp.where(h == 0, lo, hi)
            DYS[k, pl.ds(HR, HR), pl.ds(off, NT)] = jnp.where(h == 0, hi, lo).astype(BF16)
            return 0
        lax.fori_loop(0, CW // NT, body, 0)
        if k + 1 < NY:
            wq_cp(k + 1).start()
            for cp in wkv_cp(k + 1):
                cp.start()
        rc(DYS.at[k, pl.ds(HR, HR)], DYS.at[k, pl.ds(0, HR)], pxs.at[k], pxr.at[k], PT).start()

    RO = 3 * T

    def blk(k, cc, o, n):
        rows = pl.ds(pl.multiple_of(cc * T + o, TH), n)
        return MY[k, rows, :] + DYS[k, rows, :].astype(F32)

    def rs1(k):
        wait_recv(DYS.at[k, pl.ds(0, HR)], pxr.at[k])
        XS[k, 0:T, :] = blk(k, chip(2), 0, T).astype(BF16)
        s, d = XS.at[k, pl.ds(0, TH)], XS.at[k, pl.ds(RO + 0, TH)]
        rc(s, d, rss.at[k], rsr.at[k, 0], XR).start()
        s, d = XS.at[k, pl.ds(TH, TH)], XS.at[k, pl.ds(RO + TH, TH)]
        rc(s, d, rss.at[k], rsr.at[k, 1], XL).start()

    def rs2(k):
        wait_recv(XS.at[k, pl.ds(RO + 0, TH)], rsr.at[k, 0])
        XS[k, T:T + TH, :] = (blk(k, chip(1), 0, TH) + XS[k, RO + 0:RO + TH, :].astype(F32)).astype(BF16)
        XS[k, T + TH:2 * T, :] = blk(k, chip(1), TH, TH).astype(BF16)
        s, d = XS.at[k, pl.ds(T, T)], XS.at[k, pl.ds(RO + T, T)]
        rc(s, d, rss.at[k], rsr.at[k, 2], XR).start()
        wait_recv(XS.at[k, pl.ds(RO + TH, TH)], rsr.at[k, 1])
        XS[k, 2 * T:2 * T + TH, :] = blk(k, chip(-1), 0, TH).astype(BF16)
        XS[k, 2 * T + TH:3 * T, :] = (blk(k, chip(-1), TH, TH) + XS[k, RO + TH:RO + T, :].astype(F32)).astype(BF16)
        s, d = XS.at[k, pl.ds(2 * T, T)], XS.at[k, pl.ds(RO + 2 * T, T)]
        rc(s, d, rss.at[k], rsr.at[k, 3], XL).start()

    def rs3(k):
        wait_recv(XS.at[k, pl.ds(RO + T, T)], rsr.at[k, 2])
        wait_recv(XS.at[k, pl.ds(RO + 2 * T, T)], rsr.at[k, 3])
        v = blk(k, c, 0, T) + XS[k, RO + T:RO + 2 * T, :].astype(F32) + XS[k, RO + 2 * T:RO + 3 * T, :].astype(F32)
        dx_ref[:, k * CW:(k + 1) * CW] = v.astype(BF16)

    OT = tile_of(CW, 512)

    def dwo(p):
        def body(t, _):
            cols = pl.ds(mul(t, OT), OT)
            v = dot(OA[p].reshape(NY * R, 2 * E), DYC[:, :, cols].reshape(NY * R, OT), 0, 0)
            dwo_ref[2 * p, :, cols] = v[:E]
            dwo_ref[2 * p + 1, :, cols] = v[E:]
            return 0
        lax.fori_loop(0, CW // OT, body, 0)

    def dwq(p):
        def body(t, _):
            cols = pl.ds(mul(t, OT), OT)
            v = dot(XC[:, :, cols].reshape(NY * R, OT), DQA[p].reshape(NY * R, 2 * E), 0, 0)
            dwq_ref[2 * p, cols, :] = v[:, :E]
            dwq_ref[2 * p + 1, cols, :] = v[:, E:]
            return 0
        lax.fori_loop(0, CW // OT, body, 0)

    def own_cols(dst, src):
        def body(t, _):
            rows = pl.ds(pl.multiple_of(t * T, T), T)
            dst[y, rows, :] = src[y, rows, :]
            return 0
        lax.fori_loop(0, R // T, body, 0)

    own(0)
    own(1)
    rc(XS.at[seq(2), pl.ds(my_rows, T)], XC.at[y, pl.ds(my_rows, T)], a2as.at[0], a2ar.at[3], at(2, 0)).start()
    for cp in ldc:
        cp.wait()
    for j in range(1, NY):
        rc(DYS.at[seq(j), pl.ds(my_rows, T)], DYC.at[y, pl.ds(my_rows, T)],
           a2as.at[1], a2ar.at[NY - j - 1], at(j, 0)).start()

    def compute(i):
        if i < NY:
            if i < 2:
                xc_send(i)
            proj_x(i)
            if i == 3:
                copy_acc(QB)
                KV[0] = KVACC[:, :E].astype(BF16)
                KV[1] = KVACC[:, E:].astype(BF16)
                for p in range(NP):
                    attn_fwd(p)
                    yown(p)
                own_cols(XC, XS)
        elif i < 8:
            proj_dy(i - NY)
            if i == 5:
                xc_fwd(0)
            if i == 6:
                xc_fwd(1)
                yfwd(0)
            if i == 7:
                copy_acc(DOB)
                own_cols(DYC, DYS)
                KVACC[...] = jnp.zeros_like(KVACC)

    for i in range(9):
        fwd(i)
        for n in range(i + 2, N_IT if i == 7 else i + 3):
            if n < N_IT and i <= 7:
                own(n)
        if i >= 1:
            opp(i - 1)
            fin(i - 1)
            compute(i - 1)

    attn_bwd(0)
    yown(NP)
    fwd(9)
    yfwd(1)
    attn_bwd(1)
    yown(NP + 1)
    fwd(10)
    attn_bwd(2)
    yown(NP + 2)
    for k in range(NY):
        ag_sent(NY + k)
    wait_send(DYS.at[0, pl.ds(0, 3 * T)], a2as.at[1])
    dkv_send()
    yfwd(2)
    opp(8)
    dkv_sum()
    dwkv_early()
    dxc(0)
    fwd(11)
    dwkv_part(0)
    dwkv_part(1)
    dwkv_own()
    x_free()
    yfwd(NP)
    opp(9)
    dxc(1)
    pl.semaphore_wait(cred, 2)
    rs1(0)
    opp(10)
    yfwd(NP + 1)
    dxc(2)
    rs1(1)
    opp(11)
    dxc(3)
    rs1(2)
    rs1(3)
    yfwd(NP + 2)
    rs2(0)
    dwkv_mid()
    for i in range(2 * NY, N_IT):
        fin(i)
    for p in range(NP):
        yopp(p)
    dwo(0)
    rs2(1)
    dwo(1)
    rs2(2)
    dwo(2)
    rs2(3)
    for n in range(2):
        xc_fin(n)
    for p in range(NP):
        yopp(NP + p)
    dwq(0)
    rs3(0)
    dwq(1)
    rs3(1)
    dwq(2)
    rs3(2)
    dwkv_final()
    rs3(3)

    for i in range(2 * NY, N_IT):
        ag_sent(i)
    for n in range(2):
        wait_send(XC.at[0, par], xcs.at[2 + n])
    for q in range(2 * NP):
        ysent(q)
    wait_send(KVACC, exs.at[0])
    for n in range(3):
        wait_send(KS.at[n], dks.at[n])
    for k in range(NY):
        wait_send(DYS.at[k, pl.ds(HR, HR)], pxs.at[k])
        wait_send(XS.at[k, pl.ds(0, 3 * T)], rss.at[k])


def solution(mesh):
    model_size = mesh.shape['model']
    tok_spec = P(('pod', 'data'), 'model', None)

    def device_step(x_loc, dy_loc, w_q, w_k, w_v, w_o):
        T, D = x_loc.shape[1:]
        NH, E = w_q.shape[1:]
        KVH = w_k.shape[0]
        NX = model_size // 2
        NY = mesh.shape['data']
        assert NX == 4 and NY == 4 and KVH == NX and NH == 6
        NP = NH // 2
        CW = D // NY
        R = model_size * T
        KB = CW // 2
        cfg = (T, CW, E, NX, NY, NH)
        V = pltpu.VMEM
        S = pltpu.SemaphoreType.DMA
        n_it = 3 * NY
        scratch = [
            V((NY, R, CW), BF16), V((NY, R, CW), BF16), V((NY, R, CW), BF16), V((NY, R, CW), BF16),
            V((NP, NY, R, 2 * E), BF16), V((NP, NY, R, 2 * E), BF16),
            V((NP, R, 2 * E), BF16), V((NP, R, 2 * E), BF16), V((2, R, E), BF16),
            V((R, 2 * E), F32), V((R, 2 * E), F32), V((2, R, E), BF16),
            V((NH, CW, E), BF16), V((2, CW, E), BF16), V((NH, E, CW), BF16),
            V((NY, R // 2, CW), F32), V((NY - 1, KB, 2 * E), BF16), V((NY - 1, KB, 2 * E), BF16),
            S((n_it, 5)), S((n_it,)), S((NY,)), S((2,)), S((4,)), S((4,)), S((2 * NP, 4)), S((2 * NP,)),
            S((4,)), S((3,)), S((NY,)), S((NY,)), S((NY, 4)), S((NY,)), S((1,)), S((1,)),
            S((NY,)), S((NY,)), S((1,)), S((2,)), S((1,)), pltpu.SemaphoreType.REGULAR,
        ]
        any_spec = pl.BlockSpec(memory_space=pl.ANY)
        dx, dwq, dwk, dwv, dwo = pl.pallas_call(
            functools.partial(kernel, cfg),
            out_shape=[V((T, D), BF16), V((NH, CW, E), F32), V((KB, E), F32), V((KB, E), F32), V((NH, E, CW), F32)],
            in_specs=[any_spec] * 6,
            out_specs=[pl.BlockSpec(memory_space=V)] * 5,
            scratch_shapes=scratch,
            compiler_params=pltpu.CompilerParams(collective_id=0, has_side_effects=True, vmem_limit_bytes=VMEM_BYTES),
            name='attn_bwd_fused',
        )(x_loc[0], dy_loc[0], w_q.transpose(1, 0, 2), w_k, w_v, w_o)
        return dx[None], dwq.transpose(1, 0, 2), dwk, dwv, dwo

    kv_rows = P(('pod', 'model', 'data'), None)
    return jax.shard_map(device_step, mesh=mesh,
                         in_specs=(tok_spec, tok_spec, P(None, 'model', None), P(), P(), P('model', None, None)),
                         out_specs=(tok_spec, P(('pod', 'data'), 'model', None), kv_rows, kv_rows, P(('pod', 'model'), None, 'data')),
                         check_vma=False)
```

```python
import functools

import jax
import jax.numpy as jnp
from jax import lax
from jax.experimental import pallas as pl
from jax.experimental.pallas import tpu as pltpu
from jax.sharding import PartitionSpec as P

MESH = pl.DeviceIdType.MESH
F32 = jnp.float32
BF16 = jnp.bfloat16
VMEM_BYTES = 54 * 1000 * 1000
DXT = 384
OUT_IN = pl.ANY
OUT_LIM = 1024 * 1024
LOG2E = 1.4426950408889634


def dot(a, b, ca, cb):
    return lax.dot_general(a, b, (((ca,), (cb,)), ((), ())), preferred_element_type=F32)


def tile_of(n, t):
    return t if n % t == 0 else n


def kernel(cfg, x_ref, dy_ref, wq_ref, wk_ref, wv_ref, wo_ref,
           dx_ref, dwq_ref, dwk_ref, dwv_ref, dwo_ref,
           XS, DYS, XC, DYC, OA, DQA, QB, DOB, KV, KVACC, DKVR, DKVB,
           WQ, WKV, WO, MY, SX, KS, KR,
           agr, ags, a2ar, a2as, xcr, xcs, yr, ys, dkr, dks, pxr, pxs, rsr, rss, exs, exr,
           lx, ldy, lwq, lwkv, lwo, cred):
    T, CW, E, NX, NY, NH = cfg
    NP = NH // 2
    R = 2 * NX * T
    HR = NX * T
    TH = T // 2
    scale = E ** -0.5
    scale2 = scale * LOG2E
    pod = lax.axis_index('pod')
    y = lax.axis_index('data')
    m = lax.axis_index('model')
    c = lax.div(m, 2)
    h = lax.rem(m, 2)

    def at(dy_, dx_):
        return (pod, lax.rem(y + dy_ + NY, NY), 2 * lax.rem(c + dx_ + NX, NX) + h)

    XR, XL = at(0, 1), at(0, -1)
    YU, YD = at(1, 0), at(-1, 0)
    PT = (pod, y, 2 * c + 1 - h)

    def rc(src, dst, ssem, rsem, dev):
        return pltpu.make_async_remote_copy(src_ref=src, dst_ref=dst, send_sem=ssem, recv_sem=rsem,
                                            device_id=dev, device_id_type=MESH)

    def wait_recv(dst, sem):
        rc(dst, dst, sem, sem, PT).wait_recv()

    def wait_send(src, sem):
        rc(src, src, sem, sem, PT).wait_send()

    def chip(k):
        return lax.rem(c + k + NX, NX)

    def seq(k):
        return lax.rem(y + k + NY, NY)

    def rb(k):
        return pl.multiple_of((h * NX + chip(k)) * T, T)

    my_rows = rb(0)
    def mul(k, n):
        return pl.multiple_of(k * n, n)

    def wq_cp(k):
        return pltpu.make_async_copy(wq_ref.at[:, pl.ds(mul(k, CW), CW), :], WQ, lwq.at[0])

    def wkv_cp(k):
        return [pltpu.make_async_copy(wk_ref.at[c, pl.ds(mul(k, CW), CW)], WKV.at[0], lwkv.at[0]),
                pltpu.make_async_copy(wv_ref.at[c, pl.ds(mul(k, CW), CW)], WKV.at[1], lwkv.at[1])]

    def wo_cp(k):
        return pltpu.make_async_copy(wo_ref.at[:, :, pl.ds(k * CW, CW)], WO, lwo.at[0])

    bar = pltpu.get_barrier_semaphore()
    peers = [XR, XL, PT] + [at(j, 0) for j in range(1, NY)]
    for dev in peers:
        pl.semaphore_signal(bar, inc=1, device_id=dev, device_id_type=MESH)
    x_order = [seq(1), seq(-1), seq(2), y]
    lxc = [pltpu.make_async_copy(x_ref.at[:, pl.ds(k * CW, CW)], XS.at[k, pl.ds(my_rows, T)], lx.at[k]) for k in range(NY)]
    ldc = [pltpu.make_async_copy(dy_ref.at[:, pl.ds(k * CW, CW)], DYS.at[k, pl.ds(my_rows, T)], ldy.at[k]) for k in range(NY)]
    for cp in lxc:
        cp.start()
    for cp in lxc:
        cp.wait()
    for cp in ldc:
        cp.start()
    wq_cp(x_order[0]).start()
    for cp in wkv_cp(x_order[0]):
        cp.start()
    wo_cp(0).start()
    pl.semaphore_wait(bar, len(peers))

    items = ([(XS, k) for k in x_order] + [(DYS, k) for k in range(NY)]
             + [(DYC, seq(j)) for j in range(1, NY)] + [(XC, seq(2))])
    N_IT = len(items)

    def own(i):
        buf, ix = items[i]
        if i >= 2 * NY:
            wait_recv(buf.at[ix, pl.ds(my_rows, T)], a2ar.at[i - 2 * NY])
        blk = buf.at[ix, pl.ds(my_rows, T)]
        rc(blk, blk, ags.at[i], agr.at[i, 0], XR).start()
        rc(blk, blk, ags.at[i], agr.at[i, 1], XL).start()
        rc(blk, blk, ags.at[i], agr.at[i, 4], PT).start()

    def fwd(i):
        buf, ix = items[i]
        lb, rb_ = rb(-1), rb(1)
        blk = buf.at[ix, pl.ds(lb, T)]
        wait_recv(blk, agr.at[i, 0])
        half = buf.at[ix, pl.ds(lb, TH)]
        rc(half, half, ags.at[i], agr.at[i, 2], XR).start()
        rc(blk, blk, ags.at[i], agr.at[i, 4], PT).start()
        blk = buf.at[ix, pl.ds(rb_, T)]
        wait_recv(blk, agr.at[i, 1])
        half = buf.at[ix, pl.ds(pl.multiple_of(rb_ + TH, TH), TH)]
        rc(half, half, ags.at[i], agr.at[i, 3], XL).start()
        rc(blk, blk, ags.at[i], agr.at[i, 4], PT).start()

    def opp(i):
        buf, ix = items[i]
        ob = rb(2)
        wait_recv(buf.at[ix, pl.ds(ob, TH)], agr.at[i, 2])
        wait_recv(buf.at[ix, pl.ds(pl.multiple_of(ob + TH, TH), TH)], agr.at[i, 3])
        blk = buf.at[ix, pl.ds(ob, T)]
        rc(blk, blk, ags.at[i], agr.at[i, 4], PT).start()

    def fin(i):
        buf, ix = items[i]
        wait_recv(buf.at[ix, pl.ds(pl.multiple_of((1 - h) * HR, HR), HR)], agr.at[i, 4])

    def ag_sent(i):
        buf, ix = items[i]
        wait_send(buf.at[ix, pl.ds(0, 7 * T)], ags.at[i])

    par = pl.ds(mul(h, HR), HR)

    def xc_send(n):
        rc(XS.at[x_order[n], par], XC.at[y, par], xcs.at[n], xcr.at[n], (YU, YD)[n]).start()

    def xc_fwd(n):
        b = XC.at[seq((-1, 1)[n]), par]
        wait_recv(b, xcr.at[n])
        rc(b, b, xcs.at[2 + n], xcr.at[2 + n], PT).start()

    def xc_fin(n):
        wait_recv(XC.at[seq((-1, 1)[n]), pl.ds(mul(1 - h, HR), HR)], xcr.at[2 + n])

    def ybuf(q):
        return (OA if q < NP else DQA).at[q % NP]

    def yown(q):
        b = ybuf(q).at[y]
        rc(b, b, ys.at[q], yr.at[q, 0], YU).start()
        rc(b, b, ys.at[q], yr.at[q, 1], YD).start()

    def yfwd(q):
        b = ybuf(q)
        wait_recv(b.at[seq(-1)], yr.at[q, 0])
        half = b.at[seq(-1), pl.ds(0, HR)]
        rc(half, half, ys.at[q], yr.at[q, 2], YU).start()
        wait_recv(b.at[seq(1)], yr.at[q, 1])
        half = b.at[seq(1), pl.ds(HR, HR)]
        rc(half, half, ys.at[q], yr.at[q, 3], YD).start()

    def yopp(q):
        b = ybuf(q)
        wait_recv(b.at[seq(2), pl.ds(0, HR)], yr.at[q, 2])
        wait_recv(b.at[seq(2), pl.ds(HR, HR)], yr.at[q, 3])

    def ysent(q):
        wait_send(ybuf(q).at[pl.ds(0, 3)], ys.at[q])

    def acc(p, d, first):
        cols = pl.ds(mul(p, 2 * E), 2 * E)
        MY[0, :, cols] = d[:HR] if first else MY[0, :, cols] + d[:HR]
        MY[1, :, cols] = d[HR:] if first else MY[1, :, cols] + d[HR:]

    def proj_x(i):
        k = x_order[i]
        wq_cp(k).wait()
        for cp in wkv_cp(k):
            cp.wait()

        def body(p, _):
            w = jnp.concatenate([WQ[2 * p], WQ[2 * p + 1]], axis=1)
            acc(p, dot(XS[k], w, 1, 0), i == 0)
            return 0
        lax.fori_loop(0, NP, body, 0)
        d = dot(XS[k], jnp.concatenate([WKV[0], WKV[1]], axis=1), 1, 0)
        KVACC[...] = d if i == 0 else KVACC[...] + d
        nk = x_order[i + 1] if i + 1 < NY else 0
        wq_cp(nk).start()
        for cp in wkv_cp(nk):
            cp.start()

    def proj_dy(k):
        wo_cp(k).wait()

        def body(p, _):
            w = WO[pl.ds(2 * p, 2)].reshape(2 * E, CW)
            acc(p, dot(DYS[k], w, 1, 1), k == 0)
            return 0
        lax.fori_loop(0, NP, body, 0)
        if k + 1 < NY:
            wo_cp(k + 1).start()

    def copy_acc(dst):
        def body(p, _):
            cols = pl.ds(mul(p, 2 * E), 2 * E)
            dst[p, 0:HR, :] = MY[0, :, cols].astype(BF16)
            dst[p, HR:R, :] = MY[1, :, cols].astype(BF16)
            return 0
        lax.fori_loop(0, NP, body, 0)

    T2 = 2 * T

    def pos(i):
        g = lax.div(i, T)
        return (2 * lax.rem(g, NX) + lax.div(g, NX)) * T + lax.rem(i, T)

    def brow(i, g):
        return lax.div(i, T2) * HR + g * T2 + lax.rem(i, T2)

    def pick(load, g):
        return jnp.concatenate([load(slice(g * T2, g * T2 + T2)), load(slice(HR + g * T2, HR + g * T2 + T2))], axis=0)

    def put(store, g, v):
        store(slice(g * T2, g * T2 + T2), v[:T2])
        store(slice(HR + g * T2, HR + g * T2 + T2), v[T2:])

    def keys(t, g):
        return pick(lambda r: KV[t, r, :], 0) if g == 0 else KV[t]

    def probs(q, g):
        s = dot(q, keys(0, g), 1, 1) * scale2
        n = s.shape[1]
        qp = pos(brow(lax.broadcasted_iota(jnp.int32, (HR, 1), 0), g))
        kp = lax.broadcasted_iota(jnp.int32, (1, n), 1)
        kp = pos(brow(kp, 0) if g == 0 else kp)
        s = jnp.where(qp >= kp, s, -jnp.inf)
        e = jnp.exp2(s - jnp.max(s, axis=1, keepdims=True))
        return e * (1.0 / jnp.sum(e, axis=1, keepdims=True))

    def attn_fwd(p):
        for g in range(2):
            for a in range(2):
                ln = slice(a * E, (a + 1) * E)
                pr = probs(pick(lambda r: QB[p, r, ln], g), g)
                o = dot(pr.astype(BF16), keys(1, g), 1, 0).astype(BF16)

                def store(r, v):
                    OA[p, y, r, ln] = v
                put(store, g, o)

    def attn_bwd(p):
        for g in range(2):
            for a in range(2):
                ln = slice(a * E, (a + 1) * E)
                q = pick(lambda r: QB[p, r, ln], g)
                do = pick(lambda r: DOB[p, r, ln], g)
                o = pick(lambda r: OA[p, y, r, ln], g)
                pr = probs(q, g)
                delta = jnp.sum(do.astype(F32) * o.astype(F32), axis=1, keepdims=True)
                dp = dot(do, keys(1, g), 1, 1)
                ds = (pr * (dp - delta)).astype(BF16)
                dq = (dot(ds, keys(0, g), 1, 0) * scale).astype(BF16)
                dkv = jnp.concatenate([dot(ds, q, 0, 0), dot(pr.astype(BF16), do, 0, 0)], axis=1)

                def store(r, v):
                    DQA[p, y, r, ln] = v
                put(store, g, dq)
                if g == 0:
                    def add(r, v):
                        KVACC[r, :] = KVACC[r, :] + v
                    put(add, 0, dkv)
                else:
                    KVACC[...] = KVACC[...] + dkv

    def dkv_send():
        KVACC[:, :E] = KVACC[:, :E] * scale
        rc(KVACC, DKVR, exs.at[0], exr.at[0], PT).start()

    def dkv_sum():
        wait_recv(DKVR, exr.at[0])
        tot = (KVACC[...] + DKVR[...]).astype(BF16)
        DKVB[0] = tot[:, :E]
        DKVB[1] = tot[:, E:]

    KB = CW // 2
    KT = tile_of(KB, 256)

    def dwkv_tile(r, t):
        ck = 2 * h + lax.div(r, 2)
        off = pl.multiple_of(KB * lax.rem(r, 2) + t * KT, KT)
        kv = jnp.concatenate([DKVB[0], DKVB[1]], axis=1)
        return dot(XS[ck, :, pl.ds(off, KT)], kv, 0, 0)

    KH = KB // 2

    def dwkv_early():
        def body(t, _):
            KS[0, pl.ds(mul(t, KT), KT), :] = dwkv_tile(seq(2), t).astype(BF16)
            return 0
        lax.fori_loop(0, KB // KT, body, 0)
        rc(KS.at[0, pl.ds(0, KH)], KR.at[0, pl.ds(0, KH)], dks.at[0], dkr.at[0], YU).start()
        rc(KS.at[0, pl.ds(KH, KH)], KR.at[0, pl.ds(KH, KH)], dks.at[0], dkr.at[1], YD).start()

    def dwkv_part(n):
        def body(t, _):
            KS[n + 1, pl.ds(mul(t, KT), KT), :] = dwkv_tile(seq((1, -1)[n]), t).astype(BF16)
            return 0
        lax.fori_loop(0, KB // KT, body, 0)

    def dwkv_own():
        def body(t, _):
            rows = pl.ds(mul(t, KT), KT)
            v = dwkv_tile(y, t)
            dwk_ref[rows, :] = v[:, :E]
            dwv_ref[rows, :] = v[:, E:]
            return 0
        lax.fori_loop(0, KB // KT, body, 0)

    def dwkv_mid():
        for n, dev in enumerate((YU, YD)):
            half = pl.ds(n * KH, KH)
            wait_recv(KR.at[0, half], dkr.at[n])
            KS[n + 1, half, :] = (KS[n + 1, half, :].astype(F32) + KR[0, half, :].astype(F32)).astype(BF16)
            rc(KS.at[n + 1], KR.at[n + 1], dks.at[n + 1], dkr.at[n + 2], dev).start()

    def dwkv_final():
        for n in range(2):
            wait_recv(KR.at[n + 1], dkr.at[n + 2])

        def body(t, _):
            rows = pl.ds(mul(t, KT), KT)
            v = KR[1, rows, :].astype(F32) + KR[2, rows, :].astype(F32)
            dwk_ref[rows, :] = dwk_ref[rows, :] + v[:, :E]
            dwv_ref[rows, :] = dwv_ref[rows, :] + v[:, E:]
            return 0
        lax.fori_loop(0, KB // KT, body, 0)

    def rx_free():
        for dev in (XL, XR):
            pl.semaphore_signal(cred, inc=1, device_id=dev, device_id_type=MESH)

    CH = CW // 2
    NT = tile_of(CH, DXT)

    def w_half(k, g):
        rows, dst = pl.ds(k * CW + g * CH, CH), pl.ds(g * CH, CH)
        return [pltpu.make_async_copy(wq_ref.at[:, rows, :], WQ.at[:, dst, :], lwq.at[1 + g]),
                pltpu.make_async_copy(wk_ref.at[c, rows], WKV.at[0, dst], lwkv.at[2 + g]),
                pltpu.make_async_copy(wv_ref.at[c, rows], WKV.at[1, dst], lwkv.at[4 + g])]

    def dxc(k):
        if k == 0:
            wq_cp(0).wait()
            for cp in wkv_cp(0):
                cp.wait()
        for g in range(2):
            if k:
                for cp in w_half(k, g):
                    cp.wait()

            def body(t, _):
                off = pl.multiple_of(t * NT + g * CH, NT)
                rows = pl.ds(off, NT)
                w = jnp.concatenate([WQ[i, rows, :] for i in range(NH)] + [WKV[h, rows, :]], axis=1)
                v = dot(jnp.concatenate([DQA[p, y] for p in range(NP)] + [DKVB[h]], axis=1), w, 1, 1)
                lo, hi = v[:HR], v[HR:]
                MY[k, :, pl.ds(off, NT)] = jnp.where(h == 0, lo, hi)
                DYS[k, pl.ds(HR, HR), pl.ds(off, NT)] = jnp.where(h == 0, hi, lo).astype(BF16)
                return 0
            lax.fori_loop(0, CH // NT, body, 0)
            if k + 1 < NY:
                for cp in w_half(k + 1, g):
                    cp.start()
        rc(DYS.at[k, pl.ds(HR, HR)], DYS.at[k, pl.ds(0, HR)], pxs.at[k], pxr.at[k], PT).start()

    def blk(k, cc, o, n):
        rows = pl.ds(pl.multiple_of(cc * T + o, TH), n)
        return MY[k, rows, :] + DYS[k, rows, :].astype(F32)

    def rx_early(k, n):
        return WO.at[n, k * TH:(k + 1) * TH]

    def rx_full(k, n):
        i = 2 * (k % 2)
        return WO.at[2 + 2 * n + k // 2, i * TH:(i + 2) * TH]

    def rs1(k):
        wait_recv(DYS.at[k, pl.ds(0, HR)], pxr.at[k])
        SX[k, 0:T, :] = blk(k, chip(2), 0, T).astype(BF16)
        for n, dev in enumerate((XR, XL)):
            rc(SX.at[k, n * TH:(n + 1) * TH], rx_early(k, n), rss.at[k], rsr.at[k, n], dev).start()

    def rs2(k):
        for n, dev in enumerate((XR, XL)):
            o = (n + 1) * T
            add = slice(o + n * TH, o + (n + 1) * TH)
            SX[k, o + (1 - n) * TH:o + (2 - n) * TH, :] = blk(k, chip(1 - 2 * n), (1 - n) * TH, TH).astype(BF16)
            wait_recv(rx_early(k, n), rsr.at[k, n])
            SX[k, add, :] = (blk(k, chip(1 - 2 * n), n * TH, TH) + rx_early(k, n)[...].astype(F32)).astype(BF16)
            rc(SX.at[k, o:o + T], rx_full(k, n), rss.at[k], rsr.at[k, 2 + n], dev).start()

    def rs3(k):
        v = blk(k, c, 0, T)
        for n in range(2):
            wait_recv(rx_full(k, n), rsr.at[k, 2 + n])
            v = v + rx_full(k, n)[...].astype(F32)
        dx_ref[:, k * CW:(k + 1) * CW] = v.astype(BF16)

    OT = tile_of(CW, 512)

    def dwo(p):
        def body(t, _):
            cols = pl.ds(mul(t, OT), OT)
            v = dot(OA[p].reshape(NY * R, 2 * E), DYC[:, :, cols].reshape(NY * R, OT), 0, 0)
            dwo_ref[2 * p, :, cols] = v[:E]
            dwo_ref[2 * p + 1, :, cols] = v[E:]
            return 0
        lax.fori_loop(0, CW // OT, body, 0)

    def dwq(p):
        def body(t, _):
            cols = pl.ds(mul(t, OT), OT)
            v = dot(XC[:, :, cols].reshape(NY * R, OT), DQA[p].reshape(NY * R, 2 * E), 0, 0)
            dwq_ref[2 * p, cols, :] = v[:, :E]
            dwq_ref[2 * p + 1, cols, :] = v[:, E:]
            return 0
        lax.fori_loop(0, CW // OT, body, 0)

    def own_cols(dst, src):
        def body(t, _):
            rows = pl.ds(pl.multiple_of(t * T, T), T)
            dst[y, rows, :] = src[y, rows, :]
            return 0
        lax.fori_loop(0, R // T, body, 0)

    own(0)
    own(1)
    rc(XS.at[seq(2), pl.ds(my_rows, T)], XC.at[y, pl.ds(my_rows, T)], a2as.at[0], a2ar.at[3], at(2, 0)).start()

    def dy_a2a():
        for cp in ldc:
            cp.wait()
        for j in range(1, NY):
            rc(DYS.at[seq(j), pl.ds(my_rows, T)], DYC.at[y, pl.ds(my_rows, T)],
               a2as.at[1], a2ar.at[NY - j - 1], at(j, 0)).start()

    def compute(i):
        if i < NY:
            if i < 2:
                xc_send(i)
            proj_x(i)
            if i == 3:
                copy_acc(QB)
                KV[0] = KVACC[:, :E].astype(BF16)
                KV[1] = KVACC[:, E:].astype(BF16)
                for p in range(NP):
                    attn_fwd(p)
                    yown(p)
                own_cols(XC, XS)
        elif i < 8:
            proj_dy(i - NY)
            if i == 5:
                xc_fwd(0)
            if i == 6:
                xc_fwd(1)
                yfwd(0)
            if i == 7:
                rx_free()
                copy_acc(DOB)
                own_cols(DYC, DYS)
                KVACC[...] = jnp.zeros_like(KVACC)

    for i in range(9):
        fwd(i)
        if i == 0:
            dy_a2a()
        for n in range(i + 2, N_IT if i == 7 else i + 3):
            if n < N_IT and i <= 7:
                own(n)
        if i >= 1:
            opp(i - 1)
            fin(i - 1)
            compute(i - 1)

    attn_bwd(0)
    yown(NP)
    fwd(9)
    yfwd(1)
    attn_bwd(1)
    yown(NP + 1)
    fwd(10)
    attn_bwd(2)
    yown(NP + 2)
    for k in range(NY):
        ag_sent(NY + k)
    wait_send(DYS.at[0, pl.ds(0, 3 * T)], a2as.at[1])
    dkv_send()
    yfwd(2)
    dkv_sum()
    dxc(0)
    fwd(11)
    dxc(1)
    pl.semaphore_wait(cred, 2)
    rs1(0)
    dwkv_early()
    yfwd(NP)
    dxc(2)
    rs1(1)
    rs2(0)
    yfwd(NP + 1)
    dxc(3)
    rs1(2)
    rs2(1)
    rs1(3)
    dwkv_part(0)
    dwkv_part(1)
    for i in range(2 * NY, N_IT - 1):
        opp(i)
    yfwd(NP + 2)
    for i in range(2 * NY, N_IT - 1):
        fin(i)
    for p in range(NP):
        yopp(p)
    dwo(0)
    rs2(2)
    opp(N_IT - 1)
    dwkv_mid()
    dwo(1)
    rs2(3)
    dwo(2)
    rs3(0)
    for n in range(2):
        xc_fin(n)
    fin(N_IT - 1)
    for p in range(NP):
        yopp(NP + p)
    dwq(0)
    rs3(1)
    dwkv_own()
    dwq(1)
    rs3(2)
    dwq(2)
    dwkv_final()
    rs3(3)

    for i in list(range(NY)) + list(range(2 * NY, N_IT)):
        ag_sent(i)
    wait_send(XS.at[0, pl.ds(0, T)], a2as.at[0])
    for n in range(4):
        wait_send(XC.at[0, par], xcs.at[n])
    for q in range(2 * NP):
        ysent(q)
    wait_send(KVACC, exs.at[0])
    for n in range(3):
        wait_send(KS.at[n], dks.at[n])
    for k in range(NY):
        wait_send(DYS.at[k, pl.ds(HR, HR)], pxs.at[k])
        wait_send(SX.at[k], rss.at[k])


def copy_out(*refs):
    n = (len(refs) - 1) // 2
    cps = [pltpu.make_async_copy(refs[i], refs[n + i], refs[-1].at[i]) for i in range(n)]
    for cp in cps:
        cp.start()
    for cp in cps:
        cp.wait()


def solution(mesh):
    model_size = mesh.shape['model']
    tok_spec = P(('pod', 'data'), 'model', None)

    def device_step(x_loc, dy_loc, w_q, w_k, w_v, w_o):
        T, D = x_loc.shape[1:]
        NH, E = w_q.shape[1:]
        KVH = w_k.shape[0]
        NX = model_size // 2
        NY = mesh.shape['data']
        assert NX == 4 and NY == 4 and KVH == NX and NH == 6 and E == 2 * T
        NP = NH // 2
        CW = D // NY
        R = model_size * T
        KB = CW // 2
        cfg = (T, CW, E, NX, NY, NH)
        V = pltpu.VMEM
        S = pltpu.SemaphoreType.DMA
        n_it = 3 * NY
        scratch = [
            V((NY, R, CW), BF16), V((NY, R, CW), BF16), V((NY, R, CW), BF16), V((NY, R, CW), BF16),
            V((NP, NY, R, 2 * E), BF16), V((NP, NY, R, 2 * E), BF16),
            V((NP, R, 2 * E), BF16), V((NP, R, 2 * E), BF16), V((2, R, E), BF16),
            V((R, 2 * E), F32), V((R, 2 * E), F32), V((2, R, E), BF16),
            V((NH, CW, E), BF16), V((2, CW, E), BF16), V((NH, E, CW), BF16),
            V((NY, R // 2, CW), F32), V((NY, 3 * T, CW), BF16), V((NY - 1, KB, 2 * E), BF16), V((NY - 1, KB, 2 * E), BF16),
            S((n_it, 5)), S((n_it,)), S((NY,)), S((2,)), S((4,)), S((4,)), S((2 * NP, 4)), S((2 * NP,)),
            S((4,)), S((3,)), S((NY,)), S((NY,)), S((NY, 4)), S((NY,)), S((1,)), S((1,)),
            S((NY,)), S((NY,)), S((3,)), S((6,)), S((1,)), pltpu.SemaphoreType.REGULAR,
        ]
        any_spec = pl.BlockSpec(memory_space=pl.ANY)
        dx, dwq, dwk, dwv, dwo = pl.pallas_call(
            functools.partial(kernel, cfg),
            out_shape=[V((T, D), BF16), V((NH, CW, E), F32), V((KB, E), F32), V((KB, E), F32), V((NH, E, CW), F32)],
            in_specs=[any_spec] * 6,
            out_specs=[pl.BlockSpec(memory_space=V)] * 5,
            scratch_shapes=scratch,
            compiler_params=pltpu.CompilerParams(collective_id=0, has_side_effects=True, vmem_limit_bytes=VMEM_BYTES),
            name='attn_bwd_fused',
        )(x_loc[0], dy_loc[0], w_q.transpose(1, 0, 2), w_k, w_v, w_o)
        outs = (dx, dwq, dwk, dwv, dwo)
        dx, dwq, dwk, dwv, dwo = pl.pallas_call(
            copy_out,
            out_shape=[jax.ShapeDtypeStruct(o.shape, o.dtype) for o in outs],
            in_specs=[pl.BlockSpec(memory_space=OUT_IN)] * 5,
            out_specs=[any_spec] * 5,
            scratch_shapes=[S((5,))],
            compiler_params=pltpu.CompilerParams(vmem_limit_bytes=OUT_LIM),
            name='write_results',
        )(*outs)
        return dx[None], dwq.transpose(1, 0, 2), dwk, dwv, dwo

    kv_rows = P(('pod', 'model', 'data'), None)
    return jax.shard_map(device_step, mesh=mesh,
                         in_specs=(tok_spec, tok_spec, P(None, 'model', None), P(), P(), P('model', None, None)),
                         out_specs=(tok_spec, P(('pod', 'data'), 'model', None), kv_rows, kv_rows, P(('pod', 'model'), None, 'data')),
                         check_vma=False)
```

```python
import functools

import jax
import jax.numpy as jnp
from jax import lax
from jax.experimental import pallas as pl
from jax.experimental.pallas import tpu as pltpu
from jax.sharding import PartitionSpec as P

MESH = pl.DeviceIdType.MESH
F32 = jnp.float32
BF16 = jnp.bfloat16
VMEM_BYTES = 55 * 1000 * 1000
DXT = 384
KTW = 768
UNR = True
OUT_IN = pl.ANY
OUT_LIM = 1024 * 1024
LOG2E = 1.4426950408889634


def dot(a, b, ca, cb):
    return lax.dot_general(a, b, (((ca,), (cb,)), ((), ())), preferred_element_type=F32)


def tile_of(n, t):
    return t if n % t == 0 else n


def kernel(cfg, x_ref, dy_ref, wq_ref, wk_ref, wv_ref, wo_ref,
           dx_ref, dwq_ref, dwk_ref, dwv_ref, dwo_ref,
           XS, DYS, XC, DYC, OA, DQA, QB, DOB, KV, KVACC, DKVR, DKVB,
           WQ, WKV, WO, MY, SX, KS, KR, ST,
           agr, ags, a2ar, a2as, str_, sts, xcr, xcs, yr, ys, dkr, dks, pxr, pxs, rsr, rss, exs, exr,
           lx, ldy, lwq, lwkv, lwo, cred):
    T, CW, E, NX, NY, NH = cfg
    NP = NH // 2
    R = 2 * NX * T
    HR = NX * T
    TH = T // 2
    scale = E ** -0.5
    scale2 = scale * LOG2E
    pod = lax.axis_index('pod')
    y = lax.axis_index('data')
    m = lax.axis_index('model')
    c = lax.div(m, 2)
    h = lax.rem(m, 2)

    def at(dy_, dx_):
        return (pod, lax.rem(y + dy_ + NY, NY), 2 * lax.rem(c + dx_ + NX, NX) + h)

    XR, XL = at(0, 1), at(0, -1)
    YU, YD = at(1, 0), at(-1, 0)
    PT = (pod, y, 2 * c + 1 - h)

    def rc(src, dst, ssem, rsem, dev):
        return pltpu.make_async_remote_copy(src_ref=src, dst_ref=dst, send_sem=ssem, recv_sem=rsem,
                                            device_id=dev, device_id_type=MESH)

    def wait_recv(dst, sem):
        rc(dst, dst, sem, sem, PT).wait_recv()

    def wait_send(src, sem):
        rc(src, src, sem, sem, PT).wait_send()

    def chip(k):
        return lax.rem(c + k + NX, NX)

    def seq(k):
        return lax.rem(y + k + NY, NY)

    def rb(k):
        return pl.multiple_of((h * NX + chip(k)) * T, T)

    my_rows = rb(0)
    def mul(k, n):
        return pl.multiple_of(k * n, n)

    def wq_cp(k):
        return pltpu.make_async_copy(wq_ref.at[:, pl.ds(mul(k, CW), CW), :], WQ, lwq.at[0])

    def wkv_cp(k):
        return [pltpu.make_async_copy(wk_ref.at[c, pl.ds(mul(k, CW), CW)], WKV.at[0], lwkv.at[0]),
                pltpu.make_async_copy(wv_ref.at[c, pl.ds(mul(k, CW), CW)], WKV.at[1], lwkv.at[1])]

    def wo_cp(k):
        return pltpu.make_async_copy(wo_ref.at[:, :, pl.ds(mul(k, CW), CW)], WO, lwo.at[0])

    bar = pltpu.get_barrier_semaphore()
    peers = [XR, XL, PT] + [at(j, 0) for j in range(1, NY)]
    for dev in peers:
        pl.semaphore_signal(bar, inc=1, device_id=dev, device_id_type=MESH)
    x_order = [seq(1), seq(-1), seq(2), y]
    dy_order = [y, seq(1), seq(-1), seq(2)]
    lxc = [pltpu.make_async_copy(x_ref.at[:, pl.ds(k * CW, CW)], XS.at[k, pl.ds(my_rows, T)], lx.at[k]) for k in range(NY)]
    ldc = [pltpu.make_async_copy(dy_ref.at[:, pl.ds(k * CW, CW)], DYS.at[k, pl.ds(my_rows, T)], ldy.at[k]) for k in range(NY)]
    for cp in lxc + ldc:
        cp.start()
    for cp in lxc:
        cp.wait()
    wq_cp(x_order[0]).start()
    for cp in wkv_cp(x_order[0]):
        cp.start()
    wo_cp(dy_order[0]).start()
    pl.semaphore_wait(bar, len(peers))

    items = ([(XS, k) for k in x_order] + [(DYS, k) for k in dy_order]
             + [(DYC, seq(j)) for j in range(1, NY)] + [(XC, seq(2))])
    N_IT = len(items)

    def my_half(n):
        return pl.ds(pl.multiple_of(my_rows + n * TH, TH), TH)

    def far_send(t):
        for n, dev in enumerate((YU, YD)):
            rc((DYS, XS)[t].at[seq(2), my_half(n)], ST.at[t, n], sts.at[t, n], str_.at[t, n], dev).start()

    def far_fwd(t):
        for n, dev in enumerate((YU, YD)):
            wait_recv(ST.at[t, n], str_.at[t, n])
            rc(ST.at[t, n], (DYC, XC)[t].at[seq((-1, 1)[n]), my_half(n)], sts.at[t, 2 + n], str_.at[t, 2 + n], dev).start()

    def own(i):
        buf, ix = items[i]
        if i >= 2 * NY:
            if i in (2 * NY + 1, 2 * NY + 3):
                for n in range(2):
                    wait_recv(buf.at[ix, my_half(n)], str_.at[(i - 2 * NY - 1) // 2, 2 + n])
            else:
                wait_recv(buf.at[ix, pl.ds(my_rows, T)], a2ar.at[i - 2 * NY])
        blk = buf.at[ix, pl.ds(my_rows, T)]
        rc(blk, blk, ags.at[i], agr.at[i, 0], XR).start()
        rc(blk, blk, ags.at[i], agr.at[i, 1], XL).start()
        rc(blk, blk, ags.at[i], agr.at[i, 4], PT).start()

    def fwd(i):
        buf, ix = items[i]
        lb, rb_ = rb(-1), rb(1)
        blk = buf.at[ix, pl.ds(lb, T)]
        wait_recv(blk, agr.at[i, 0])
        half = buf.at[ix, pl.ds(lb, TH)]
        rc(half, half, ags.at[i], agr.at[i, 2], XR).start()
        rc(blk, blk, ags.at[i], agr.at[i, 4], PT).start()
        blk = buf.at[ix, pl.ds(rb_, T)]
        wait_recv(blk, agr.at[i, 1])
        half = buf.at[ix, pl.ds(pl.multiple_of(rb_ + TH, TH), TH)]
        rc(half, half, ags.at[i], agr.at[i, 3], XL).start()
        rc(blk, blk, ags.at[i], agr.at[i, 4], PT).start()

    def opp(i):
        buf, ix = items[i]
        ob = rb(2)
        wait_recv(buf.at[ix, pl.ds(ob, TH)], agr.at[i, 2])
        wait_recv(buf.at[ix, pl.ds(pl.multiple_of(ob + TH, TH), TH)], agr.at[i, 3])
        blk = buf.at[ix, pl.ds(ob, T)]
        rc(blk, blk, ags.at[i], agr.at[i, 4], PT).start()

    def fin(i):
        buf, ix = items[i]
        wait_recv(buf.at[ix, pl.ds(pl.multiple_of((1 - h) * HR, HR), HR)], agr.at[i, 4])

    def ag_sent(i):
        buf, ix = items[i]
        wait_send(buf.at[ix, pl.ds(0, 7 * T)], ags.at[i])

    par = pl.ds(mul(h, HR), HR)

    def xc_send(n):
        rc(XS.at[x_order[n], par], XC.at[y, par], xcs.at[n], xcr.at[n], (YU, YD)[n]).start()

    def xc_fwd(n):
        b = XC.at[seq((-1, 1)[n]), par]
        wait_recv(b, xcr.at[n])
        rc(b, b, xcs.at[2 + n], xcr.at[2 + n], PT).start()

    def xc_fin(n):
        wait_recv(XC.at[seq((-1, 1)[n]), pl.ds(mul(1 - h, HR), HR)], xcr.at[2 + n])

    def ybuf(q):
        return (OA if q < NP else DQA).at[q % NP]

    def yown(q):
        b = ybuf(q).at[y]
        rc(b, b, ys.at[q], yr.at[q, 0], YU).start()
        rc(b, b, ys.at[q], yr.at[q, 1], YD).start()

    def yfwd(q):
        b = ybuf(q)
        wait_recv(b.at[seq(-1)], yr.at[q, 0])
        half = b.at[seq(-1), pl.ds(0, HR)]
        rc(half, half, ys.at[q], yr.at[q, 2], YU).start()
        wait_recv(b.at[seq(1)], yr.at[q, 1])
        half = b.at[seq(1), pl.ds(HR, HR)]
        rc(half, half, ys.at[q], yr.at[q, 3], YD).start()

    def yopp(q):
        b = ybuf(q)
        wait_recv(b.at[seq(2), pl.ds(0, HR)], yr.at[q, 2])
        wait_recv(b.at[seq(2), pl.ds(HR, HR)], yr.at[q, 3])

    def ysent(q):
        wait_send(ybuf(q).at[pl.ds(0, 3)], ys.at[q])

    def acc(p, d, first):
        cols = pl.ds(mul(p, 2 * E), 2 * E)
        MY[0, :, cols] = d[:HR] if first else MY[0, :, cols] + d[:HR]
        MY[1, :, cols] = d[HR:] if first else MY[1, :, cols] + d[HR:]

    def proj_x(i):
        k = x_order[i]
        wq_cp(k).wait()
        for cp in wkv_cp(k):
            cp.wait()

        def body(p, _):
            w = jnp.concatenate([WQ[2 * p], WQ[2 * p + 1]], axis=1)
            acc(p, dot(XS[k], w, 1, 0), i == 0)
            return 0
        lax.fori_loop(0, NP, body, 0)
        d = dot(XS[k], jnp.concatenate([WKV[0], WKV[1]], axis=1), 1, 0)
        KVACC[...] = d if i == 0 else KVACC[...] + d
        nk = x_order[i + 1] if i + 1 < NY else 0
        wq_cp(nk).start()
        for cp in wkv_cp(nk):
            cp.start()

    def proj_dy(i):
        k = dy_order[i]
        wo_cp(k).wait()

        def body(p, _):
            w = WO[pl.ds(2 * p, 2)].reshape(2 * E, CW)
            acc(p, dot(DYS[k], w, 1, 1), i == 0)
            return 0
        lax.fori_loop(0, NP, body, 0, unroll=UNR if i == NY - 1 else None)
        if i + 1 < NY:
            wo_cp(dy_order[i + 1]).start()

    def copy_acc(dst):
        def body(p, _):
            cols = pl.ds(mul(p, 2 * E), 2 * E)
            dst[p, 0:HR, :] = MY[0, :, cols].astype(BF16)
            dst[p, HR:R, :] = MY[1, :, cols].astype(BF16)
            return 0
        lax.fori_loop(0, NP, body, 0)

    T2 = 2 * T

    def pos(i):
        g = lax.div(i, T)
        return (2 * lax.rem(g, NX) + lax.div(g, NX)) * T + lax.rem(i, T)

    def brow(i, g):
        return lax.div(i, T2) * HR + g * T2 + lax.rem(i, T2)

    def pick(load, g):
        return jnp.concatenate([load(slice(g * T2, g * T2 + T2)), load(slice(HR + g * T2, HR + g * T2 + T2))], axis=0)

    def put(store, g, v):
        store(slice(g * T2, g * T2 + T2), v[:T2])
        store(slice(HR + g * T2, HR + g * T2 + T2), v[T2:])

    def keys(t, g):
        return pick(lambda r: KV[t, r, :], 0) if g == 0 else KV[t]

    def probs(q, g):
        s = dot(q, keys(0, g), 1, 1) * scale2
        n = s.shape[1]
        qp = pos(brow(lax.broadcasted_iota(jnp.int32, (HR, 1), 0), g))
        kp = lax.broadcasted_iota(jnp.int32, (1, n), 1)
        kp = pos(brow(kp, 0) if g == 0 else kp)
        s = jnp.where(qp >= kp, s, -jnp.inf)
        e = jnp.exp2(s - jnp.max(s, axis=1, keepdims=True))
        return e * (1.0 / jnp.sum(e, axis=1, keepdims=True))

    def prow(g, b):
        r = (g * T2 * 2 // E + b) * HR
        return slice(r, r + HR)

    def attn_fwd(p):
        for g in range(2):
            for a in range(2):
                ln = slice(a * E, (a + 1) * E)
                pr = probs(pick(lambda r: QB[p, r, ln], g), g)
                for b in range(pr.shape[1] // E):
                    dwq_ref[2 * p + a, prow(g, b), :] = pr[:, b * E:(b + 1) * E]
                o = dot(pr.astype(BF16), keys(1, g), 1, 0).astype(BF16)

                def store(r, v):
                    OA[p, y, r, ln] = v
                put(store, g, o)

    def attn_bwd(p):
        for g in range(2):
            for a in range(2):
                ln = slice(a * E, (a + 1) * E)
                q = pick(lambda r: QB[p, r, ln], g)
                do = pick(lambda r: DOB[p, r, ln], g)
                o = pick(lambda r: OA[p, y, r, ln], g)
                pr = jnp.concatenate([dwq_ref[2 * p + a, prow(g, b), :] for b in range((2 + 2 * g) * T2 // E)], axis=1)
                delta = jnp.sum(do.astype(F32) * o.astype(F32), axis=1, keepdims=True)
                dp = dot(do, keys(1, g), 1, 1)
                ds = (pr * (dp - delta)).astype(BF16)
                dq = (dot(ds, keys(0, g), 1, 0) * scale).astype(BF16)
                dkv = jnp.concatenate([dot(ds, q, 0, 0), dot(pr.astype(BF16), do, 0, 0)], axis=1)

                def store(r, v):
                    DQA[p, y, r, ln] = v
                put(store, g, dq)
                if g == 0:
                    def add(r, v):
                        KVACC[r, :] = KVACC[r, :] + v
                    put(add, 0, dkv)
                else:
                    KVACC[...] = KVACC[...] + dkv

    def dkv_send():
        KVACC[:, :E] = KVACC[:, :E] * scale
        rc(KVACC, DKVR, exs.at[0], exr.at[0], PT).start()

    def dkv_sum():
        wait_recv(DKVR, exr.at[0])
        tot = (KVACC[...] + DKVR[...]).astype(BF16)
        DKVB[0] = tot[:, :E]
        DKVB[1] = tot[:, E:]

    KB = CW // 2
    KT = tile_of(KB, KTW)

    def dwkv_tile(r, t):
        ck = 2 * h + lax.div(r, 2)
        off = pl.multiple_of(KB * lax.rem(r, 2) + t * KT, KT)
        kv = jnp.concatenate([DKVB[0], DKVB[1]], axis=1)
        return dot(XS[ck, :, pl.ds(off, KT)], kv, 0, 0)

    KH = KB // 2

    def dwkv_early():
        def body(t, _):
            KS[0, pl.ds(mul(t, KT), KT), :] = dwkv_tile(seq(2), t).astype(BF16)
            return 0
        lax.fori_loop(0, KB // KT, body, 0)
        rc(KS.at[0, pl.ds(0, KH)], KR.at[0, pl.ds(0, KH)], dks.at[0], dkr.at[0], YU).start()
        rc(KS.at[0, pl.ds(KH, KH)], KR.at[0, pl.ds(KH, KH)], dks.at[0], dkr.at[1], YD).start()

    def dwkv_part(n):
        def body(t, _):
            KS[n + 1, pl.ds(mul(t, KT), KT), :] = dwkv_tile(seq((1, -1)[n]), t).astype(BF16)
            return 0
        lax.fori_loop(0, KB // KT, body, 0)

    def dwkv_own():
        def body(t, _):
            rows = pl.ds(mul(t, KT), KT)
            v = dwkv_tile(y, t)
            dwk_ref[rows, :] = v[:, :E]
            dwv_ref[rows, :] = v[:, E:]
            return 0
        lax.fori_loop(0, KB // KT, body, 0)

    def dwkv_mid():
        for n, dev in enumerate((YU, YD)):
            half = pl.ds(n * KH, KH)
            wait_recv(KR.at[0, half], dkr.at[n])
            KS[n + 1, half, :] = (KS[n + 1, half, :].astype(F32) + KR[0, half, :].astype(F32)).astype(BF16)
            rc(KS.at[n + 1], KR.at[n + 1], dks.at[n + 1], dkr.at[n + 2], dev).start()

    def dwkv_final():
        for n in range(2):
            wait_recv(KR.at[n + 1], dkr.at[n + 2])

        def body(t, _):
            rows = pl.ds(mul(t, KT), KT)
            v = KR[1, rows, :].astype(F32) + KR[2, rows, :].astype(F32)
            dwk_ref[rows, :] = dwk_ref[rows, :] + v[:, :E]
            dwv_ref[rows, :] = dwv_ref[rows, :] + v[:, E:]
            return 0
        lax.fori_loop(0, KB // KT, body, 0)

    def rx_free():
        for dev in (XL, XR):
            pl.semaphore_signal(cred, inc=1, device_id=dev, device_id_type=MESH)

    CH = CW // 2
    NT = tile_of(CH, DXT)

    def w_half(k, g):
        rows, dst = pl.ds(k * CW + g * CH, CH), pl.ds(g * CH, CH)
        return [pltpu.make_async_copy(wq_ref.at[:, rows, :], WQ.at[:, dst, :], lwq.at[1 + g]),
                pltpu.make_async_copy(wk_ref.at[c, rows], WKV.at[0, dst], lwkv.at[2 + g]),
                pltpu.make_async_copy(wv_ref.at[c, rows], WKV.at[1, dst], lwkv.at[4 + g])]

    def dxc(k):
        if k == 0:
            wq_cp(0).wait()
            for cp in wkv_cp(0):
                cp.wait()
        for g in range(2):
            if k:
                for cp in w_half(k, g):
                    cp.wait()

            def body(t, _):
                off = pl.multiple_of(t * NT + g * CH, NT)
                rows = pl.ds(off, NT)
                w = jnp.concatenate([WQ[i, rows, :] for i in range(NH)] + [WKV[h, rows, :]], axis=1)
                v = dot(jnp.concatenate([DQA[p, y] for p in range(NP)] + [DKVB[h]], axis=1), w, 1, 1)
                lo, hi = v[:HR], v[HR:]
                MY[k, :, pl.ds(off, NT)] = jnp.where(h == 0, lo, hi)
                DYS[k, pl.ds(HR, HR), pl.ds(off, NT)] = jnp.where(h == 0, hi, lo).astype(BF16)
                return 0
            lax.fori_loop(0, CH // NT, body, 0, unroll=UNR)
            if k + 1 < NY:
                for cp in w_half(k + 1, g):
                    cp.start()
        rc(DYS.at[k, pl.ds(HR, HR)], DYS.at[k, pl.ds(0, HR)], pxs.at[k], pxr.at[k], PT).start()

    def blk(k, cc, o, n):
        rows = pl.ds(pl.multiple_of(cc * T + o, TH), n)
        return MY[k, rows, :] + DYS[k, rows, :].astype(F32)

    def rx_early(k, n):
        return WO.at[n, k * TH:(k + 1) * TH]

    def rx_full(k, n):
        i = 2 * (k % 2)
        return WO.at[2 + 2 * n + k // 2, i * TH:(i + 2) * TH]

    def rs1(k):
        wait_recv(DYS.at[k, pl.ds(0, HR)], pxr.at[k])
        SX[k, 0:T, :] = blk(k, chip(2), 0, T).astype(BF16)
        for n, dev in enumerate((XR, XL)):
            rc(SX.at[k, n * TH:(n + 1) * TH], rx_early(k, n), rss.at[k], rsr.at[k, n], dev).start()

    def rs2(k):
        for n, dev in enumerate((XR, XL)):
            o = (n + 1) * T
            add = slice(o + n * TH, o + (n + 1) * TH)
            SX[k, o + (1 - n) * TH:o + (2 - n) * TH, :] = blk(k, chip(1 - 2 * n), (1 - n) * TH, TH).astype(BF16)
            wait_recv(rx_early(k, n), rsr.at[k, n])
            SX[k, add, :] = (blk(k, chip(1 - 2 * n), n * TH, TH) + rx_early(k, n)[...].astype(F32)).astype(BF16)
            rc(SX.at[k, o:o + T], rx_full(k, n), rss.at[k], rsr.at[k, 2 + n], dev).start()

    def rs3(k):
        v = blk(k, c, 0, T)
        for n in range(2):
            wait_recv(rx_full(k, n), rsr.at[k, 2 + n])
            v = v + rx_full(k, n)[...].astype(F32)
        dx_ref[:, k * CW:(k + 1) * CW] = v.astype(BF16)

    OT = tile_of(CW, 512)

    others = [seq(1), seq(-1), seq(2)]

    def dwo_own(p):
        def body(t, _):
            cols = pl.ds(mul(t, OT), OT)
            v = dot(OA[p, y], DYC[y, :, cols], 0, 0)
            dwo_ref[2 * p, :, cols] = v[:E]
            dwo_ref[2 * p + 1, :, cols] = v[E:]
            return 0
        lax.fori_loop(0, CW // OT, body, 0)

    def dwo(p):
        def body(t, _):
            cols = pl.ds(mul(t, OT), OT)
            v = dot(jnp.concatenate([OA[p, s] for s in others], axis=0),
                    jnp.concatenate([DYC[s, :, cols] for s in others], axis=0), 0, 0)
            dwo_ref[2 * p, :, cols] = dwo_ref[2 * p, :, cols] + v[:E]
            dwo_ref[2 * p + 1, :, cols] = dwo_ref[2 * p + 1, :, cols] + v[E:]
            return 0
        lax.fori_loop(0, CW // OT, body, 0)

    def dwq_own(p):
        def body(t, _):
            cols = pl.ds(mul(t, OT), OT)
            v = dot(XC[y, :, cols], DQA[p, y], 0, 0)
            dwq_ref[2 * p, cols, :] = v[:, :E]
            dwq_ref[2 * p + 1, cols, :] = v[:, E:]
            return 0
        lax.fori_loop(0, CW // OT, body, 0)

    def dwq(p):
        def body(t, _):
            cols = pl.ds(mul(t, OT), OT)
            v = dot(jnp.concatenate([XC[s, :, cols] for s in others], axis=0),
                    jnp.concatenate([DQA[p, s] for s in others], axis=0), 0, 0)
            dwq_ref[2 * p, cols, :] = dwq_ref[2 * p, cols, :] + v[:, :E]
            dwq_ref[2 * p + 1, cols, :] = dwq_ref[2 * p + 1, cols, :] + v[:, E:]
            return 0
        lax.fori_loop(0, CW // OT, body, 0)

    def own_cols(dst, src):
        def body(t, _):
            rows = pl.ds(pl.multiple_of(t * T, T), T)
            dst[y, rows, :] = src[y, rows, :]
            return 0
        lax.fori_loop(0, R // T, body, 0)

    own(0)
    own(1)
    far_send(1)
    for cp in ldc:
        cp.wait()
    far_send(0)
    for j, dev in ((1, YU), (-1, YD)):
        rc(DYS.at[seq(j), pl.ds(my_rows, T)], DYC.at[y, pl.ds(my_rows, T)],
           a2as.at[0], a2ar.at[1 + j], dev).start()

    def compute(i):
        if i < NY:
            if i < 2:
                xc_send(i)
            proj_x(i)
            if i == 3:
                copy_acc(QB)
                KV[0] = KVACC[:, :E].astype(BF16)
                KV[1] = KVACC[:, E:].astype(BF16)
                for p in range(NP):
                    attn_fwd(p)
                    yown(p)
                    if p == 0:
                        fwd(5)
                        own(7)
                own_cols(XC, XS)
        elif i < 8:
            proj_dy(i - NY)
            if i == 4:
                own_cols(DYC, DYS)
            if i == 5:
                xc_fwd(0)
                yfwd(0)
                dwo_own(0)
                dwo_own(1)
            if i == 6:
                xc_fwd(1)
                yfwd(1)
                dwo_own(2)
            if i == 7:
                rx_free()
                yfwd(2)
                copy_acc(DOB)
                KVACC[...] = jnp.zeros_like(KVACC)

    for i in range(9):
        if i < 8 and i != 5:
            fwd(i)
        if i == 0:
            far_fwd(1)
        if i == 1:
            far_fwd(0)
        for n in range(i + 2, i + 3) if i < 5 else range(8, N_IT) if i == 7 else ():
            own(n)
        if i >= 1:
            opp(i - 1)
            fin(i - 1)
            compute(i - 1)

    attn_bwd(0)
    yown(NP)
    fwd(8)
    attn_bwd(1)
    yown(NP + 1)
    attn_bwd(2)
    yown(NP + 2)
    fwd(9)
    for k in range(NY):
        ag_sent(NY + k)
    wait_send(DYS.at[0, pl.ds(0, 2 * T)], a2as.at[0])
    for n in range(2):
        wait_send(DYS.at[0, pl.ds(0, TH)], sts.at[0, n])
    dkv_send()
    for p in range(NP):
        dwq_own(p)
    fwd(10)
    dkv_sum()
    dxc(0)
    yfwd(NP)
    dxc(1)
    fwd(11)
    pl.semaphore_wait(cred, 2)
    rs1(0)
    opp(8)
    dwkv_early()
    dxc(2)
    rs1(1)
    yfwd(NP + 1)
    opp(9)
    dwkv_part(0)
    dxc(3)
    rs1(2)
    rs2(0)
    opp(10)
    yfwd(NP + 2)
    dwkv_part(1)
    rs1(3)
    rs2(1)
    opp(11)
    for i in range(2 * NY, N_IT - 1):
        fin(i)
    for p in range(NP):
        yopp(p)
        dwo(p)
        if p == 1:
            dwkv_mid()
    rs2(2)
    for n in range(2):
        xc_fin(n)
    fin(N_IT - 1)
    yopp(NP)
    dwq(0)
    dwkv_own()
    rs3(0)
    yopp(NP + 1)
    dwq(1)
    rs2(3)
    rs3(1)
    yopp(NP + 2)
    dwq(2)
    rs3(2)
    dwkv_final()
    rs3(3)

    for i in list(range(NY)) + list(range(2 * NY, N_IT)):
        ag_sent(i)
    for n in range(2):
        wait_send(XS.at[0, pl.ds(0, TH)], sts.at[1, n])
        for t in range(2):
            wait_send(ST.at[t, n], sts.at[t, 2 + n])
    for n in range(4):
        wait_send(XC.at[0, par], xcs.at[n])
    for q in range(2 * NP):
        ysent(q)
    wait_send(KVACC, exs.at[0])
    for n in range(3):
        wait_send(KS.at[n], dks.at[n])
    for k in range(NY):
        wait_send(DYS.at[k, pl.ds(HR, HR)], pxs.at[k])
        wait_send(SX.at[k], rss.at[k])


def copy_out(*refs):
    n = (len(refs) - 1) // 2
    cps = [pltpu.make_async_copy(refs[i], refs[n + i], refs[-1].at[i]) for i in range(n)]
    for cp in cps:
        cp.start()
    for cp in cps:
        cp.wait()


def solution(mesh):
    model_size = mesh.shape['model']
    tok_spec = P(('pod', 'data'), 'model', None)

    def device_step(x_loc, dy_loc, w_q, w_k, w_v, w_o):
        T, D = x_loc.shape[1:]
        NH, E = w_q.shape[1:]
        KVH = w_k.shape[0]
        NX = model_size // 2
        NY = mesh.shape['data']
        assert NX == 4 and NY == 4 and KVH == NX and NH == 6 and E == 2 * T
        NP = NH // 2
        CW = D // NY
        assert CW == 6 * NX * T
        R = model_size * T
        KB = CW // 2
        cfg = (T, CW, E, NX, NY, NH)
        V = pltpu.VMEM
        S = pltpu.SemaphoreType.DMA
        n_it = 3 * NY
        scratch = [
            V((NY, R, CW), BF16), V((NY, R, CW), BF16), V((NY, R, CW), BF16), V((NY, R, CW), BF16),
            V((NP, NY, R, 2 * E), BF16), V((NP, NY, R, 2 * E), BF16),
            V((NP, R, 2 * E), BF16), V((NP, R, 2 * E), BF16), V((2, R, E), BF16),
            V((R, 2 * E), F32), V((R, 2 * E), F32), V((2, R, E), BF16),
            V((NH, CW, E), BF16), V((2, CW, E), BF16), V((NH, E, CW), BF16),
            V((NY, R // 2, CW), F32), V((NY, 3 * T, CW), BF16), V((NY - 1, KB, 2 * E), BF16), V((NY - 1, KB, 2 * E), BF16),
            V((2, 2, T // 2, CW), BF16),
            S((n_it, 5)), S((n_it,)), S((NY,)), S((1,)), S((2, 4)), S((2, 4)), S((4,)), S((4,)), S((2 * NP, 4)), S((2 * NP,)),
            S((4,)), S((3,)), S((NY,)), S((NY,)), S((NY, 4)), S((NY,)), S((1,)), S((1,)),
            S((NY,)), S((NY,)), S((3,)), S((6,)), S((1,)), pltpu.SemaphoreType.REGULAR,
        ]
        any_spec = pl.BlockSpec(memory_space=pl.ANY)
        dx, dwq, dwk, dwv, dwo = pl.pallas_call(
            functools.partial(kernel, cfg),
            out_shape=[V((T, D), BF16), V((NH, CW, E), F32), V((KB, E), F32), V((KB, E), F32), V((NH, E, CW), F32)],
            in_specs=[any_spec] * 6,
            out_specs=[pl.BlockSpec(memory_space=V)] * 5,
            scratch_shapes=scratch,
            compiler_params=pltpu.CompilerParams(collective_id=0, has_side_effects=True, vmem_limit_bytes=VMEM_BYTES),
            name='attn_bwd_fused',
        )(x_loc[0], dy_loc[0], w_q.transpose(1, 0, 2), w_k, w_v, w_o)
        outs = (dx, dwq, dwk, dwv, dwo)
        dx, dwq, dwk, dwv, dwo = pl.pallas_call(
            copy_out,
            out_shape=[jax.ShapeDtypeStruct(o.shape, o.dtype) for o in outs],
            in_specs=[pl.BlockSpec(memory_space=OUT_IN)] * 5,
            out_specs=[any_spec] * 5,
            scratch_shapes=[S((5,))],
            compiler_params=pltpu.CompilerParams(vmem_limit_bytes=OUT_LIM),
            name='write_results',
        )(*outs)
        return dx[None], dwq.transpose(1, 0, 2), dwk, dwv, dwo

    kv_rows = P(('pod', 'model', 'data'), None)
    return jax.shard_map(device_step, mesh=mesh,
                         in_specs=(tok_spec, tok_spec, P(None, 'model', None), P(), P(), P('model', None, None)),
                         out_specs=(tok_spec, P(('pod', 'data'), 'model', None), kv_rows, kv_rows, P(('pod', 'model'), None, 'data')),
                         check_vma=False)
```

```python
import functools

import jax
import jax.numpy as jnp
from jax import lax
from jax.experimental import pallas as pl
from jax.experimental.pallas import tpu as pltpu
from jax.sharding import PartitionSpec as P

MESH = pl.DeviceIdType.MESH
F32 = jnp.float32
BF16 = jnp.bfloat16
VMEM_BYTES = 55 * 1000 * 1000
DXT = 384
KTW = 768
UNR = True
OUT_IN = pl.ANY
OUT_LIM = 1024 * 1024
LOG2E = 1.4426950408889634


def dot(ca, cb, a, b):
    return lax.dot_general(a, b, (((ca,), (cb,)), ((), ())), preferred_element_type=F32)


nn = functools.partial(dot, 1, 0)
nt = functools.partial(dot, 1, 1)
tn = functools.partial(dot, 0, 0)


def loop(n, body, unroll=None):
    def step(t, z):
        body(t)
        return z
    lax.fori_loop(0, n, step, 0, unroll=unroll)


def tile_of(n, t):
    return t if n % t == 0 else n


def kernel(cfg, x_ref, dy_ref, wq_ref, wk_ref, wv_ref, wo_ref,
           dx_ref, dwq_ref, dwk_ref, dwv_ref, dwo_ref,
           XS, DYS, XC, DYC, OA, DQA, QB, DOB, KV, KVACC, DKVR, DKVB,
           WQ, WKV, WO, MY, SX, KS, KR, ST,
           agr, ags, a2ar, a2as, str_, sts, xcr, xcs, yr, ys, dkr, dks, pxr, pxs, rsr, rss, exs, exr,
           lx, ldy, lwq, lwkv, lwo, cred):
    T, CW, E, NX, NY, NH = cfg
    NP = NH // 2
    R = 2 * NX * T
    HR = NX * T
    TH = T // 2
    scale = E ** -0.5
    scale2 = scale * LOG2E
    pod = lax.axis_index('pod')
    y = lax.axis_index('data')
    m = lax.axis_index('model')
    c = lax.div(m, 2)
    h = lax.rem(m, 2)

    def at(dy_, dx_):
        return (pod, lax.rem(y + dy_ + NY, NY), 2 * lax.rem(c + dx_ + NX, NX) + h)

    XR, XL = at(0, 1), at(0, -1)
    YU, YD = at(1, 0), at(-1, 0)
    PT = (pod, y, 2 * c + 1 - h)

    def rc(src, dst, ssem, rsem, dev):
        return pltpu.make_async_remote_copy(src_ref=src, dst_ref=dst, send_sem=ssem, recv_sem=rsem,
                                            device_id=dev, device_id_type=MESH)

    def wait_recv(dst, sem):
        rc(dst, dst, sem, sem, PT).wait_recv()

    def wait_send(src, sem):
        rc(src, src, sem, sem, PT).wait_send()

    def chip(k):
        return lax.rem(c + k + NX, NX)

    def seq(k):
        return lax.rem(y + k + NY, NY)

    def rb(k):
        return pl.multiple_of((h * NX + chip(k)) * T, T)

    my_rows = rb(0)
    def mul(k, n):
        return pl.multiple_of(k * n, n)

    def wq_cp(k):
        return pltpu.make_async_copy(wq_ref.at[:, pl.ds(mul(k, CW), CW), :], WQ, lwq.at[0])

    def wkv_cp(k):
        return [pltpu.make_async_copy(wk_ref.at[c, pl.ds(mul(k, CW), CW)], WKV.at[0], lwkv.at[0]),
                pltpu.make_async_copy(wv_ref.at[c, pl.ds(mul(k, CW), CW)], WKV.at[1], lwkv.at[1])]

    def wo_cp(k):
        return pltpu.make_async_copy(wo_ref.at[:, :, pl.ds(mul(k, CW), CW)], WO, lwo.at[0])

    bar = pltpu.get_barrier_semaphore()
    peers = [XR, XL, PT] + [at(j, 0) for j in range(1, NY)]
    for dev in peers:
        pl.semaphore_signal(bar, inc=1, device_id=dev, device_id_type=MESH)
    x_order = [seq(1), seq(-1), seq(2), y]
    dy_order = [y, seq(1), seq(-1), seq(2)]
    lxc = [pltpu.make_async_copy(x_ref.at[:, pl.ds(k * CW, CW)], XS.at[k, pl.ds(my_rows, T)], lx.at[k]) for k in range(NY)]
    ldc = [pltpu.make_async_copy(dy_ref.at[:, pl.ds(k * CW, CW)], DYS.at[k, pl.ds(my_rows, T)], ldy.at[k]) for k in range(NY)]
    for cp in lxc + ldc:
        cp.start()
    for cp in lxc:
        cp.wait()
    wq_cp(x_order[0]).start()
    for cp in wkv_cp(x_order[0]):
        cp.start()
    wo_cp(dy_order[0]).start()
    pl.semaphore_wait(bar, len(peers))

    items = ([(XS, k) for k in x_order] + [(DYS, k) for k in dy_order]
             + [(DYC, seq(j)) for j in range(1, NY)] + [(XC, seq(2))])
    N_IT = len(items)

    def my_half(n):
        return pl.ds(pl.multiple_of(my_rows + n * TH, TH), TH)

    def far_send(t):
        for n, dev in enumerate((YU, YD)):
            rc((DYS, XS)[t].at[seq(2), my_half(n)], ST.at[t, n], sts.at[t, n], str_.at[t, n], dev).start()

    def far_fwd(t):
        for n, dev in enumerate((YU, YD)):
            wait_recv(ST.at[t, n], str_.at[t, n])
            rc(ST.at[t, n], (DYC, XC)[t].at[seq((-1, 1)[n]), my_half(n)], sts.at[t, 2 + n], str_.at[t, 2 + n], dev).start()

    def own(i):
        buf, ix = items[i]
        if i >= 2 * NY:
            if i in (2 * NY + 1, 2 * NY + 3):
                for n in range(2):
                    wait_recv(buf.at[ix, my_half(n)], str_.at[(i - 2 * NY - 1) // 2, 2 + n])
            else:
                wait_recv(buf.at[ix, pl.ds(my_rows, T)], a2ar.at[i - 2 * NY])
        blk = buf.at[ix, pl.ds(my_rows, T)]
        rc(blk, blk, ags.at[i], agr.at[i, 0], XR).start()
        rc(blk, blk, ags.at[i], agr.at[i, 1], XL).start()
        rc(blk, blk, ags.at[i], agr.at[i, 4], PT).start()

    def fwd(i):
        buf, ix = items[i]
        lb, rb_ = rb(-1), rb(1)
        blk = buf.at[ix, pl.ds(lb, T)]
        wait_recv(blk, agr.at[i, 0])
        half = buf.at[ix, pl.ds(lb, TH)]
        rc(half, half, ags.at[i], agr.at[i, 2], XR).start()
        rc(blk, blk, ags.at[i], agr.at[i, 4], PT).start()
        blk = buf.at[ix, pl.ds(rb_, T)]
        wait_recv(blk, agr.at[i, 1])
        half = buf.at[ix, pl.ds(pl.multiple_of(rb_ + TH, TH), TH)]
        rc(half, half, ags.at[i], agr.at[i, 3], XL).start()
        rc(blk, blk, ags.at[i], agr.at[i, 4], PT).start()

    def opp(i):
        buf, ix = items[i]
        ob = rb(2)
        wait_recv(buf.at[ix, pl.ds(ob, TH)], agr.at[i, 2])
        wait_recv(buf.at[ix, pl.ds(pl.multiple_of(ob + TH, TH), TH)], agr.at[i, 3])
        blk = buf.at[ix, pl.ds(ob, T)]
        rc(blk, blk, ags.at[i], agr.at[i, 4], PT).start()

    def fin(i):
        buf, ix = items[i]
        wait_recv(buf.at[ix, pl.ds(pl.multiple_of((1 - h) * HR, HR), HR)], agr.at[i, 4])

    def ag_sent(i):
        buf, ix = items[i]
        wait_send(buf.at[ix, pl.ds(0, 7 * T)], ags.at[i])

    par = pl.ds(mul(h, HR), HR)

    def xc_send(n):
        rc(XS.at[x_order[n], par], XC.at[y, par], xcs.at[n], xcr.at[n], (YU, YD)[n]).start()

    def xc_fwd(n):
        b = XC.at[seq((-1, 1)[n]), par]
        wait_recv(b, xcr.at[n])
        rc(b, b, xcs.at[2 + n], xcr.at[2 + n], PT).start()

    def xc_fin(n):
        wait_recv(XC.at[seq((-1, 1)[n]), pl.ds(mul(1 - h, HR), HR)], xcr.at[2 + n])

    def ybuf(q):
        return (OA if q < NP else DQA).at[q % NP]

    def yown(q):
        b = ybuf(q).at[y]
        rc(b, b, ys.at[q], yr.at[q, 0], YU).start()
        rc(b, b, ys.at[q], yr.at[q, 1], YD).start()

    def yfwd(q):
        b = ybuf(q)
        wait_recv(b.at[seq(-1)], yr.at[q, 0])
        half = b.at[seq(-1), pl.ds(0, HR)]
        rc(half, half, ys.at[q], yr.at[q, 2], YU).start()
        wait_recv(b.at[seq(1)], yr.at[q, 1])
        half = b.at[seq(1), pl.ds(HR, HR)]
        rc(half, half, ys.at[q], yr.at[q, 3], YD).start()

    def yopp(q):
        b = ybuf(q)
        wait_recv(b.at[seq(2), pl.ds(0, HR)], yr.at[q, 2])
        wait_recv(b.at[seq(2), pl.ds(HR, HR)], yr.at[q, 3])

    def ysent(q):
        wait_send(ybuf(q).at[pl.ds(0, 3)], ys.at[q])

    def acc(p, d, first):
        cols = pl.ds(mul(p, 2 * E), 2 * E)
        MY[0, :, cols] = d[:HR] if first else MY[0, :, cols] + d[:HR]
        MY[1, :, cols] = d[HR:] if first else MY[1, :, cols] + d[HR:]

    def proj_x(i):
        k = x_order[i]
        wq_cp(k).wait()
        for cp in wkv_cp(k):
            cp.wait()

        def body(p):
            w = jnp.concatenate([WQ[2 * p], WQ[2 * p + 1]], axis=1)
            acc(p, nn(XS[k], w), i == 0)
        loop(NP, body)
        d = nn(XS[k], jnp.concatenate([WKV[0], WKV[1]], axis=1))
        KVACC[...] = d if i == 0 else KVACC[...] + d
        nk = x_order[i + 1] if i + 1 < NY else 0
        wq_cp(nk).start()
        for cp in wkv_cp(nk):
            cp.start()

    def proj_dy(i):
        k = dy_order[i]
        wo_cp(k).wait()

        def body(p):
            w = WO[pl.ds(2 * p, 2)].reshape(2 * E, CW)
            acc(p, nt(DYS[k], w), i == 0)
        loop(NP, body, unroll=UNR if i == NY - 1 else None)
        if i + 1 < NY:
            wo_cp(dy_order[i + 1]).start()

    def copy_acc(dst):
        def body(p):
            cols = pl.ds(mul(p, 2 * E), 2 * E)
            dst[p, 0:HR, :] = MY[0, :, cols].astype(BF16)
            dst[p, HR:R, :] = MY[1, :, cols].astype(BF16)
        loop(NP, body)

    T2 = 2 * T

    def pos(i):
        g = lax.div(i, T)
        return (2 * lax.rem(g, NX) + lax.div(g, NX)) * T + lax.rem(i, T)

    def brow(i, g):
        return lax.div(i, T2) * HR + g * T2 + lax.rem(i, T2)

    def pick(load, g):
        return jnp.concatenate([load(slice(g * T2, g * T2 + T2)), load(slice(HR + g * T2, HR + g * T2 + T2))], axis=0)

    def put(store, g, v):
        store(slice(g * T2, g * T2 + T2), v[:T2])
        store(slice(HR + g * T2, HR + g * T2 + T2), v[T2:])

    def keys(t, g):
        return pick(lambda r: KV[t, r, :], 0) if g == 0 else KV[t]

    def probs(q, g):
        s = nt(q, keys(0, g)) * scale2
        n = s.shape[1]
        qp = pos(brow(lax.broadcasted_iota(jnp.int32, (HR, 1), 0), g))
        kp = lax.broadcasted_iota(jnp.int32, (1, n), 1)
        kp = pos(brow(kp, 0) if g == 0 else kp)
        s = jnp.where(qp >= kp, s, -jnp.inf)
        e = jnp.exp2(s - jnp.max(s, axis=1, keepdims=True))
        return e * (1.0 / jnp.sum(e, axis=1, keepdims=True))

    def prow(g, b):
        r = (g * T2 * 2 // E + b) * HR
        return slice(r, r + HR)

    def attn_fwd(p):
        for g in range(2):
            for a in range(2):
                ln = slice(a * E, (a + 1) * E)
                pr = probs(pick(lambda r: QB[p, r, ln], g), g)
                for b in range(pr.shape[1] // E):
                    dwq_ref[2 * p + a, prow(g, b), :] = pr[:, b * E:(b + 1) * E]
                o = nn(pr.astype(BF16), keys(1, g)).astype(BF16)

                def store(r, v):
                    OA[p, y, r, ln] = v
                put(store, g, o)

    def attn_bwd(p):
        for g in range(2):
            for a in range(2):
                ln = slice(a * E, (a + 1) * E)
                q = pick(lambda r: QB[p, r, ln], g)
                do = pick(lambda r: DOB[p, r, ln], g)
                o = pick(lambda r: OA[p, y, r, ln], g)
                pr = jnp.concatenate([dwq_ref[2 * p + a, prow(g, b), :] for b in range((2 + 2 * g) * T2 // E)], axis=1)
                delta = jnp.sum(do.astype(F32) * o.astype(F32), axis=1, keepdims=True)
                dp = nt(do, keys(1, g))
                ds = (pr * (dp - delta)).astype(BF16)
                dq = (nn(ds, keys(0, g)) * scale).astype(BF16)
                dkv = jnp.concatenate([tn(ds, q), tn(pr.astype(BF16), do)], axis=1)

                def store(r, v):
                    DQA[p, y, r, ln] = v
                put(store, g, dq)
                if g == 0:
                    def add(r, v):
                        KVACC[r, :] = KVACC[r, :] + v
                    put(add, 0, dkv)
                else:
                    KVACC[...] = KVACC[...] + dkv

    def dkv_send():
        KVACC[:, :E] = KVACC[:, :E] * scale
        rc(KVACC, DKVR, exs.at[0], exr.at[0], PT).start()

    def dkv_sum():
        wait_recv(DKVR, exr.at[0])
        tot = (KVACC[...] + DKVR[...]).astype(BF16)
        DKVB[0] = tot[:, :E]
        DKVB[1] = tot[:, E:]

    KB = CW // 2
    KT = tile_of(KB, KTW)

    def dwkv_tile(r, t):
        ck = 2 * h + lax.div(r, 2)
        off = pl.multiple_of(KB * lax.rem(r, 2) + t * KT, KT)
        kv = jnp.concatenate([DKVB[0], DKVB[1]], axis=1)
        return tn(XS[ck, :, pl.ds(off, KT)], kv)

    KH = KB // 2

    def dwkv_early():
        def body(t):
            KS[0, pl.ds(mul(t, KT), KT), :] = dwkv_tile(seq(2), t).astype(BF16)
        loop(KB // KT, body)
        rc(KS.at[0, pl.ds(0, KH)], KR.at[0, pl.ds(0, KH)], dks.at[0], dkr.at[0], YU).start()
        rc(KS.at[0, pl.ds(KH, KH)], KR.at[0, pl.ds(KH, KH)], dks.at[0], dkr.at[1], YD).start()

    def dwkv_part(n):
        def body(t):
            KS[n + 1, pl.ds(mul(t, KT), KT), :] = dwkv_tile(seq((1, -1)[n]), t).astype(BF16)
        loop(KB // KT, body)

    def dwkv_own():
        def body(t):
            rows = pl.ds(mul(t, KT), KT)
            v = dwkv_tile(y, t)
            dwk_ref[rows, :] = v[:, :E]
            dwv_ref[rows, :] = v[:, E:]
        loop(KB // KT, body)

    def dwkv_mid():
        for n, dev in enumerate((YU, YD)):
            half = pl.ds(n * KH, KH)
            wait_recv(KR.at[0, half], dkr.at[n])
            KS[n + 1, half, :] = (KS[n + 1, half, :].astype(F32) + KR[0, half, :].astype(F32)).astype(BF16)
            rc(KS.at[n + 1], KR.at[n + 1], dks.at[n + 1], dkr.at[n + 2], dev).start()

    def dwkv_final():
        for n in range(2):
            wait_recv(KR.at[n + 1], dkr.at[n + 2])

        def body(t):
            rows = pl.ds(mul(t, KT), KT)
            v = KR[1, rows, :].astype(F32) + KR[2, rows, :].astype(F32)
            dwk_ref[rows, :] = dwk_ref[rows, :] + v[:, :E]
            dwv_ref[rows, :] = dwv_ref[rows, :] + v[:, E:]
        loop(KB // KT, body)

    def rx_free():
        for dev in (XL, XR):
            pl.semaphore_signal(cred, inc=1, device_id=dev, device_id_type=MESH)

    CH = CW // 2
    NT = tile_of(CH, DXT)

    def w_half(k, g):
        rows, dst = pl.ds(k * CW + g * CH, CH), pl.ds(g * CH, CH)
        return [pltpu.make_async_copy(wq_ref.at[:, rows, :], WQ.at[:, dst, :], lwq.at[1 + g]),
                pltpu.make_async_copy(wk_ref.at[c, rows], WKV.at[0, dst], lwkv.at[2 + g]),
                pltpu.make_async_copy(wv_ref.at[c, rows], WKV.at[1, dst], lwkv.at[4 + g])]

    def dxc(k):
        if k == 0:
            wq_cp(0).wait()
            for cp in wkv_cp(0):
                cp.wait()
        for g in range(2):
            if k:
                for cp in w_half(k, g):
                    cp.wait()

            def body(t):
                off = pl.multiple_of(t * NT + g * CH, NT)
                rows = pl.ds(off, NT)
                w = jnp.concatenate([WQ[i, rows, :] for i in range(NH)] + [WKV[h, rows, :]], axis=1)
                v = nt(jnp.concatenate([DQA[p, y] for p in range(NP)] + [DKVB[h]], axis=1), w)
                lo, hi = v[:HR], v[HR:]
                MY[k, :, pl.ds(off, NT)] = jnp.where(h == 0, lo, hi)
                DYS[k, pl.ds(HR, HR), pl.ds(off, NT)] = jnp.where(h == 0, hi, lo).astype(BF16)
            loop(CH // NT, body, unroll=UNR)
            if k + 1 < NY:
                for cp in w_half(k + 1, g):
                    cp.start()
        rc(DYS.at[k, pl.ds(HR, HR)], DYS.at[k, pl.ds(0, HR)], pxs.at[k], pxr.at[k], PT).start()

    def blk(k, cc, o, n):
        rows = pl.ds(pl.multiple_of(cc * T + o, TH), n)
        return MY[k, rows, :] + DYS[k, rows, :].astype(F32)

    def rx_early(k, n):
        return WO.at[n, k * TH:(k + 1) * TH]

    def rx_full(k, n):
        i = 2 * (k % 2)
        return WO.at[2 + 2 * n + k // 2, i * TH:(i + 2) * TH]

    def rs1(k):
        wait_recv(DYS.at[k, pl.ds(0, HR)], pxr.at[k])
        SX[k, 0:T, :] = blk(k, chip(2), 0, T).astype(BF16)
        for n, dev in enumerate((XR, XL)):
            rc(SX.at[k, n * TH:(n + 1) * TH], rx_early(k, n), rss.at[k], rsr.at[k, n], dev).start()

    def rs2(k):
        for n, dev in enumerate((XR, XL)):
            o = (n + 1) * T
            add = slice(o + n * TH, o + (n + 1) * TH)
            SX[k, o + (1 - n) * TH:o + (2 - n) * TH, :] = blk(k, chip(1 - 2 * n), (1 - n) * TH, TH).astype(BF16)
            wait_recv(rx_early(k, n), rsr.at[k, n])
            SX[k, add, :] = (blk(k, chip(1 - 2 * n), n * TH, TH) + rx_early(k, n)[...].astype(F32)).astype(BF16)
            rc(SX.at[k, o:o + T], rx_full(k, n), rss.at[k], rsr.at[k, 2 + n], dev).start()

    def rs3(k):
        v = blk(k, c, 0, T)
        for n in range(2):
            wait_recv(rx_full(k, n), rsr.at[k, 2 + n])
            v = v + rx_full(k, n)[...].astype(F32)
        dx_ref[:, k * CW:(k + 1) * CW] = v.astype(BF16)

    OT = tile_of(CW, 512)

    others = [seq(1), seq(-1), seq(2)]

    def dwo_own(p):
        def body(t):
            cols = pl.ds(mul(t, OT), OT)
            v = tn(OA[p, y], DYC[y, :, cols])
            dwo_ref[2 * p, :, cols] = v[:E]
            dwo_ref[2 * p + 1, :, cols] = v[E:]
        loop(CW // OT, body)

    def dwo(p):
        def body(t):
            cols = pl.ds(mul(t, OT), OT)
            v = tn(jnp.concatenate([OA[p, s] for s in others], axis=0),
                    jnp.concatenate([DYC[s, :, cols] for s in others], axis=0))
            dwo_ref[2 * p, :, cols] = dwo_ref[2 * p, :, cols] + v[:E]
            dwo_ref[2 * p + 1, :, cols] = dwo_ref[2 * p + 1, :, cols] + v[E:]
        loop(CW // OT, body)

    def dwq_own(p):
        def body(t):
            cols = pl.ds(mul(t, OT), OT)
            v = tn(XC[y, :, cols], DQA[p, y])
            dwq_ref[2 * p, cols, :] = v[:, :E]
            dwq_ref[2 * p + 1, cols, :] = v[:, E:]
        loop(CW // OT, body)

    def dwq(p):
        def body(t):
            cols = pl.ds(mul(t, OT), OT)
            v = tn(jnp.concatenate([XC[s, :, cols] for s in others], axis=0),
                    jnp.concatenate([DQA[p, s] for s in others], axis=0))
            dwq_ref[2 * p, cols, :] = dwq_ref[2 * p, cols, :] + v[:, :E]
            dwq_ref[2 * p + 1, cols, :] = dwq_ref[2 * p + 1, cols, :] + v[:, E:]
        loop(CW // OT, body)

    def own_cols(dst, src):
        def body(t):
            rows = pl.ds(pl.multiple_of(t * T, T), T)
            dst[y, rows, :] = src[y, rows, :]
        loop(R // T, body)

    own(0)
    own(1)
    far_send(1)
    for cp in ldc:
        cp.wait()
    far_send(0)
    for j, dev in ((1, YU), (-1, YD)):
        rc(DYS.at[seq(j), pl.ds(my_rows, T)], DYC.at[y, pl.ds(my_rows, T)],
           a2as.at[0], a2ar.at[1 + j], dev).start()

    def compute(i):
        if i < NY:
            if i < 2:
                xc_send(i)
            proj_x(i)
            if i == 3:
                copy_acc(QB)
                KV[0] = KVACC[:, :E].astype(BF16)
                KV[1] = KVACC[:, E:].astype(BF16)
                for p in range(NP):
                    attn_fwd(p)
                    yown(p)
                    if p == 0:
                        fwd(5)
                        own(7)
                own_cols(XC, XS)
        elif i < 8:
            proj_dy(i - NY)
            if i == 4:
                own_cols(DYC, DYS)
            if i == 5:
                xc_fwd(0)
                yfwd(0)
                dwo_own(0)
                dwo_own(1)
            if i == 6:
                xc_fwd(1)
                yfwd(1)
                dwo_own(2)
            if i == 7:
                rx_free()
                yfwd(2)
                copy_acc(DOB)
                KVACC[...] = jnp.zeros_like(KVACC)

    for i in range(9):
        if i < 8 and i != 5:
            fwd(i)
        if i == 0:
            far_fwd(1)
        if i == 1:
            far_fwd(0)
        for n in (i + 2,) if i < 5 else range(8, N_IT) if i == 7 else ():
            own(n)
        if i >= 1:
            opp(i - 1)
            fin(i - 1)
            compute(i - 1)

    attn_bwd(0)
    yown(NP)
    fwd(8)
    attn_bwd(1)
    yown(NP + 1)
    attn_bwd(2)
    yown(NP + 2)
    fwd(9)
    for k in range(NY):
        ag_sent(NY + k)
    wait_send(DYS.at[0, pl.ds(0, 2 * T)], a2as.at[0])
    for n in range(2):
        wait_send(DYS.at[0, pl.ds(0, TH)], sts.at[0, n])
    dkv_send()
    for p in range(NP):
        dwq_own(p)
    fwd(10)
    dkv_sum()
    dxc(0)
    yfwd(NP)
    dxc(1)
    fwd(11)
    pl.semaphore_wait(cred, 2)
    rs1(0)
    opp(8)
    dwkv_early()
    dxc(2)
    rs1(1)
    yfwd(NP + 1)
    opp(9)
    dwkv_part(0)
    dxc(3)
    rs1(2)
    rs2(0)
    opp(10)
    yfwd(NP + 2)
    dwkv_part(1)
    rs1(3)
    rs2(1)
    opp(11)
    for i in range(2 * NY, N_IT - 1):
        fin(i)
    for p in range(NP):
        yopp(p)
        dwo(p)
        if p == 1:
            rs2(2)
            dwkv_mid()
    for n in range(2):
        xc_fin(n)
    fin(N_IT - 1)
    yopp(NP)
    dwq(0)
    rs2(3)
    dwkv_own()
    rs3(0)
    yopp(NP + 1)
    dwq(1)
    rs3(1)
    yopp(NP + 2)
    dwq(2)
    rs3(2)
    dwkv_final()
    rs3(3)

    for i in list(range(NY)) + list(range(2 * NY, N_IT)):
        ag_sent(i)
    for n in range(2):
        wait_send(XS.at[0, pl.ds(0, TH)], sts.at[1, n])
        for t in range(2):
            wait_send(ST.at[t, n], sts.at[t, 2 + n])
    for n in range(4):
        wait_send(XC.at[0, par], xcs.at[n])
    for q in range(2 * NP):
        ysent(q)
    wait_send(KVACC, exs.at[0])
    for n in range(3):
        wait_send(KS.at[n], dks.at[n])
    for k in range(NY):
        wait_send(DYS.at[k, pl.ds(HR, HR)], pxs.at[k])
        wait_send(SX.at[k], rss.at[k])


def copy_out(*refs):
    n = (len(refs) - 1) // 2
    cps = [pltpu.make_async_copy(refs[i], refs[n + i], refs[-1].at[i]) for i in range(n)]
    for cp in cps:
        cp.start()
    for cp in cps:
        cp.wait()


def solution(mesh):
    model_size = mesh.shape['model']
    tok_spec = P(('pod', 'data'), 'model', None)

    def device_step(x_loc, dy_loc, w_q, w_k, w_v, w_o):
        T, D = x_loc.shape[1:]
        NH, E = w_q.shape[1:]
        KVH = w_k.shape[0]
        NX = model_size // 2
        NY = mesh.shape['data']
        assert NX == 4 and NY == 4 and KVH == NX and NH == 6 and E == 2 * T
        NP = NH // 2
        CW = D // NY
        assert CW == 6 * NX * T
        R = model_size * T
        KB = CW // 2
        cfg = (T, CW, E, NX, NY, NH)
        V = pltpu.VMEM
        S = pltpu.SemaphoreType.DMA
        n_it = 3 * NY
        scratch = [
            V((NY, R, CW), BF16), V((NY, R, CW), BF16), V((NY, R, CW), BF16), V((NY, R, CW), BF16),
            V((NP, NY, R, 2 * E), BF16), V((NP, NY, R, 2 * E), BF16),
            V((NP, R, 2 * E), BF16), V((NP, R, 2 * E), BF16), V((2, R, E), BF16),
            V((R, 2 * E), F32), V((R, 2 * E), F32), V((2, R, E), BF16),
            V((NH, CW, E), BF16), V((2, CW, E), BF16), V((NH, E, CW), BF16),
            V((NY, R // 2, CW), F32), V((NY, 3 * T, CW), BF16), V((NY - 1, KB, 2 * E), BF16), V((NY - 1, KB, 2 * E), BF16),
            V((2, 2, T // 2, CW), BF16),
            S((n_it, 5)), S((n_it,)), S((NY,)), S((1,)), S((2, 4)), S((2, 4)), S((4,)), S((4,)), S((2 * NP, 4)), S((2 * NP,)),
            S((4,)), S((3,)), S((NY,)), S((NY,)), S((NY, 4)), S((NY,)), S((1,)), S((1,)),
            S((NY,)), S((NY,)), S((3,)), S((6,)), S((1,)), pltpu.SemaphoreType.REGULAR,
        ]
        any_spec = pl.BlockSpec(memory_space=pl.ANY)
        dx, dwq, dwk, dwv, dwo = pl.pallas_call(
            functools.partial(kernel, cfg),
            out_shape=[V((T, D), BF16), V((NH, CW, E), F32), V((KB, E), F32), V((KB, E), F32), V((NH, E, CW), F32)],
            in_specs=[any_spec] * 6,
            out_specs=[pl.BlockSpec(memory_space=V)] * 5,
            scratch_shapes=scratch,
            compiler_params=pltpu.CompilerParams(collective_id=0, has_side_effects=True, vmem_limit_bytes=VMEM_BYTES),
            name='attn_bwd_fused',
        )(x_loc[0], dy_loc[0], w_q.transpose(1, 0, 2), w_k, w_v, w_o)
        outs = (dx, dwq, dwk, dwv, dwo)
        dx, dwq, dwk, dwv, dwo = pl.pallas_call(
            copy_out,
            out_shape=[jax.ShapeDtypeStruct(o.shape, o.dtype) for o in outs],
            in_specs=[pl.BlockSpec(memory_space=OUT_IN)] * 5,
            out_specs=[any_spec] * 5,
            scratch_shapes=[S((5,))],
            compiler_params=pltpu.CompilerParams(vmem_limit_bytes=OUT_LIM),
            name='write_results',
        )(*outs)
        return dx[None], dwq.transpose(1, 0, 2), dwk, dwv, dwo

    kv_rows = P(('pod', 'model', 'data'), None)
    return jax.shard_map(device_step, mesh=mesh,
                         in_specs=(tok_spec, tok_spec, P(None, 'model', None), P(), P(), P('model', None, None)),
                         out_specs=(tok_spec, P(('pod', 'data'), 'model', None), kv_rows, kv_rows, P(('pod', 'model'), None, 'data')),
                         check_vma=False)
```

```python
import functools

import jax
import jax.numpy as jnp
from jax import lax
from jax.experimental import pallas as pl
from jax.experimental.pallas import tpu as pltpu
from jax.sharding import PartitionSpec as P

MESH = pl.DeviceIdType.MESH
F32 = jnp.float32
BF16 = jnp.bfloat16
VMEM_BYTES = 55 * 1000 * 1000
DXT = 384
BY_Y = (8, 10)
KTW = 768
UNR = True
OUT_IN = pl.ANY
OUT_LIM = 1024 * 1024
LOG2E = 1.4426950408889634


def dot(ca, cb, a, b):
    return lax.dot_general(a, b, (((ca,), (cb,)), ((), ())), preferred_element_type=F32)


nn = functools.partial(dot, 1, 0)
nt = functools.partial(dot, 1, 1)
tn = functools.partial(dot, 0, 0)


def loop(n, body, unroll=None):
    def step(t, z):
        body(t)
        return z
    lax.fori_loop(0, n, step, 0, unroll=unroll)


def tile_of(n, t):
    return t if n % t == 0 else n


def kernel(cfg, x_ref, dy_ref, wq_ref, wk_ref, wv_ref, wo_ref,
           dx_ref, dwq_ref, dwk_ref, dwv_ref, dwo_ref,
           XS, DYS, XC, DYC, OA, DQA, QB, DOB, KV, KVACC, DKVR, DKVB,
           WQ, WKV, WO, MY, SX, KS, KR, ST,
           agr, ags, a2ar, a2as, str_, sts, dcs, xcr, xcs, yr, ys, dkr, dks, pxr, pxs, rsr, rss, exs, exr,
           lx, ldy, lwq, lwkv, lwo, cred):
    T, CW, E, NX, NY, NH = cfg
    NP = NH // 2
    R = 2 * NX * T
    HR = NX * T
    TH = T // 2
    scale = E ** -0.5
    scale2 = scale * LOG2E
    pod = lax.axis_index('pod')
    y = lax.axis_index('data')
    m = lax.axis_index('model')
    c = lax.div(m, 2)
    h = lax.rem(m, 2)

    def at(dy_, dx_):
        return (pod, lax.rem(y + dy_ + NY, NY), 2 * lax.rem(c + dx_ + NX, NX) + h)

    XR, XL = at(0, 1), at(0, -1)
    YU, YD = at(1, 0), at(-1, 0)
    PT = (pod, y, 2 * c + 1 - h)

    def rc(src, dst, ssem, rsem, dev):
        return pltpu.make_async_remote_copy(src_ref=src, dst_ref=dst, send_sem=ssem, recv_sem=rsem,
                                            device_id=dev, device_id_type=MESH)

    def wait_recv(dst, sem):
        rc(dst, dst, sem, sem, PT).wait_recv()

    def wait_send(src, sem):
        rc(src, src, sem, sem, PT).wait_send()

    def chip(k):
        return lax.rem(c + k + NX, NX)

    def seq(k):
        return lax.rem(y + k + NY, NY)

    def rb(k):
        return pl.multiple_of((h * NX + chip(k)) * T, T)

    my_rows = rb(0)
    def mul(k, n):
        return pl.multiple_of(k * n, n)

    def wq_cp(k):
        return pltpu.make_async_copy(wq_ref.at[:, pl.ds(mul(k, CW), CW), :], WQ, lwq.at[0])

    def wkv_cp(k):
        return [pltpu.make_async_copy(wk_ref.at[c, pl.ds(mul(k, CW), CW)], WKV.at[0], lwkv.at[0]),
                pltpu.make_async_copy(wv_ref.at[c, pl.ds(mul(k, CW), CW)], WKV.at[1], lwkv.at[1])]

    def wo_cp(k):
        return pltpu.make_async_copy(wo_ref.at[:, :, pl.ds(mul(k, CW), CW)], WO, lwo.at[0])

    bar = pltpu.get_barrier_semaphore()
    peers = [XR, XL, PT] + [at(j, 0) for j in range(1, NY)]
    for dev in peers:
        pl.semaphore_signal(bar, inc=1, device_id=dev, device_id_type=MESH)
    x_order = [seq(1), seq(-1), seq(2), y]
    dy_order = [y, seq(1), seq(-1), seq(2)]
    lxc = [pltpu.make_async_copy(x_ref.at[:, pl.ds(k * CW, CW)], XS.at[k, pl.ds(my_rows, T)], lx.at[k]) for k in range(NY)]
    ldc = [pltpu.make_async_copy(dy_ref.at[:, pl.ds(k * CW, CW)], DYS.at[k, pl.ds(my_rows, T)], ldy.at[k]) for k in range(NY)]
    for cp in lxc + ldc:
        cp.start()
    for cp in lxc:
        cp.wait()
    wq_cp(x_order[0]).start()
    for cp in wkv_cp(x_order[0]):
        cp.start()
    wo_cp(dy_order[0]).start()
    pl.semaphore_wait(bar, len(peers))

    items = ([(XS, k) for k in x_order] + [(DYS, k) for k in dy_order]
             + [(DYC, seq(j)) for j in range(1, NY)] + [(XC, seq(2))])
    N_IT = len(items)

    def my_half(n):
        return pl.ds(pl.multiple_of(my_rows + n * TH, TH), TH)

    def far_send(t):
        for n, dev in enumerate((YU, YD)):
            rc((DYS, XS)[t].at[seq(2), my_half(n)], ST.at[t, n], sts.at[t, n], str_.at[t, n], dev).start()

    def far_fwd(t):
        for n, dev in enumerate((YU, YD)):
            wait_recv(ST.at[t, n], str_.at[t, n])
            rc(ST.at[t, n], (DYC, XC)[t].at[seq((-1, 1)[n]), my_half(n)], sts.at[t, 2 + n], str_.at[t, 2 + n], dev).start()

    def opp_half(n):
        return pl.ds(pl.multiple_of(rb(2) + n * TH, TH), TH)

    def dyc_send():
        for n, dev in enumerate((YD, YU)):
            rc(DYS.at[dy_order[2 - n], opp_half(n)], DYC.at[y, opp_half(n)], dcs.at[n], agr.at[BY_Y[n], 2 + n], dev).start()

    def own(i):
        buf, ix = items[i]
        if i >= 2 * NY:
            if i in (2 * NY + 1, 2 * NY + 3):
                for n in range(2):
                    wait_recv(buf.at[ix, my_half(n)], str_.at[(i - 2 * NY - 1) // 2, 2 + n])
            else:
                wait_recv(buf.at[ix, pl.ds(my_rows, T)], a2ar.at[i - 2 * NY])
        blk = buf.at[ix, pl.ds(my_rows, T)]
        rc(blk, blk, ags.at[i], agr.at[i, 0], XR).start()
        rc(blk, blk, ags.at[i], agr.at[i, 1], XL).start()
        rc(blk, blk, ags.at[i], agr.at[i, 4], PT).start()

    def fwd(i):
        buf, ix = items[i]
        lb, rb_ = rb(-1), rb(1)
        blk = buf.at[ix, pl.ds(lb, T)]
        wait_recv(blk, agr.at[i, 0])
        half = buf.at[ix, pl.ds(lb, TH)]
        if i != BY_Y[0]:
            rc(half, half, ags.at[i], agr.at[i, 2], XR).start()
        rc(blk, blk, ags.at[i], agr.at[i, 4], PT).start()
        blk = buf.at[ix, pl.ds(rb_, T)]
        wait_recv(blk, agr.at[i, 1])
        half = buf.at[ix, pl.ds(pl.multiple_of(rb_ + TH, TH), TH)]
        if i != BY_Y[1]:
            rc(half, half, ags.at[i], agr.at[i, 3], XL).start()
        rc(blk, blk, ags.at[i], agr.at[i, 4], PT).start()

    def opp(i):
        buf, ix = items[i]
        ob = rb(2)
        wait_recv(buf.at[ix, pl.ds(ob, TH)], agr.at[i, 2])
        wait_recv(buf.at[ix, pl.ds(pl.multiple_of(ob + TH, TH), TH)], agr.at[i, 3])
        blk = buf.at[ix, pl.ds(ob, T)]
        rc(blk, blk, ags.at[i], agr.at[i, 4], PT).start()

    def fin(i):
        buf, ix = items[i]
        wait_recv(buf.at[ix, pl.ds(pl.multiple_of((1 - h) * HR, HR), HR)], agr.at[i, 4])

    def ag_sent(i):
        buf, ix = items[i]
        wait_send(buf.at[ix, pl.ds(0, 7 * T - (TH if i in BY_Y else 0))], ags.at[i])

    par = pl.ds(mul(h, HR), HR)

    def xc_send(n):
        rc(XS.at[x_order[n], par], XC.at[y, par], xcs.at[n], xcr.at[n], (YU, YD)[n]).start()

    def xc_fwd(n):
        b = XC.at[seq((-1, 1)[n]), par]
        wait_recv(b, xcr.at[n])
        rc(b, b, xcs.at[2 + n], xcr.at[2 + n], PT).start()

    def xc_fin(n):
        wait_recv(XC.at[seq((-1, 1)[n]), pl.ds(mul(1 - h, HR), HR)], xcr.at[2 + n])

    def ybuf(q):
        return (OA if q < NP else DQA).at[q % NP]

    def yown(q):
        b = ybuf(q).at[y]
        rc(b, b, ys.at[q], yr.at[q, 0], YU).start()
        rc(b, b, ys.at[q], yr.at[q, 1], YD).start()

    def yfwd(q):
        b = ybuf(q)
        wait_recv(b.at[seq(-1)], yr.at[q, 0])
        half = b.at[seq(-1), pl.ds(0, HR)]
        rc(half, half, ys.at[q], yr.at[q, 2], YU).start()
        wait_recv(b.at[seq(1)], yr.at[q, 1])
        half = b.at[seq(1), pl.ds(HR, HR)]
        rc(half, half, ys.at[q], yr.at[q, 3], YD).start()

    def yopp(q):
        b = ybuf(q)
        wait_recv(b.at[seq(2), pl.ds(0, HR)], yr.at[q, 2])
        wait_recv(b.at[seq(2), pl.ds(HR, HR)], yr.at[q, 3])

    def ysent(q):
        wait_send(ybuf(q).at[pl.ds(0, 3)], ys.at[q])

    def acc(p, d, first):
        cols = pl.ds(mul(p, 2 * E), 2 * E)
        MY[0, :, cols] = d[:HR] if first else MY[0, :, cols] + d[:HR]
        MY[1, :, cols] = d[HR:] if first else MY[1, :, cols] + d[HR:]

    def proj_x(i):
        k = x_order[i]
        wq_cp(k).wait()
        for cp in wkv_cp(k):
            cp.wait()

        def body(p):
            w = jnp.concatenate([WQ[2 * p], WQ[2 * p + 1]], axis=1)
            acc(p, nn(XS[k], w), i == 0)
        loop(NP, body)
        d = nn(XS[k], jnp.concatenate([WKV[0], WKV[1]], axis=1))
        KVACC[...] = d if i == 0 else KVACC[...] + d
        nk = x_order[i + 1] if i + 1 < NY else 0
        wq_cp(nk).start()
        for cp in wkv_cp(nk):
            cp.start()

    def proj_dy(i):
        k = dy_order[i]
        wo_cp(k).wait()

        def body(p):
            w = WO[pl.ds(2 * p, 2)].reshape(2 * E, CW)
            acc(p, nt(DYS[k], w), i == 0)
        loop(NP, body, unroll=UNR if i == NY - 1 else None)
        if i + 1 < NY:
            wo_cp(dy_order[i + 1]).start()

    def copy_acc(dst):
        def body(p):
            cols = pl.ds(mul(p, 2 * E), 2 * E)
            dst[p, 0:HR, :] = MY[0, :, cols].astype(BF16)
            dst[p, HR:R, :] = MY[1, :, cols].astype(BF16)
        loop(NP, body)

    T2 = 2 * T

    def pos(i):
        g = lax.div(i, T)
        return (2 * lax.rem(g, NX) + lax.div(g, NX)) * T + lax.rem(i, T)

    def brow(i, g):
        return lax.div(i, T2) * HR + g * T2 + lax.rem(i, T2)

    def pick(load, g):
        return jnp.concatenate([load(slice(g * T2, g * T2 + T2)), load(slice(HR + g * T2, HR + g * T2 + T2))], axis=0)

    def put(store, g, v):
        store(slice(g * T2, g * T2 + T2), v[:T2])
        store(slice(HR + g * T2, HR + g * T2 + T2), v[T2:])

    def keys(t, g):
        return pick(lambda r: KV[t, r, :], 0) if g == 0 else KV[t]

    def probs(q, g):
        s = nt(q, keys(0, g)) * scale2
        n = s.shape[1]
        qp = pos(brow(lax.broadcasted_iota(jnp.int32, (HR, 1), 0), g))
        kp = lax.broadcasted_iota(jnp.int32, (1, n), 1)
        kp = pos(brow(kp, 0) if g == 0 else kp)
        s = jnp.where(qp >= kp, s, -jnp.inf)
        e = jnp.exp2(s - jnp.max(s, axis=1, keepdims=True))
        return e * (1.0 / jnp.sum(e, axis=1, keepdims=True))

    def prow(g, b):
        r = (g * T2 * 2 // E + b) * HR
        return slice(r, r + HR)

    def attn_fwd(p):
        for g in range(2):
            for a in range(2):
                ln = slice(a * E, (a + 1) * E)
                pr = probs(pick(lambda r: QB[p, r, ln], g), g)
                for b in range(pr.shape[1] // E):
                    dwq_ref[2 * p + a, prow(g, b), :] = pr[:, b * E:(b + 1) * E]
                o = nn(pr.astype(BF16), keys(1, g)).astype(BF16)

                def store(r, v):
                    OA[p, y, r, ln] = v
                put(store, g, o)

    def attn_bwd(p):
        for g in range(2):
            for a in range(2):
                ln = slice(a * E, (a + 1) * E)
                q = pick(lambda r: QB[p, r, ln], g)
                do = pick(lambda r: DOB[p, r, ln], g)
                o = pick(lambda r: OA[p, y, r, ln], g)
                pr = jnp.concatenate([dwq_ref[2 * p + a, prow(g, b), :] for b in range((2 + 2 * g) * T2 // E)], axis=1)
                delta = jnp.sum(do.astype(F32) * o.astype(F32), axis=1, keepdims=True)
                dp = nt(do, keys(1, g))
                ds = (pr * (dp - delta)).astype(BF16)
                dq = (nn(ds, keys(0, g)) * scale).astype(BF16)
                dkv = jnp.concatenate([tn(ds, q), tn(pr.astype(BF16), do)], axis=1)

                def store(r, v):
                    DQA[p, y, r, ln] = v
                put(store, g, dq)
                if g == 0:
                    def add(r, v):
                        KVACC[r, :] = KVACC[r, :] + v
                    put(add, 0, dkv)
                else:
                    KVACC[...] = KVACC[...] + dkv

    def dkv_send():
        KVACC[:, :E] = KVACC[:, :E] * scale
        rc(KVACC, DKVR, exs.at[0], exr.at[0], PT).start()

    def dkv_sum():
        wait_recv(DKVR, exr.at[0])
        tot = (KVACC[...] + DKVR[...]).astype(BF16)
        DKVB[0] = tot[:, :E]
        DKVB[1] = tot[:, E:]

    KB = CW // 2
    KT = tile_of(KB, KTW)

    def dwkv_tile(r, t):
        ck = 2 * h + lax.div(r, 2)
        off = pl.multiple_of(KB * lax.rem(r, 2) + t * KT, KT)
        kv = jnp.concatenate([DKVB[0], DKVB[1]], axis=1)
        return tn(XS[ck, :, pl.ds(off, KT)], kv)

    KH = KB // 2

    def dwkv_early():
        def body(t):
            KS[0, pl.ds(mul(t, KT), KT), :] = dwkv_tile(seq(2), t).astype(BF16)
        loop(KB // KT, body)
        rc(KS.at[0, pl.ds(0, KH)], KR.at[0, pl.ds(0, KH)], dks.at[0], dkr.at[0], YU).start()
        rc(KS.at[0, pl.ds(KH, KH)], KR.at[0, pl.ds(KH, KH)], dks.at[0], dkr.at[1], YD).start()

    def dwkv_part(n):
        def body(t):
            KS[n + 1, pl.ds(mul(t, KT), KT), :] = dwkv_tile(seq((1, -1)[n]), t).astype(BF16)
        loop(KB // KT, body)

    def dwkv_own():
        def body(t):
            rows = pl.ds(mul(t, KT), KT)
            v = dwkv_tile(y, t)
            dwk_ref[rows, :] = v[:, :E]
            dwv_ref[rows, :] = v[:, E:]
        loop(KB // KT, body)

    def dwkv_mid():
        for n, dev in enumerate((YU, YD)):
            half = pl.ds(n * KH, KH)
            wait_recv(KR.at[0, half], dkr.at[n])
            KS[n + 1, half, :] = (KS[n + 1, half, :].astype(F32) + KR[0, half, :].astype(F32)).astype(BF16)
            rc(KS.at[n + 1], KR.at[n + 1], dks.at[n + 1], dkr.at[n + 2], dev).start()

    def dwkv_final():
        for n in range(2):
            wait_recv(KR.at[n + 1], dkr.at[n + 2])

        def body(t):
            rows = pl.ds(mul(t, KT), KT)
            v = KR[1, rows, :].astype(F32) + KR[2, rows, :].astype(F32)
            dwk_ref[rows, :] = dwk_ref[rows, :] + v[:, :E]
            dwv_ref[rows, :] = dwv_ref[rows, :] + v[:, E:]
        loop(KB // KT, body)

    def rx_free():
        for dev in (XL, XR):
            pl.semaphore_signal(cred, inc=1, device_id=dev, device_id_type=MESH)

    CH = CW // 2
    NT = tile_of(CH, DXT)

    def w_half(k, g):
        rows, dst = pl.ds(k * CW + g * CH, CH), pl.ds(g * CH, CH)
        return [pltpu.make_async_copy(wq_ref.at[:, rows, :], WQ.at[:, dst, :], lwq.at[1 + g]),
                pltpu.make_async_copy(wk_ref.at[c, rows], WKV.at[0, dst], lwkv.at[2 + g]),
                pltpu.make_async_copy(wv_ref.at[c, rows], WKV.at[1, dst], lwkv.at[4 + g])]

    def dxc(k):
        if k == 0:
            wq_cp(0).wait()
            for cp in wkv_cp(0):
                cp.wait()
        for g in range(2):
            if k:
                for cp in w_half(k, g):
                    cp.wait()

            def body(t):
                off = pl.multiple_of(t * NT + g * CH, NT)
                rows = pl.ds(off, NT)
                w = jnp.concatenate([WQ[i, rows, :] for i in range(NH)] + [WKV[h, rows, :]], axis=1)
                v = nt(jnp.concatenate([DQA[p, y] for p in range(NP)] + [DKVB[h]], axis=1), w)
                lo, hi = v[:HR], v[HR:]
                MY[k, :, pl.ds(off, NT)] = jnp.where(h == 0, lo, hi)
                DYS[k, pl.ds(HR, HR), pl.ds(off, NT)] = jnp.where(h == 0, hi, lo).astype(BF16)
            loop(CH // NT, body, unroll=UNR)
            if k + 1 < NY:
                for cp in w_half(k + 1, g):
                    cp.start()
        rc(DYS.at[k, pl.ds(HR, HR)], DYS.at[k, pl.ds(0, HR)], pxs.at[k], pxr.at[k], PT).start()

    def blk(k, cc, o, n):
        rows = pl.ds(pl.multiple_of(cc * T + o, TH), n)
        return MY[k, rows, :] + DYS[k, rows, :].astype(F32)

    def rx_early(k, n):
        return WO.at[n, k * TH:(k + 1) * TH]

    def rx_full(k, n):
        i = 2 * (k % 2)
        return WO.at[2 + 2 * n + k // 2, i * TH:(i + 2) * TH]

    def rs1(k):
        wait_recv(DYS.at[k, pl.ds(0, HR)], pxr.at[k])
        SX[k, 0:T, :] = blk(k, chip(2), 0, T).astype(BF16)
        for n, dev in enumerate((XR, XL)):
            rc(SX.at[k, n * TH:(n + 1) * TH], rx_early(k, n), rss.at[k], rsr.at[k, n], dev).start()

    def rs2(k):
        for n, dev in enumerate((XR, XL)):
            o = (n + 1) * T
            add = slice(o + n * TH, o + (n + 1) * TH)
            SX[k, o + (1 - n) * TH:o + (2 - n) * TH, :] = blk(k, chip(1 - 2 * n), (1 - n) * TH, TH).astype(BF16)
            wait_recv(rx_early(k, n), rsr.at[k, n])
            SX[k, add, :] = (blk(k, chip(1 - 2 * n), n * TH, TH) + rx_early(k, n)[...].astype(F32)).astype(BF16)
            rc(SX.at[k, o:o + T], rx_full(k, n), rss.at[k], rsr.at[k, 2 + n], dev).start()

    def rs3(k):
        v = blk(k, c, 0, T)
        for n in range(2):
            wait_recv(rx_full(k, n), rsr.at[k, 2 + n])
            v = v + rx_full(k, n)[...].astype(F32)
        dx_ref[:, k * CW:(k + 1) * CW] = v.astype(BF16)

    OT = tile_of(CW, 512)

    others = [seq(1), seq(-1), seq(2)]

    def dwo_own(p):
        def body(t):
            cols = pl.ds(mul(t, OT), OT)
            v = tn(OA[p, y], DYC[y, :, cols])
            dwo_ref[2 * p, :, cols] = v[:E]
            dwo_ref[2 * p + 1, :, cols] = v[E:]
        loop(CW // OT, body)

    def dwo(p):
        def body(t):
            cols = pl.ds(mul(t, OT), OT)
            v = tn(jnp.concatenate([OA[p, s] for s in others], axis=0),
                    jnp.concatenate([DYC[s, :, cols] for s in others], axis=0))
            dwo_ref[2 * p, :, cols] = dwo_ref[2 * p, :, cols] + v[:E]
            dwo_ref[2 * p + 1, :, cols] = dwo_ref[2 * p + 1, :, cols] + v[E:]
        loop(CW // OT, body)

    def dwq_own(p):
        def body(t):
            cols = pl.ds(mul(t, OT), OT)
            v = tn(XC[y, :, cols], DQA[p, y])
            dwq_ref[2 * p, cols, :] = v[:, :E]
            dwq_ref[2 * p + 1, cols, :] = v[:, E:]
        loop(CW // OT, body)

    def dwq(p):
        def body(t):
            cols = pl.ds(mul(t, OT), OT)
            v = tn(jnp.concatenate([XC[s, :, cols] for s in others], axis=0),
                    jnp.concatenate([DQA[p, s] for s in others], axis=0))
            dwq_ref[2 * p, cols, :] = dwq_ref[2 * p, cols, :] + v[:, :E]
            dwq_ref[2 * p + 1, cols, :] = dwq_ref[2 * p + 1, cols, :] + v[:, E:]
        loop(CW // OT, body)

    def own_cols(dst, src):
        def body(t):
            rows = pl.ds(pl.multiple_of(t * T, T), T)
            dst[y, rows, :] = src[y, rows, :]
        loop(R // T, body)

    own(0)
    own(1)
    far_send(1)
    for cp in ldc:
        cp.wait()
    far_send(0)
    for j, dev in ((1, YU), (-1, YD)):
        rc(DYS.at[seq(j), pl.ds(my_rows, T)], DYC.at[y, pl.ds(my_rows, T)],
           a2as.at[0], a2ar.at[1 + j], dev).start()

    def compute(i):
        if i < NY:
            if i < 2:
                xc_send(i)
            proj_x(i)
            if i == 3:
                copy_acc(QB)
                KV[0] = KVACC[:, :E].astype(BF16)
                KV[1] = KVACC[:, E:].astype(BF16)
                for p in range(NP):
                    if p < 2:
                        fwd(NY + p)
                        own(NY + p + 2)
                    attn_fwd(p)
                    yown(p)
                own_cols(XC, XS)
        elif i < 8:
            proj_dy(i - NY)
            if i == 4:
                own_cols(DYC, DYS)
            if i == 5:
                xc_fwd(0)
                yfwd(0)
                dwo_own(0)
                dwo_own(1)
            if i == 6:
                dyc_send()
                xc_fwd(1)
                yfwd(1)
                dwo_own(2)
            if i == 7:
                rx_free()
                yfwd(2)
                copy_acc(DOB)
                KVACC[...] = jnp.zeros_like(KVACC)

    for i in range(9):
        if i not in (4, 5, 8):
            fwd(i)
        if i == 0:
            far_fwd(1)
        if i == 1:
            far_fwd(0)
        for n in (4, 5) if i == 3 else () if i == 2 else (i + 2,) if i < 4 else range(8, N_IT) if i == 7 else ():
            own(n)
        if i >= 1:
            opp(i - 1)
            fin(i - 1)
            compute(i - 1)

    attn_bwd(0)
    yown(NP)
    fwd(8)
    attn_bwd(1)
    yown(NP + 1)
    attn_bwd(2)
    yown(NP + 2)
    fwd(9)
    for k in range(NY):
        ag_sent(NY + k)
    wait_send(DYS.at[0, pl.ds(0, 2 * T)], a2as.at[0])
    for n in range(2):
        wait_send(DYS.at[0, pl.ds(0, TH)], sts.at[0, n])
        wait_send(DYS.at[0, pl.ds(0, TH)], dcs.at[n])
    dkv_send()
    for p in range(NP):
        dwq_own(p)
    fwd(10)
    dkv_sum()
    dxc(0)
    dxc(1)
    fwd(11)
    pl.semaphore_wait(cred, 2)
    rs1(0)
    opp(8)
    dwkv_early()
    yfwd(NP)
    dxc(2)
    rs1(1)
    yfwd(NP + 1)
    opp(9)
    dwkv_part(0)
    dxc(3)
    rs1(2)
    rs2(0)
    opp(10)
    yfwd(NP + 2)
    dwkv_part(1)
    rs1(3)
    rs2(1)
    opp(11)
    for i in range(2 * NY, N_IT - 1):
        fin(i)
    for p in range(NP):
        yopp(p)
        dwo(p)
        if p == 1:
            rs2(2)
            dwkv_mid()
    for n in range(2):
        xc_fin(n)
    fin(N_IT - 1)
    yopp(NP)
    dwq(0)
    rs2(3)
    dwkv_own()
    rs3(0)
    yopp(NP + 1)
    dwq(1)
    rs3(1)
    yopp(NP + 2)
    dwq(2)
    rs3(2)
    dwkv_final()
    rs3(3)

    for i in list(range(NY)) + list(range(2 * NY, N_IT)):
        ag_sent(i)
    for n in range(2):
        wait_send(XS.at[0, pl.ds(0, TH)], sts.at[1, n])
        for t in range(2):
            wait_send(ST.at[t, n], sts.at[t, 2 + n])
    for n in range(4):
        wait_send(XC.at[0, par], xcs.at[n])
    for q in range(2 * NP):
        ysent(q)
    wait_send(KVACC, exs.at[0])
    for n in range(3):
        wait_send(KS.at[n], dks.at[n])
    for k in range(NY):
        wait_send(DYS.at[k, pl.ds(HR, HR)], pxs.at[k])
        wait_send(SX.at[k], rss.at[k])


def copy_out(*refs):
    n = (len(refs) - 1) // 2
    cps = [pltpu.make_async_copy(refs[i], refs[n + i], refs[-1].at[i]) for i in range(n)]
    for cp in cps:
        cp.start()
    for cp in cps:
        cp.wait()


def solution(mesh):
    model_size = mesh.shape['model']
    tok_spec = P(('pod', 'data'), 'model', None)

    def device_step(x_loc, dy_loc, w_q, w_k, w_v, w_o):
        T, D = x_loc.shape[1:]
        NH, E = w_q.shape[1:]
        KVH = w_k.shape[0]
        NX = model_size // 2
        NY = mesh.shape['data']
        assert NX == 4 and NY == 4 and KVH == NX and NH == 6 and E == 2 * T
        NP = NH // 2
        CW = D // NY
        assert CW == 6 * NX * T
        R = model_size * T
        KB = CW // 2
        cfg = (T, CW, E, NX, NY, NH)
        V = pltpu.VMEM
        S = pltpu.SemaphoreType.DMA
        n_it = 3 * NY
        scratch = [
            V((NY, R, CW), BF16), V((NY, R, CW), BF16), V((NY, R, CW), BF16), V((NY, R, CW), BF16),
            V((NP, NY, R, 2 * E), BF16), V((NP, NY, R, 2 * E), BF16),
            V((NP, R, 2 * E), BF16), V((NP, R, 2 * E), BF16), V((2, R, E), BF16),
            V((R, 2 * E), F32), V((R, 2 * E), F32), V((2, R, E), BF16),
            V((NH, CW, E), BF16), V((2, CW, E), BF16), V((NH, E, CW), BF16),
            V((NY, R // 2, CW), F32), V((NY, 3 * T, CW), BF16), V((NY - 1, KB, 2 * E), BF16), V((NY - 1, KB, 2 * E), BF16),
            V((2, 2, T // 2, CW), BF16),
            S((n_it, 5)), S((n_it,)), S((NY,)), S((1,)), S((2, 4)), S((2, 4)), S((2,)), S((4,)), S((4,)), S((2 * NP, 4)), S((2 * NP,)),
            S((4,)), S((3,)), S((NY,)), S((NY,)), S((NY, 4)), S((NY,)), S((1,)), S((1,)),
            S((NY,)), S((NY,)), S((3,)), S((6,)), S((1,)), pltpu.SemaphoreType.REGULAR,
        ]
        any_spec = pl.BlockSpec(memory_space=pl.ANY)
        dx, dwq, dwk, dwv, dwo = pl.pallas_call(
            functools.partial(kernel, cfg),
            out_shape=[V((T, D), BF16), V((NH, CW, E), F32), V((KB, E), F32), V((KB, E), F32), V((NH, E, CW), F32)],
            in_specs=[any_spec] * 6,
            out_specs=[pl.BlockSpec(memory_space=V)] * 5,
            scratch_shapes=scratch,
            compiler_params=pltpu.CompilerParams(collective_id=0, has_side_effects=True, vmem_limit_bytes=VMEM_BYTES),
            name='attn_bwd_fused',
        )(x_loc[0], dy_loc[0], w_q.transpose(1, 0, 2), w_k, w_v, w_o)
        outs = (dx, dwq, dwk, dwv, dwo)
        dx, dwq, dwk, dwv, dwo = pl.pallas_call(
            copy_out,
            out_shape=[jax.ShapeDtypeStruct(o.shape, o.dtype) for o in outs],
            in_specs=[pl.BlockSpec(memory_space=OUT_IN)] * 5,
            out_specs=[any_spec] * 5,
            scratch_shapes=[S((5,))],
            compiler_params=pltpu.CompilerParams(vmem_limit_bytes=OUT_LIM),
            name='write_results',
        )(*outs)
        return dx[None], dwq.transpose(1, 0, 2), dwk, dwv, dwo

    kv_rows = P(('pod', 'model', 'data'), None)
    return jax.shard_map(device_step, mesh=mesh,
                         in_specs=(tok_spec, tok_spec, P(None, 'model', None), P(), P(), P('model', None, None)),
                         out_specs=(tok_spec, P(('pod', 'data'), 'model', None), kv_rows, kv_rows, P(('pod', 'model'), None, 'data')),
                         check_vma=False)
```

```python
import functools

import jax
import jax.numpy as jnp
from jax import lax
from jax.experimental import pallas as pl
from jax.experimental.pallas import tpu as pltpu
from jax.sharding import PartitionSpec as P

MESH = pl.DeviceIdType.MESH
F32 = jnp.float32
BF16 = jnp.bfloat16
VMEM_BYTES = 55 * 1000 * 1000
DXT = 384
BY_Y = (8, 10)
KTW = 768
UNR = True
OUT_IN = pl.ANY
OUT_LIM = 1024 * 1024
LOG2E = 1.4426950408889634


def dot(ca, cb, a, b):
    return lax.dot_general(a, b, (((ca,), (cb,)), ((), ())), preferred_element_type=F32)


nn = functools.partial(dot, 1, 0)
nt = functools.partial(dot, 1, 1)
tn = functools.partial(dot, 0, 0)


def loop(n, body, unroll=None):
    def step(t, z):
        body(t)
        return z
    lax.fori_loop(0, n, step, 0, unroll=unroll)


def tile_of(n, t):
    return t if n % t == 0 else n


def kernel(cfg, x_ref, dy_ref, wq_ref, wk_ref, wv_ref, wo_ref,
           dx_ref, dwq_ref, dwk_ref, dwv_ref, dwo_ref,
           XS, DYS, XC, DYC, OA, DQA, QB, DOB, KV, KVACC, DKVR, DKVB,
           WQ, WKV, WO, MY, SX, KS, KR, ST,
           agr, ags, a2ar, a2as, str_, sts, dcs, xcr, xcs, yr, ys, dkr, dks, pxr, pxs, rsr, rss, exs, exr,
           lx, ldy, lwq, lwkv, lwo, cred):
    T, CW, E, NX, NY, NH = cfg
    NP = NH // 2
    R = 2 * NX * T
    HR = NX * T
    TH = T // 2
    TQ = T // 4
    scale = E ** -0.5
    scale2 = scale * LOG2E
    pod = lax.axis_index('pod')
    y = lax.axis_index('data')
    m = lax.axis_index('model')
    c = lax.div(m, 2)
    h = lax.rem(m, 2)

    def at(dy_, dx_):
        return (pod, lax.rem(y + dy_ + NY, NY), 2 * lax.rem(c + dx_ + NX, NX) + h)

    XR, XL = at(0, 1), at(0, -1)
    YU, YD = at(1, 0), at(-1, 0)
    PT = (pod, y, 2 * c + 1 - h)

    def rc(src, dst, ssem, rsem, dev):
        return pltpu.make_async_remote_copy(src_ref=src, dst_ref=dst, send_sem=ssem, recv_sem=rsem,
                                            device_id=dev, device_id_type=MESH)

    def wait_recv(dst, sem):
        rc(dst, dst, sem, sem, PT).wait_recv()

    def wait_send(src, sem):
        rc(src, src, sem, sem, PT).wait_send()

    def chip(k):
        return lax.rem(c + k + NX, NX)

    def seq(k):
        return lax.rem(y + k + NY, NY)

    def rb(k):
        return pl.multiple_of((h * NX + chip(k)) * T, T)

    my_rows = rb(0)
    def mul(k, n):
        return pl.multiple_of(k * n, n)

    def wq_cp(k):
        return pltpu.make_async_copy(wq_ref.at[:, pl.ds(mul(k, CW), CW), :], WQ, lwq.at[0])

    def wkv_cp(k):
        return [pltpu.make_async_copy(wk_ref.at[c, pl.ds(mul(k, CW), CW)], WKV.at[0], lwkv.at[0]),
                pltpu.make_async_copy(wv_ref.at[c, pl.ds(mul(k, CW), CW)], WKV.at[1], lwkv.at[1])]

    def wo_cp(k):
        return pltpu.make_async_copy(wo_ref.at[:, :, pl.ds(mul(k, CW), CW)], WO, lwo.at[0])

    bar = pltpu.get_barrier_semaphore()
    peers = [XR, XL, PT] + [at(j, 0) for j in range(1, NY)]
    for dev in peers:
        pl.semaphore_signal(bar, inc=1, device_id=dev, device_id_type=MESH)
    x_order = [seq(1), seq(-1), seq(2), y]
    dy_order = [y, seq(1), seq(-1), seq(2)]
    lxc = [pltpu.make_async_copy(x_ref.at[:, pl.ds(k * CW, CW)], XS.at[k, pl.ds(my_rows, T)], lx.at[k]) for k in range(NY)]
    ldc = [pltpu.make_async_copy(dy_ref.at[:, pl.ds(k * CW, CW)], DYS.at[k, pl.ds(my_rows, T)], ldy.at[k]) for k in range(NY)]
    for cp in lxc + ldc:
        cp.start()
    for cp in lxc:
        cp.wait()
    wq_cp(x_order[0]).start()
    for cp in wkv_cp(x_order[0]):
        cp.start()
    wo_cp(dy_order[0]).start()
    pl.semaphore_wait(bar, len(peers))

    items = ([(XS, k) for k in x_order] + [(DYS, k) for k in dy_order]
             + [(DYC, seq(j)) for j in range(1, NY)] + [(XC, seq(2))])
    N_IT = len(items)

    def my_half(n):
        return pl.ds(pl.multiple_of(my_rows + n * TH, TH), TH)

    def far_send(t):
        for n, dev in enumerate((YU, YD)):
            rc((DYS, XS)[t].at[seq(2), my_half(n)], ST.at[t, n], sts.at[t, n], str_.at[t, n], dev).start()

    def far_fwd(t):
        for n, dev in enumerate((YU, YD)):
            wait_recv(ST.at[t, n], str_.at[t, n])
            rc(ST.at[t, n], (DYC, XC)[t].at[seq((-1, 1)[n]), my_half(n)], sts.at[t, 2 + n], str_.at[t, 2 + n], dev).start()

    def opp_half(n):
        return pl.ds(pl.multiple_of(rb(2) + n * TH + TQ, TQ), TQ)

    def dyc_send():
        for n, dev in enumerate((YD, YU)):
            rc(DYS.at[dy_order[2 - n], opp_half(n)], DYC.at[y, opp_half(n)], dcs.at[n], agr.at[BY_Y[n], 2 + n], dev).start()

    def own(i):
        buf, ix = items[i]
        if i >= 2 * NY:
            if i in (2 * NY + 1, 2 * NY + 3):
                for n in range(2):
                    wait_recv(buf.at[ix, my_half(n)], str_.at[(i - 2 * NY - 1) // 2, 2 + n])
            else:
                wait_recv(buf.at[ix, pl.ds(my_rows, T)], a2ar.at[i - 2 * NY])
        blk = buf.at[ix, pl.ds(my_rows, T)]
        rc(blk, blk, ags.at[i], agr.at[i, 0], XR).start()
        rc(blk, blk, ags.at[i], agr.at[i, 1], XL).start()
        rc(blk, blk, ags.at[i], agr.at[i, 4], PT).start()

    def fwd(i):
        buf, ix = items[i]
        lb, rb_ = rb(-1), rb(1)
        blk = buf.at[ix, pl.ds(lb, T)]
        wait_recv(blk, agr.at[i, 0])
        half = buf.at[ix, pl.ds(lb, TQ if i == BY_Y[0] else TH)]
        rc(half, half, ags.at[i], agr.at[i, 2], XR).start()
        rc(blk, blk, ags.at[i], agr.at[i, 4], PT).start()
        blk = buf.at[ix, pl.ds(rb_, T)]
        wait_recv(blk, agr.at[i, 1])
        half = buf.at[ix, pl.ds(pl.multiple_of(rb_ + TH, TH), TQ if i == BY_Y[1] else TH)]
        rc(half, half, ags.at[i], agr.at[i, 3], XL).start()
        rc(blk, blk, ags.at[i], agr.at[i, 4], PT).start()

    def opp(i):
        buf, ix = items[i]
        ob = rb(2)
        wait_recv(buf.at[ix, pl.ds(ob, TH)], agr.at[i, 2])
        wait_recv(buf.at[ix, pl.ds(pl.multiple_of(ob + TH, TH), TH)], agr.at[i, 3])
        blk = buf.at[ix, pl.ds(ob, T)]
        rc(blk, blk, ags.at[i], agr.at[i, 4], PT).start()

    def fin(i):
        buf, ix = items[i]
        wait_recv(buf.at[ix, pl.ds(pl.multiple_of((1 - h) * HR, HR), HR)], agr.at[i, 4])

    def ag_sent(i):
        buf, ix = items[i]
        wait_send(buf.at[ix, pl.ds(0, 7 * T - (TQ if i in BY_Y else 0))], ags.at[i])

    par = pl.ds(mul(h, HR), HR)

    def xc_send(n):
        rc(XS.at[x_order[n], par], XC.at[y, par], xcs.at[n], xcr.at[n], (YU, YD)[n]).start()

    def xc_fwd(n):
        b = XC.at[seq((-1, 1)[n]), par]
        wait_recv(b, xcr.at[n])
        rc(b, b, xcs.at[2 + n], xcr.at[2 + n], PT).start()

    def xc_fin(n):
        wait_recv(XC.at[seq((-1, 1)[n]), pl.ds(mul(1 - h, HR), HR)], xcr.at[2 + n])

    def ybuf(q):
        return (OA if q < NP else DQA).at[q % NP]

    def yown(q):
        b = ybuf(q).at[y]
        rc(b, b, ys.at[q], yr.at[q, 0], YU).start()
        rc(b, b, ys.at[q], yr.at[q, 1], YD).start()

    def yfwd(q):
        b = ybuf(q)
        wait_recv(b.at[seq(-1)], yr.at[q, 0])
        half = b.at[seq(-1), pl.ds(0, HR)]
        rc(half, half, ys.at[q], yr.at[q, 2], YU).start()
        wait_recv(b.at[seq(1)], yr.at[q, 1])
        half = b.at[seq(1), pl.ds(HR, HR)]
        rc(half, half, ys.at[q], yr.at[q, 3], YD).start()

    def yopp(q):
        b = ybuf(q)
        wait_recv(b.at[seq(2), pl.ds(0, HR)], yr.at[q, 2])
        wait_recv(b.at[seq(2), pl.ds(HR, HR)], yr.at[q, 3])

    def ysent(q):
        wait_send(ybuf(q).at[pl.ds(0, 3)], ys.at[q])

    def acc(p, d, first):
        cols = pl.ds(mul(p, 2 * E), 2 * E)
        MY[0, :, cols] = d[:HR] if first else MY[0, :, cols] + d[:HR]
        MY[1, :, cols] = d[HR:] if first else MY[1, :, cols] + d[HR:]

    def proj_x(i):
        k = x_order[i]
        wq_cp(k).wait()
        for cp in wkv_cp(k):
            cp.wait()

        def body(p):
            w = jnp.concatenate([WQ[2 * p], WQ[2 * p + 1]], axis=1)
            acc(p, nn(XS[k], w), i == 0)
        loop(NP, body)
        d = nn(XS[k], jnp.concatenate([WKV[0], WKV[1]], axis=1))
        KVACC[...] = d if i == 0 else KVACC[...] + d
        nk = x_order[i + 1] if i + 1 < NY else 0
        wq_cp(nk).start()
        for cp in wkv_cp(nk):
            cp.start()

    def proj_dy(i):
        k = dy_order[i]
        wo_cp(k).wait()

        def body(p):
            w = WO[pl.ds(2 * p, 2)].reshape(2 * E, CW)
            acc(p, nt(DYS[k], w), i == 0)
        loop(NP, body, unroll=UNR if i == NY - 1 else None)
        if i + 1 < NY:
            wo_cp(dy_order[i + 1]).start()

    def copy_acc(dst):
        def body(p):
            cols = pl.ds(mul(p, 2 * E), 2 * E)
            dst[p, 0:HR, :] = MY[0, :, cols].astype(BF16)
            dst[p, HR:R, :] = MY[1, :, cols].astype(BF16)
        loop(NP, body)

    T2 = 2 * T

    def pos(i):
        g = lax.div(i, T)
        return (2 * lax.rem(g, NX) + lax.div(g, NX)) * T + lax.rem(i, T)

    def brow(i, g):
        return lax.div(i, T2) * HR + g * T2 + lax.rem(i, T2)

    def pick(load, g):
        return jnp.concatenate([load(slice(g * T2, g * T2 + T2)), load(slice(HR + g * T2, HR + g * T2 + T2))], axis=0)

    def put(store, g, v):
        store(slice(g * T2, g * T2 + T2), v[:T2])
        store(slice(HR + g * T2, HR + g * T2 + T2), v[T2:])

    def keys(t, g):
        return pick(lambda r: KV[t, r, :], 0) if g == 0 else KV[t]

    def probs(q, g):
        s = nt(q, keys(0, g)) * scale2
        n = s.shape[1]
        qp = pos(brow(lax.broadcasted_iota(jnp.int32, (HR, 1), 0), g))
        kp = lax.broadcasted_iota(jnp.int32, (1, n), 1)
        kp = pos(brow(kp, 0) if g == 0 else kp)
        s = jnp.where(qp >= kp, s, -jnp.inf)
        e = jnp.exp2(s - jnp.max(s, axis=1, keepdims=True))
        return e * (1.0 / jnp.sum(e, axis=1, keepdims=True))

    def prow(g, b):
        r = (g * T2 * 2 // E + b) * HR
        return slice(r, r + HR)

    def attn_fwd(p):
        for g in range(2):
            for a in range(2):
                ln = slice(a * E, (a + 1) * E)
                pr = probs(pick(lambda r: QB[p, r, ln], g), g)
                for b in range(pr.shape[1] // E):
                    dwq_ref[2 * p + a, prow(g, b), :] = pr[:, b * E:(b + 1) * E]
                o = nn(pr.astype(BF16), keys(1, g)).astype(BF16)

                def store(r, v):
                    OA[p, y, r, ln] = v
                put(store, g, o)

    def attn_bwd(p):
        for g in range(2):
            for a in range(2):
                ln = slice(a * E, (a + 1) * E)
                q = pick(lambda r: QB[p, r, ln], g)
                do = pick(lambda r: DOB[p, r, ln], g)
                o = pick(lambda r: OA[p, y, r, ln], g)
                pr = jnp.concatenate([dwq_ref[2 * p + a, prow(g, b), :] for b in range((2 + 2 * g) * T2 // E)], axis=1)
                delta = jnp.sum(do.astype(F32) * o.astype(F32), axis=1, keepdims=True)
                dp = nt(do, keys(1, g))
                ds = (pr * (dp - delta)).astype(BF16)
                dq = (nn(ds, keys(0, g)) * scale).astype(BF16)
                dkv = jnp.concatenate([tn(ds, q), tn(pr.astype(BF16), do)], axis=1)

                def store(r, v):
                    DQA[p, y, r, ln] = v
                put(store, g, dq)
                if g == 0:
                    def add(r, v):
                        KVACC[r, :] = KVACC[r, :] + v
                    put(add, 0, dkv)
                else:
                    KVACC[...] = KVACC[...] + dkv

    def dkv_send():
        KVACC[:, :E] = KVACC[:, :E] * scale
        rc(KVACC, DKVR, exs.at[0], exr.at[0], PT).start()

    def dkv_sum():
        wait_recv(DKVR, exr.at[0])
        tot = (KVACC[...] + DKVR[...]).astype(BF16)
        DKVB[0] = tot[:, :E]
        DKVB[1] = tot[:, E:]

    KB = CW // 2
    KT = tile_of(KB, KTW)

    def dwkv_tile(r, t):
        ck = 2 * h + lax.div(r, 2)
        off = pl.multiple_of(KB * lax.rem(r, 2) + t * KT, KT)
        kv = jnp.concatenate([DKVB[0], DKVB[1]], axis=1)
        return tn(XS[ck, :, pl.ds(off, KT)], kv)

    KH = KB // 2

    def dwkv_early():
        def body(t):
            KS[0, pl.ds(mul(t, KT), KT), :] = dwkv_tile(seq(2), t).astype(BF16)
        loop(KB // KT, body)
        rc(KS.at[0, pl.ds(0, KH)], KR.at[0, pl.ds(0, KH)], dks.at[0], dkr.at[0], YU).start()
        rc(KS.at[0, pl.ds(KH, KH)], KR.at[0, pl.ds(KH, KH)], dks.at[0], dkr.at[1], YD).start()

    def dwkv_part(n):
        def body(t):
            KS[n + 1, pl.ds(mul(t, KT), KT), :] = dwkv_tile(seq((1, -1)[n]), t).astype(BF16)
        loop(KB // KT, body)

    def dwkv_own():
        def body(t):
            rows = pl.ds(mul(t, KT), KT)
            v = dwkv_tile(y, t)
            dwk_ref[rows, :] = v[:, :E]
            dwv_ref[rows, :] = v[:, E:]
        loop(KB // KT, body)

    def dwkv_mid():
        for n, dev in enumerate((YU, YD)):
            half = pl.ds(n * KH, KH)
            wait_recv(KR.at[0, half], dkr.at[n])
            KS[n + 1, half, :] = (KS[n + 1, half, :].astype(F32) + KR[0, half, :].astype(F32)).astype(BF16)
            rc(KS.at[n + 1], KR.at[n + 1], dks.at[n + 1], dkr.at[n + 2], dev).start()

    def dwkv_final():
        for n in range(2):
            wait_recv(KR.at[n + 1], dkr.at[n + 2])

        def body(t):
            rows = pl.ds(mul(t, KT), KT)
            v = KR[1, rows, :].astype(F32) + KR[2, rows, :].astype(F32)
            dwk_ref[rows, :] = dwk_ref[rows, :] + v[:, :E]
            dwv_ref[rows, :] = dwv_ref[rows, :] + v[:, E:]
        loop(KB // KT, body)

    def rx_free():
        for dev in (XL, XR):
            pl.semaphore_signal(cred, inc=1, device_id=dev, device_id_type=MESH)

    CH = CW // 2
    NT = tile_of(CH, DXT)

    def w_half(k, g):
        rows, dst = pl.ds(k * CW + g * CH, CH), pl.ds(g * CH, CH)
        return [pltpu.make_async_copy(wq_ref.at[:, rows, :], WQ.at[:, dst, :], lwq.at[1 + g]),
                pltpu.make_async_copy(wk_ref.at[c, rows], WKV.at[0, dst], lwkv.at[2 + g]),
                pltpu.make_async_copy(wv_ref.at[c, rows], WKV.at[1, dst], lwkv.at[4 + g])]

    def dxc(k):
        if k == 0:
            wq_cp(0).wait()
            for cp in wkv_cp(0):
                cp.wait()
        for g in range(2):
            if k:
                for cp in w_half(k, g):
                    cp.wait()

            def body(t):
                off = pl.multiple_of(t * NT + g * CH, NT)
                rows = pl.ds(off, NT)
                w = jnp.concatenate([WQ[i, rows, :] for i in range(NH)] + [WKV[h, rows, :]], axis=1)
                v = nt(jnp.concatenate([DQA[p, y] for p in range(NP)] + [DKVB[h]], axis=1), w)
                lo, hi = v[:HR], v[HR:]
                MY[k, :, pl.ds(off, NT)] = jnp.where(h == 0, lo, hi)
                DYS[k, pl.ds(HR, HR), pl.ds(off, NT)] = jnp.where(h == 0, hi, lo).astype(BF16)
            loop(CH // NT, body, unroll=UNR)
            if k + 1 < NY:
                for cp in w_half(k + 1, g):
                    cp.start()
        rc(DYS.at[k, pl.ds(HR, HR)], DYS.at[k, pl.ds(0, HR)], pxs.at[k], pxr.at[k], PT).start()

    def blk(k, cc, o, n):
        rows = pl.ds(pl.multiple_of(cc * T + o, TH), n)
        return MY[k, rows, :] + DYS[k, rows, :].astype(F32)

    def rx_early(k, n):
        return WO.at[n, k * TH:(k + 1) * TH]

    def rx_full(k, n):
        i = 2 * (k % 2)
        return WO.at[2 + 2 * n + k // 2, i * TH:(i + 2) * TH]

    def rs1(k):
        wait_recv(DYS.at[k, pl.ds(0, HR)], pxr.at[k])
        SX[k, 0:T, :] = blk(k, chip(2), 0, T).astype(BF16)
        for n, dev in enumerate((XR, XL)):
            rc(SX.at[k, n * TH:(n + 1) * TH], rx_early(k, n), rss.at[k], rsr.at[k, n], dev).start()

    def rs2(k):
        for n, dev in enumerate((XR, XL)):
            o = (n + 1) * T
            add = slice(o + n * TH, o + (n + 1) * TH)
            SX[k, o + (1 - n) * TH:o + (2 - n) * TH, :] = blk(k, chip(1 - 2 * n), (1 - n) * TH, TH).astype(BF16)
            wait_recv(rx_early(k, n), rsr.at[k, n])
            SX[k, add, :] = (blk(k, chip(1 - 2 * n), n * TH, TH) + rx_early(k, n)[...].astype(F32)).astype(BF16)
            rc(SX.at[k, o:o + T], rx_full(k, n), rss.at[k], rsr.at[k, 2 + n], dev).start()

    def rs3(k):
        v = blk(k, c, 0, T)
        for n in range(2):
            wait_recv(rx_full(k, n), rsr.at[k, 2 + n])
            v = v + rx_full(k, n)[...].astype(F32)
        dx_ref[:, k * CW:(k + 1) * CW] = v.astype(BF16)

    OT = tile_of(CW, 512)

    others = [seq(1), seq(-1), seq(2)]

    def dwo_own(p):
        def body(t):
            cols = pl.ds(mul(t, OT), OT)
            v = tn(OA[p, y], DYC[y, :, cols])
            dwo_ref[2 * p, :, cols] = v[:E]
            dwo_ref[2 * p + 1, :, cols] = v[E:]
        loop(CW // OT, body)

    def dwo(p):
        def body(t):
            cols = pl.ds(mul(t, OT), OT)
            v = tn(jnp.concatenate([OA[p, s] for s in others], axis=0),
                    jnp.concatenate([DYC[s, :, cols] for s in others], axis=0))
            dwo_ref[2 * p, :, cols] = dwo_ref[2 * p, :, cols] + v[:E]
            dwo_ref[2 * p + 1, :, cols] = dwo_ref[2 * p + 1, :, cols] + v[E:]
        loop(CW // OT, body)

    def dwq_own(p):
        def body(t):
            cols = pl.ds(mul(t, OT), OT)
            v = tn(XC[y, :, cols], DQA[p, y])
            dwq_ref[2 * p, cols, :] = v[:, :E]
            dwq_ref[2 * p + 1, cols, :] = v[:, E:]
        loop(CW // OT, body)

    def dwq(p):
        def body(t):
            cols = pl.ds(mul(t, OT), OT)
            v = tn(jnp.concatenate([XC[s, :, cols] for s in others], axis=0),
                    jnp.concatenate([DQA[p, s] for s in others], axis=0))
            dwq_ref[2 * p, cols, :] = dwq_ref[2 * p, cols, :] + v[:, :E]
            dwq_ref[2 * p + 1, cols, :] = dwq_ref[2 * p + 1, cols, :] + v[:, E:]
        loop(CW // OT, body)

    def own_cols(dst, src):
        def body(t):
            rows = pl.ds(pl.multiple_of(t * T, T), T)
            dst[y, rows, :] = src[y, rows, :]
        loop(R // T, body)

    own(0)
    own(1)
    far_send(1)
    for cp in ldc:
        cp.wait()
    far_send(0)
    for j, dev in ((1, YU), (-1, YD)):
        rc(DYS.at[seq(j), pl.ds(my_rows, T)], DYC.at[y, pl.ds(my_rows, T)],
           a2as.at[0], a2ar.at[1 + j], dev).start()

    def compute(i):
        if i < NY:
            if i < 2:
                xc_send(i)
            proj_x(i)
            if i == 3:
                copy_acc(QB)
                KV[0] = KVACC[:, :E].astype(BF16)
                KV[1] = KVACC[:, E:].astype(BF16)
                for p in range(NP):
                    if p < 2:
                        fwd(NY + p)
                        own(NY + p + 2)
                    attn_fwd(p)
                    yown(p)
                own_cols(XC, XS)
        elif i < 8:
            proj_dy(i - NY)
            if i == 4:
                own_cols(DYC, DYS)
            if i == 5:
                xc_fwd(0)
                yfwd(0)
                dwo_own(0)
                dwo_own(1)
            if i == 6:
                dyc_send()
                xc_fwd(1)
                yfwd(1)
                dwo_own(2)
            if i == 7:
                rx_free()
                yfwd(2)
                copy_acc(DOB)
                KVACC[...] = jnp.zeros_like(KVACC)

    for i in range(9):
        if i not in (4, 5, 8):
            fwd(i)
        if i == 0:
            far_fwd(1)
        if i == 1:
            far_fwd(0)
        for n in (4, 5) if i == 3 else () if i == 2 else (i + 2,) if i < 4 else range(8, N_IT) if i == 7 else ():
            own(n)
        if i >= 1:
            opp(i - 1)
            fin(i - 1)
            compute(i - 1)

    attn_bwd(0)
    yown(NP)
    fwd(8)
    attn_bwd(1)
    yown(NP + 1)
    attn_bwd(2)
    yown(NP + 2)
    fwd(9)
    for k in range(NY):
        ag_sent(NY + k)
    wait_send(DYS.at[0, pl.ds(0, 2 * T)], a2as.at[0])
    for n in range(2):
        wait_send(DYS.at[0, pl.ds(0, TH)], sts.at[0, n])
        wait_send(DYS.at[0, pl.ds(0, TQ)], dcs.at[n])
    dkv_send()
    for p in range(NP):
        dwq_own(p)
    fwd(10)
    dkv_sum()
    dxc(0)
    dxc(1)
    fwd(11)
    pl.semaphore_wait(cred, 2)
    rs1(0)
    opp(8)
    dwkv_early()
    yfwd(NP)
    dxc(2)
    rs1(1)
    yfwd(NP + 1)
    opp(9)
    dwkv_part(0)
    dxc(3)
    rs1(2)
    rs2(0)
    opp(10)
    yfwd(NP + 2)
    dwkv_part(1)
    rs1(3)
    rs2(1)
    opp(11)
    for i in range(2 * NY, N_IT - 1):
        fin(i)
    for p in range(NP):
        yopp(p)
        dwo(p)
        if p == 1:
            rs2(2)
            dwkv_mid()
    for n in range(2):
        xc_fin(n)
    fin(N_IT - 1)
    yopp(NP)
    dwq(0)
    rs2(3)
    dwkv_own()
    rs3(0)
    yopp(NP + 1)
    dwq(1)
    rs3(1)
    yopp(NP + 2)
    dwq(2)
    rs3(2)
    dwkv_final()
    rs3(3)

    for i in list(range(NY)) + list(range(2 * NY, N_IT)):
        ag_sent(i)
    for n in range(2):
        wait_send(XS.at[0, pl.ds(0, TH)], sts.at[1, n])
        for t in range(2):
            wait_send(ST.at[t, n], sts.at[t, 2 + n])
    for n in range(4):
        wait_send(XC.at[0, par], xcs.at[n])
    for q in range(2 * NP):
        ysent(q)
    wait_send(KVACC, exs.at[0])
    for n in range(3):
        wait_send(KS.at[n], dks.at[n])
    for k in range(NY):
        wait_send(DYS.at[k, pl.ds(HR, HR)], pxs.at[k])
        wait_send(SX.at[k], rss.at[k])


def copy_out(*refs):
    n = (len(refs) - 1) // 2
    cps = [pltpu.make_async_copy(refs[i], refs[n + i], refs[-1].at[i]) for i in range(n)]
    for cp in cps:
        cp.start()
    for cp in cps:
        cp.wait()


def solution(mesh):
    model_size = mesh.shape['model']
    tok_spec = P(('pod', 'data'), 'model', None)

    def device_step(x_loc, dy_loc, w_q, w_k, w_v, w_o):
        T, D = x_loc.shape[1:]
        NH, E = w_q.shape[1:]
        KVH = w_k.shape[0]
        NX = model_size // 2
        NY = mesh.shape['data']
        assert NX == 4 and NY == 4 and KVH == NX and NH == 6 and E == 2 * T
        NP = NH // 2
        CW = D // NY
        assert CW == 6 * NX * T
        R = model_size * T
        KB = CW // 2
        cfg = (T, CW, E, NX, NY, NH)
        V = pltpu.VMEM
        S = pltpu.SemaphoreType.DMA
        n_it = 3 * NY
        scratch = [
            V((NY, R, CW), BF16), V((NY, R, CW), BF16), V((NY, R, CW), BF16), V((NY, R, CW), BF16),
            V((NP, NY, R, 2 * E), BF16), V((NP, NY, R, 2 * E), BF16),
            V((NP, R, 2 * E), BF16), V((NP, R, 2 * E), BF16), V((2, R, E), BF16),
            V((R, 2 * E), F32), V((R, 2 * E), F32), V((2, R, E), BF16),
            V((NH, CW, E), BF16), V((2, CW, E), BF16), V((NH, E, CW), BF16),
            V((NY, R // 2, CW), F32), V((NY, 3 * T, CW), BF16), V((NY - 1, KB, 2 * E), BF16), V((NY - 1, KB, 2 * E), BF16),
            V((2, 2, T // 2, CW), BF16),
            S((n_it, 5)), S((n_it,)), S((NY,)), S((1,)), S((2, 4)), S((2, 4)), S((2,)), S((4,)), S((4,)), S((2 * NP, 4)), S((2 * NP,)),
            S((4,)), S((3,)), S((NY,)), S((NY,)), S((NY, 4)), S((NY,)), S((1,)), S((1,)),
            S((NY,)), S((NY,)), S((3,)), S((6,)), S((1,)), pltpu.SemaphoreType.REGULAR,
        ]
        any_spec = pl.BlockSpec(memory_space=pl.ANY)
        dx, dwq, dwk, dwv, dwo = pl.pallas_call(
            functools.partial(kernel, cfg),
            out_shape=[V((T, D), BF16), V((NH, CW, E), F32), V((KB, E), F32), V((KB, E), F32), V((NH, E, CW), F32)],
            in_specs=[any_spec] * 6,
            out_specs=[pl.BlockSpec(memory_space=V)] * 5,
            scratch_shapes=scratch,
            compiler_params=pltpu.CompilerParams(collective_id=0, has_side_effects=True, vmem_limit_bytes=VMEM_BYTES),
            name='attn_bwd_fused',
        )(x_loc[0], dy_loc[0], w_q.transpose(1, 0, 2), w_k, w_v, w_o)
        outs = (dx, dwq, dwk, dwv, dwo)
        dx, dwq, dwk, dwv, dwo = pl.pallas_call(
            copy_out,
            out_shape=[jax.ShapeDtypeStruct(o.shape, o.dtype) for o in outs],
            in_specs=[pl.BlockSpec(memory_space=OUT_IN)] * 5,
            out_specs=[any_spec] * 5,
            scratch_shapes=[S((5,))],
            compiler_params=pltpu.CompilerParams(vmem_limit_bytes=OUT_LIM),
            name='write_results',
        )(*outs)
        return dx[None], dwq.transpose(1, 0, 2), dwk, dwv, dwo

    kv_rows = P(('pod', 'model', 'data'), None)
    return jax.shard_map(device_step, mesh=mesh,
                         in_specs=(tok_spec, tok_spec, P(None, 'model', None), P(), P(), P('model', None, None)),
                         out_specs=(tok_spec, P(('pod', 'data'), 'model', None), kv_rows, kv_rows, P(('pod', 'model'), None, 'data')),
                         check_vma=False)
```
